128 devices in a mesh: dom: 32 (over y, x, core), dim: 4 (over z).
Axes of the slice: x: 4, y: 4, z: 4, core: 2. Of those that a mesh axis runs over, the one named last changes fastest.
Arguments:
- particles: float32 [256, 1024], P('dom', 'dim'), may hold values from -5 to 5
- data_rows: bfloat16 [256, 16, 1024], P('dom', None, 'dim'), may hold values from -0.375 to 0.375
- labels: int32 [256, 16], P('dom'), may hold values from 0 to 1
Outputs:
- updates: float32 [2, 256, 1024], P(None, 'dom', 'dim')
The draws below stay inside these ranges and needn't reach their ends.
All inputs are finite; a program needn't handle non-finite values.
Results may differ from the reference program's by a relative error of at most 0.0003.
Values may be sent and summed in bfloat16 or wider, within the bound.
No kernel may reach another device: no remote copies, remote signals or barrier semaphores. Data moves between devices by JAX's collectives and lax.ppermute only.
A program may use at most 64 MiB of HBM per device.

```python
import math
import jax
import jax.numpy as jnp
from jax import lax

D = 1024
R = 16
NEWTON = 2
CG_STEPS = 2
BAND = 1
PARTICLES = 256


def draw_particles(key, part):
    scale_key, value_key = jax.random.split(key, 2)
    spread = jnp.exp(jax.random.uniform(scale_key, (PARTICLES, 1), jnp.float32, math.log(0.4), math.log(1.1)))
    values = jax.random.truncated_normal(value_key, -4.0, 4.0, (PARTICLES, D), jnp.float32)
    return spread * values


def touch_ends(result, key, least, largest):
    shape = result.shape
    spot = [jax.random.randint(jax.random.fold_in(key, axis), (), 0, shape[axis]) for axis in range(len(shape))]
    result = result.at[tuple(spot)].set(least)
    longest = shape.index(max(shape))
    spot[longest] = (spot[longest] + 1) % shape[longest]
    return result.at[tuple(spot)].set(largest)


def shard_levels(rng, dims, shards, least, top_value):
    def one(axis_at, parts):
        heights = jax.random.uniform(jax.random.fold_in(jax.random.fold_in(rng, 6), axis_at), (parts,), jnp.float32, least / len(shards), top_value / len(shards))
        return jnp.repeat(jnp.exp(heights), dims[axis_at] // parts).reshape((-1,) + (1,) * (len(dims) - axis_at - 1))

    loudness = one(*shards[0])
    for cut in shards[1:]:
        loudness = loudness * one(*cut)
    return loudness


def noise(key, dims, width, limit, shards=(), kind=jnp.bfloat16):
    array = jax.random.normal(key, dims, jnp.float32) * width
    if len(shards) > 0:
        array = shard_levels(key, dims, shards, -0.22, 0.18) * array
    return jnp.clip(array, min=-limit, max=limit).astype(kind)


def setup_inputs(seed: int = 0) -> dict:
    keys = jax.random.split(jax.random.key(seed), 4)
    particles = draw_particles(jax.random.fold_in(keys[3], 71), 0)
    data_rows = noise(keys[1], (PARTICLES, R, D), (D // 4) ** -0.5, 0.375, ((0, 32), (2, 4)))
    labels = touch_ends(jax.random.randint(keys[2], (PARTICLES, R), 0, 2), jax.random.fold_in(keys[2], 1), 0, 1).astype(jnp.int32)
    return {"particles": particles, "data_rows": data_rows, "labels": labels}


prior_precision = 0.05
like_weight = 4.0
move_size = 0.5
highest = lax.Precision.HIGHEST


def reference(particles, data_rows, labels):
    factor_rows = data_rows.astype(jnp.float32)
    targets = labels.astype(jnp.float32)
    count = particles.shape[0]
    kernel_scale = 1.0 * BAND * D
    cross_scale = 4.0 / (kernel_scale * kernel_scale)
    current = particles
    outputs = []
    for newton_step in range(NEWTON):
        logits = jnp.einsum("jrd,jd->jr", factor_rows, current, precision=highest)
        probs = jax.nn.sigmoid(logits)
        gradient = -prior_precision * current + like_weight * jnp.einsum("jr,jrd->jd", targets - probs, factor_rows, precision=highest)
        curvature = like_weight * probs * (1.0 - probs)
        squares = jnp.sum(current * current, axis=1)
        inner_rows = jnp.dot(current, current.T, precision=highest)
        distance = squares[:, None] + squares[None, :] - 2.0 * inner_rows
        kernel = jnp.exp(-distance / kernel_scale)
        kernel_sq = kernel * kernel
        kernel_total = jnp.sum(kernel, axis=1)
        square_total = jnp.sum(kernel_sq, axis=1)
        kernel_grad = jnp.dot(kernel, gradient, precision=highest)
        kernel_pos = jnp.dot(kernel, current, precision=highest)
        square_pos = jnp.dot(kernel_sq, current, precision=highest)
        drift = (kernel_grad + (2.0 / kernel_scale) * (current * kernel_total[:, None] - kernel_pos)) / count

        def apply_operator(vectors):
            along_self = jnp.sum(current * vectors, axis=1)
            along_mean = jnp.sum(vectors * square_pos, axis=1)
            projected = jnp.einsum("jrd,id->jri", factor_rows, vectors, precision=highest)
            weighted = projected * curvature[:, :, None] * kernel_sq.T[:, None, :]
            pairs = jnp.einsum("jrd,jri->id", factor_rows, weighted, precision=highest)
            along_pair = jnp.dot(current, vectors.T, precision=highest)
            pairs = pairs + cross_scale * jnp.dot((kernel_sq.T * along_pair).T, current, precision=highest)
            local = prior_precision * square_total[:, None] * vectors + cross_scale * (current * (along_self * square_total - along_mean)[:, None] - along_self[:, None] * square_pos)
            return (pairs + local) / count

        solution = jnp.zeros_like(drift)
        residual = drift
        direction = drift
        norm_now = jnp.sum(residual * residual)
        for solve_step in range(CG_STEPS):
            image = apply_operator(direction)
            alpha = norm_now / jnp.sum(direction * image)
            solution = solution + alpha * direction
            residual = residual - alpha * image
            if solve_step + 1 < CG_STEPS:
                norm_next = jnp.sum(residual * residual)
                direction = residual + (norm_next / norm_now) * direction
                norm_now = norm_next
        outputs.append(solution)
        current = current + move_size * solution
    return jnp.stack(outputs)
```

```python
from functools import partial

import jax
import jax.numpy as jnp
import numpy as np
from jax import lax
from jax.experimental import pallas as pl
from jax.experimental.pallas import tpu as pltpu
from jax.sharding import Mesh
from jax.sharding import PartitionSpec as P


AXES = ("y", "x", "c", "z")
NEWTON = 2
prior_precision = 0.05
like_weight = 4.0
move_size = 0.5

f32 = jnp.float32
bf16 = jnp.bfloat16
WIDE = 1024
MANY = 256
HALF = 128
DATA = 16
SLICE = 256
scale = 1.0 * WIDE
cross = 4.0 / (scale * scale)

MASKS = (1, 3)
ORDERS = ("xyz", "yzx", "zxy")
SPOT = {"y": 0, "x": 1, "z": 3}
STACK = {"z": 0, "y": 1, "x": 2}
ROWS = (768, 768, 512)
STARTS = (0, 768, 1536)


def pairs(axis, step):
    sizes = (4, 4, 2, 4)
    out = []
    for at in np.ndindex(*sizes):
        to = list(at)
        to[SPOT[axis]] ^= MASKS[(step + at[2]) % 2]
        out.append((int(np.ravel_multi_index(at, sizes)), int(np.ravel_multi_index(to, sizes))))
    return out


def swap_cores(x):
    return lax.ppermute(x, "c", [(0, 1), (1, 0)])


def gathered(own):
    parts = [own[48 * k : 48 * k + 48][None, None, None] for k in range(3)]
    for step in range(6):
        axes = [order[step // 2] for order in ORDERS]
        came = [lax.ppermute(p, AXES, pairs(a, step % 2)) for p, a in zip(parts, axes)]
        parts = [jnp.concatenate([p, q], axis=STACK[a]) for p, q, a in zip(parts, came, axes)]
    return [p.reshape(4, 16, 48, SLICE) for p in parts]


def row_owner():
    owner = []
    for first, count in ((0, 3), (3, 3), (6, 2)):
        for spot in range(16):
            for p in range(count):
                owner += [spot * 8 + first + p] * DATA
    return np.asarray(owner, np.int32)[None]


def two(v):
    high = v.astype(bf16)
    return high, (v - high.astype(f32)).astype(bf16)


def nt(a, b):
    return lax.dot_general(a, b, (((1,), (1,)), ((), ())), preferred_element_type=f32)


def nn(a, b):
    return lax.dot_general(a, b, (((1,), (0,)), ((), ())), preferred_element_type=f32)


def three(dot, a, b):
    return dot(a[0], b[0]) + (dot(a[0], b[1]) + dot(a[1], b[0]))


def z_spot(core, k):
    return k if k in (0, 3) else jnp.where(core == 0, k, 3 - k)


def block(refs, core, color, k):
    rows = ROWS[color]
    return refs[color][z_spot(core, k), :, : rows // 16, :].reshape(rows, SLICE)


def cols(k):
    return slice(k * SLICE, (k + 1) * SLICE)


def span(color):
    return slice(STARTS[color], STARTS[color] + ROWS[color])


def one_hot(owner_ref, color):
    return lax.broadcasted_iota(jnp.int32, (HALF, ROWS[color]), 0) == owner_ref[:, span(color)]


def grad_kernel(core_ref, g0, g1, g2, owner_ref, x_ref, grad_ref, curve_ref):
    core = core_ref[0]
    refs = (g0, g1, g2)
    x = x_ref[pl.ds(pl.multiple_of(core * HALF, HALF), HALF), :]
    high, low = two(x)
    both = jnp.concatenate([high, low], axis=0)
    sums = [None] * 4
    for color in range(3):
        logit = sum(nt(both[:, cols(k)], block(refs, core, color, k)) for k in range(4))
        hot = one_hot(owner_ref, color)
        logit = jnp.sum(jnp.where(hot, logit[:HALF] + logit[HALF:], 0.0), axis=0, keepdims=True)
        prob = 1.0 / (1.0 + jnp.exp(logit))
        curve_ref[:, span(color)] = like_weight * prob * (1.0 - prob)
        weight = jnp.concatenate(two(jnp.where(hot, like_weight * prob, 0.0)), axis=0)
        for k in range(4):
            part = nn(weight, block(refs, core, color, k))
            sums[k] = part if sums[k] is None else sums[k] + part
    for k in range(4):
        grad_ref[:, cols(k)] = (
            sums[k][:HALF] + sums[k][HALF:] - (prior_precision + 2.0 / scale) * x[:, cols(k)]
        )


def kernel_kernel(x_ref, kernel_ref):
    high, low = two(x_ref[...])
    both = (high, low)
    gram = three(nt, both, both)
    same = lax.broadcasted_iota(jnp.int32, (MANY, MANY), 0) == lax.broadcasted_iota(
        jnp.int32, (MANY, MANY), 1
    )
    diag = jnp.where(same, gram, 0.0)
    distance = (
        jnp.sum(diag, axis=1, keepdims=True) + jnp.sum(diag, axis=0, keepdims=True) - 2.0 * gram
    )
    kernel_ref[...] = jnp.exp(-distance / scale)


def first_kernel(
    core_ref, g0, g1, g2, owner_ref, x_ref, kernel_ref, own_ref, other_ref, curve_ref,
    drift_ref, image_ref, factor_ref,
):
    core = core_ref[0]
    refs = (g0, g1, g2)
    mine = pl.ds(pl.multiple_of(core * HALF, HALF), HALF)
    others = pl.ds(pl.multiple_of((1 - core) * HALF, HALF), HALF)
    kernel_own = kernel_ref[:, mine]
    drift = three(nn, two(kernel_own), two(own_ref[...])) + three(
        nn, two(kernel_ref[:, others]), two(other_ref[...])
    )
    total = jnp.sum(kernel_ref[...], axis=1, keepdims=True)
    x = x_ref[...]
    drift = (drift + (2.0 / scale) * total * x) / MANY
    drift_ref[...] = drift
    square = kernel_own * kernel_own
    square_two = two(square)
    drift_two = two(drift)
    sums = [None] * 4
    for color in range(3):
        hot = one_hot(owner_ref, color).astype(bf16)
        factor = (nn(square_two[0], hot) + nn(square_two[1], hot)) * curve_ref[:, span(color)]
        factor_ref[:, span(color)] = factor
        projected = sum(
            nt(d[:, cols(k)], block(refs, core, color, k)) for k in range(4) for d in drift_two
        )
        weighted = two(projected * factor)
        for k in range(4):
            part = sum(nn(w, block(refs, core, color, k)) for w in weighted)
            sums[k] = part if sums[k] is None else sums[k] + part
    x_own = two(x_ref[mine, :])
    along = three(nt, drift_two, x_own)
    self_along = jnp.sum(x * drift, axis=1, keepdims=True)
    q = square * (self_along - along)
    q_two = two(q)
    q_total = jnp.sum(q, axis=1, keepdims=True)
    square_total = jnp.sum(square, axis=1, keepdims=True)
    for k in range(4):
        pull = three(nn, q_two, (x_own[0][:, cols(k)], x_own[1][:, cols(k)]))
        image_ref[:, cols(k)] = (
            sums[k]
            + prior_precision * square_total * drift[:, cols(k)]
            + cross * (x[:, cols(k)] * q_total - pull)
        ) / MANY


def second_kernel(
    core_ref, g0, g1, g2, x_ref, kernel_ref, factor_ref, drift_ref, own_ref, other_ref,
    image_ref, sums_ref,
):
    core = core_ref[0]
    refs = (g0, g1, g2)
    mine = pl.ds(pl.multiple_of(core * HALF, HALF), HALF)
    image = own_ref[...] + other_ref[...]
    image_ref[...] = image
    drift = drift_ref[...]
    image_two = two(image)
    total = jnp.zeros((MANY, 1), f32)
    for color in range(3):
        projected = sum(
            nt(d[:, cols(k)], block(refs, core, color, k)) for k in range(4) for d in image_two
        )
        total += jnp.sum(
            projected * projected * factor_ref[:, span(color)], axis=1, keepdims=True
        )
    square = kernel_ref[:, mine] * kernel_ref[:, mine]
    x = x_ref[...]
    along = three(nt, image_two, two(x_ref[mine, :]))
    gap = jnp.sum(x * image, axis=1, keepdims=True) - along
    total += cross * jnp.sum(square * gap * gap, axis=1, keepdims=True)
    length = jnp.sum(image * image, axis=1, keepdims=True)
    total += prior_precision * jnp.sum(square, axis=1, keepdims=True) * length
    figures = (
        jnp.sum(drift * drift),
        jnp.sum(drift * image),
        jnp.sum(length),
        jnp.sum(total) / MANY,
    )
    row = lax.broadcasted_iota(jnp.int32, (8, 128), 0)
    out = jnp.zeros((8, 128), f32)
    for at, value in enumerate(figures):
        out = jnp.where(row == at, value, out)
    sums_ref[...] = out


def call(kernel, outs, *args):
    whole = pl.BlockSpec(memory_space=pltpu.VMEM)
    specs = [
        pl.BlockSpec(memory_space=pltpu.SMEM) if a.size == 1 else whole for a in args
    ]
    return pl.pallas_call(
        kernel,
        out_shape=[jax.ShapeDtypeStruct(s, f32) for s in outs],
        in_specs=specs,
        out_specs=[whole] * len(outs),
        compiler_params=pltpu.CompilerParams(vmem_limit_bytes=48 * 1024 * 1024),
    )(*args)


def per_device(particles, data_rows, labels):
    core = lax.axis_index("c")
    core_ref = core.astype(jnp.int32)[None]
    sign = (2 * labels - 1).astype(bf16)
    rows = (data_rows * sign[:, :, None]).reshape(8 * DATA, SLICE)
    rounded = lax.reduce_precision(particles, 8, 7)
    high, low = rounded.astype(bf16), (particles - rounded).astype(bf16)
    refs = gathered(jnp.concatenate([rows, high, low], axis=0))
    tail = refs[2][:, :, 32:, :].astype(f32)
    pieces = tail[:, :, :8] + tail[:, :, 8:]
    pieces = pieces.reshape(4, HALF, SLICE)
    first = core == 0
    middle = jnp.where(first, pieces[1], pieces[2]), jnp.where(first, pieces[2], pieces[1])
    x_own = jnp.concatenate([pieces[0], *middle, pieces[3]], axis=1)
    x_other = swap_cores(x_own)
    x = jnp.where(
        first,
        jnp.concatenate([x_own, x_other], axis=0),
        jnp.concatenate([x_other, x_own], axis=0),
    )
    owner = jnp.asarray(row_owner())
    outputs = []
    for newton_step in range(NEWTON):
        grad, curve = call(
            grad_kernel, [(HALF, WIDE), (1, HALF * DATA)], core_ref, *refs, owner, x
        )
        grad_other = swap_cores(grad)
        (kernel,) = call(kernel_kernel, [(MANY, MANY)], x)
        drift, image_own, factor = call(
            first_kernel,
            [(MANY, WIDE), (MANY, WIDE), (MANY, HALF * DATA)],
            core_ref, *refs, owner, x, kernel, grad, grad_other, curve,
        )
        image, sums = call(
            second_kernel,
            [(MANY, WIDE), (8, 128)],
            core_ref, *refs, x, kernel, factor, drift, image_own, swap_cores(image_own),
        )
        other = swap_cores(sums)
        mu0, mu1, mu2 = sums[0, 0], sums[1, 0], sums[2, 0]
        mu3 = sums[3, 0] + other[3, 0]
        alpha = mu0 / mu1
        left = mu0 - 2.0 * alpha * mu1 + alpha * alpha * mu2
        beta = left / mu0
        curved = (1.0 + beta) ** 2 * mu1 - 2.0 * (1.0 + beta) * alpha * mu2 + alpha * alpha * mu3
        gamma = left / curved
        on_drift = alpha + gamma * (1.0 + beta)
        on_image = -gamma * alpha
        own = lambda v: lax.dynamic_slice(v, (core * HALF, 0), (8, SLICE))
        outputs.append(on_drift * own(drift) + on_image * own(image))
        if newton_step + 1 < NEWTON:
            x = x + move_size * (on_drift * drift + on_image * image)
    return jnp.stack(outputs)


def solution(mesh):
    torus = Mesh(mesh.devices.reshape(4, 4, 2, mesh.shape["dim"]), AXES)
    groups = ("y", "x", "c")
    in_specs = (P(groups, "z"), P(groups, None, "z"), P(groups, None))
    out_specs = P(None, groups, "z")
    return jax.shard_map(
        per_device, mesh=torus, in_specs=in_specs, out_specs=out_specs, check_vma=False
    )
```

```python
from functools import partial

import jax
import jax.numpy as jnp
import numpy as np
from jax import lax
from jax.experimental import pallas as pl
from jax.experimental.pallas import tpu as pltpu
from jax.sharding import Mesh
from jax.sharding import PartitionSpec as P


AXES = ("y", "x", "c", "z")
NEWTON = 2
prior_precision = 0.05
like_weight = 4.0
move_size = 0.5

f32 = jnp.float32
bf16 = jnp.bfloat16
WIDE = 1024
MANY = 256
HALF = 128
DATA = 16
SLICE = 256
scale = 1.0 * WIDE
cross = 4.0 / (scale * scale)

MASKS = (1, 3)
ORDERS = ("xyz", "yzx", "zxy")
SPOT = {"y": 0, "x": 1, "z": 3}
STACK = {"z": 0, "y": 1, "x": 2}
ROWS = (768, 768, 512)
STARTS = (0, 768, 1536)
CHUNK = 512
VMEM_LIMIT = 24 * 1024 * 1024


def pairs(axis, step):
    sizes = (4, 4, 2, 4)
    out = []
    for at in np.ndindex(*sizes):
        to = list(at)
        to[SPOT[axis]] ^= MASKS[(step + at[2]) % 2]
        out.append((int(np.ravel_multi_index(at, sizes)), int(np.ravel_multi_index(to, sizes))))
    return out


def swap_cores(x):
    return lax.ppermute(x, "c", [(0, 1), (1, 0)])


def gathered(own):
    parts = [own[48 * k : 48 * k + 48][None, None, None] for k in range(3)]
    for step in range(6):
        axes = [order[step // 2] for order in ORDERS]
        came = [lax.ppermute(p, AXES, pairs(a, step % 2)) for p, a in zip(parts, axes)]
        parts = [jnp.concatenate([p, q], axis=STACK[a]) for p, q, a in zip(parts, came, axes)]
        parts = lax.optimization_barrier(parts)
    return [p.reshape(4, 16, 48, SLICE) for p in parts]


def two(v):
    high = v.astype(bf16)
    return high, (v - high.astype(f32)).astype(bf16)


def nn(a, b):
    return lax.dot_general(a, b, (((1,), (0,)), ((), ())), preferred_element_type=f32)


def tn(a, b):
    return lax.dot_general(a, b, (((0,), (0,)), ((), ())), preferred_element_type=f32)


def stacked(a, b):
    left = jnp.concatenate([a[0], a[1], a[0]], axis=1)
    right = jnp.concatenate([b[0], b[0], b[1]], axis=0)
    return nn(left, right)


def z_spot(core, k):
    return k if k in (0, 3) else jnp.where(core == 0, k, 3 - k)


def cols(k):
    return slice(k * SLICE, (k + 1) * SLICE)


def span(color):
    return slice(STARTS[color], STARTS[color] + ROWS[color])


def half_of(core):
    return pl.ds(pl.multiple_of(core * HALF, HALF), HALF)


def in_order(core, own, other, axis):
    pair = jnp.where(core == 0, own, other), jnp.where(core == 0, other, own)
    return jnp.concatenate(pair, axis=axis)


def assemble_kernel(core_ref, g0, g1, g2, rows_ref, turned_ref, hot_ref, x_ref):
    core = core_ref[0]
    for k in range(4):
        at = z_spot(core, k)
        for color, ref in enumerate((g0, g1, g2)):
            count = ROWS[color]
            piece = ref[at, :, : count // 16, :].reshape(count, SLICE)
            rows_ref[span(color), cols(k)] = piece
            turned_ref[cols(k), span(color)] = piece.T
        tail = g2[at, :, 32:, :].astype(f32)
        x_ref[cols(k), :] = (tail[:, :8] + tail[:, 8:]).reshape(HALF, SLICE).T
    for color, first in enumerate((0, 3, 6)):
        count = ROWS[color]
        row = lax.broadcasted_iota(jnp.int32, (count, HALF), 0)
        spot = (row * 43691) >> 21 if color < 2 else row >> 5
        owner = spot * 8 + first + ((row - spot * (count // 16)) >> 4)
        hot = owner == lax.broadcasted_iota(jnp.int32, (count, HALF), 1)
        hot = jnp.where(hot, 1.0, 0.0).astype(bf16)
        hot_ref[span(color), :HALF] = hot
        hot_ref[span(color), HALF:] = hot


def gradient(rows_ref, turned_ref, hot_ref, x, grad_ref, curve_ref):
    both = jnp.concatenate(two(x), axis=1)
    weights = []
    for at in range(0, HALF * DATA, CHUNK):
        part = pl.ds(at, CHUNK)
        logit = nn(rows_ref[part, :], both)
        hot = hot_ref[part, :HALF].astype(f32)
        logit = jnp.sum((logit[:, :HALF] + logit[:, HALF:]) * hot, axis=1, keepdims=True)
        prob = 1.0 / (1.0 + jnp.exp(logit))
        curve_ref[part, :] = jnp.broadcast_to(like_weight * prob * (1.0 - prob), (CHUNK, HALF))
        weights.append(jnp.concatenate(two(like_weight * prob * hot), axis=1))
    total = nn(turned_ref[...], jnp.concatenate(weights, axis=0))
    grad_ref[...] = total[:, :HALF] + total[:, HALF:] - (prior_precision + 2.0 / scale) * x


def grad_kernel(rows_ref, turned_ref, hot_ref, x_ref, grad_ref, curve_ref):
    gradient(rows_ref, turned_ref, hot_ref, x_ref[...], grad_ref, curve_ref)


def factors(own_ref, other_ref):
    mu0, mu1, mu2 = (own_ref[k : k + 1, :1] for k in range(3))
    mu3 = own_ref[3:4, :1] + other_ref[3:4, :1]
    alpha = mu0 / mu1
    left = mu0 - 2.0 * alpha * mu1 + alpha * alpha * mu2
    grown = 1.0 + left / mu0
    gamma = left / (grown * grown * mu1 - 2.0 * grown * alpha * mu2 + alpha * alpha * mu3)
    return alpha + gamma * grown, -gamma * alpha


def own_update(core, on_drift, on_image, drift_ref, image_ref, out_ref):
    mine = half_of(core)
    update = on_drift * drift_ref[:SLICE, mine] + on_image * image_ref[:SLICE, mine]
    out_ref[...] = update.T[:8, :]


def next_kernel(
    core_ref, rows_ref, turned_ref, hot_ref, x_ref, drift_ref, image_ref, own_ref, other_ref,
    grad_ref, curve_ref, new_ref, out_ref,
):
    core = core_ref[0]
    on_drift, on_image = factors(own_ref, other_ref)
    own_update(core, on_drift, on_image, drift_ref, image_ref, out_ref)
    update = on_drift * drift_ref[...] + on_image * image_ref[...]
    new_ref[...] = x_ref[...] + move_size * update
    gradient(rows_ref, turned_ref, hot_ref, new_ref[:, half_of(core)], grad_ref, curve_ref)


def last_kernel(core_ref, drift_ref, image_ref, own_ref, other_ref, out_ref):
    on_drift, on_image = factors(own_ref, other_ref)
    own_update(core_ref[0], on_drift, on_image, drift_ref, image_ref, out_ref)


def similarity(x, kernel_ref):
    high, low = two(x)
    gram = tn(high, high) + (tn(high, low) + tn(low, high))
    shape = (MANY, MANY)
    same = lax.broadcasted_iota(jnp.int32, shape, 0) == lax.broadcasted_iota(jnp.int32, shape, 1)
    diag = jnp.where(same, gram, 0.0)
    squares = jnp.sum(diag, axis=1, keepdims=True) + jnp.sum(diag, axis=0, keepdims=True)
    kernel_ref[...] = jnp.exp((2.0 * gram - squares) / scale)


def start_kernel(core_ref, own_ref, other_ref, kernel_ref, x_ref):
    x = in_order(core_ref[0], own_ref[...], other_ref[...], 1)
    x_ref[...] = x
    similarity(x, kernel_ref)


def again_kernel(x_ref, kernel_ref):
    similarity(x_ref[...], kernel_ref)


def first_kernel(
    core_ref, rows_ref, turned_ref, hot_ref, x_ref, kernel_ref, own_ref, other_ref, curve_ref,
    drift_ref, image_ref, factor_ref, weighted_ref,
):
    core = core_ref[0]
    mine = half_of(core)
    x = x_ref[...]
    grad = in_order(core, own_ref[...], other_ref[...], 1)
    drift = stacked(two(grad), two(kernel_ref[...]))
    total = jnp.sum(kernel_ref[...], axis=0, keepdims=True)
    drift = (drift + (2.0 / scale) * total * x) / MANY
    drift_ref[...] = drift
    drift_two = two(drift)
    kernel_own = kernel_ref[mine, :]
    square = kernel_own * kernel_own
    square_two = jnp.concatenate(two(square), axis=0)
    for at in range(0, HALF * DATA, CHUNK):
        part = pl.ds(at, CHUNK)
        curve = curve_ref[part, :]
        factor = nn(hot_ref[part, :], square_two) * jnp.concatenate([curve, curve], axis=1)
        factor_ref[part, :] = factor
        rows = rows_ref[part, :]
        high, low = two((nn(rows, drift_two[0]) + nn(rows, drift_two[1])) * factor)
        weighted_ref[0, part, :] = high
        weighted_ref[1, part, :] = low
    x_own = x_ref[:, mine]
    x_two = two(x_own)
    along = stacked(two(x_own.T), drift_two)
    q = square * (jnp.sum(x * drift, axis=0, keepdims=True) - along)
    pull = x * jnp.sum(q, axis=0, keepdims=True) - stacked(x_two, two(q))
    turned = turned_ref[...]
    image_ref[...] = (
        (nn(turned, weighted_ref[0]) + nn(turned, weighted_ref[1]))
        + (prior_precision * jnp.sum(square, axis=0, keepdims=True) * drift + cross * pull)
    ) / MANY


def second_kernel(
    core_ref, rows_ref, x_ref, kernel_ref, factor_ref, drift_ref, own_ref, other_ref,
    image_ref, sums_ref,
):
    mine = half_of(core_ref[0])
    image = own_ref[...] + other_ref[...]
    image_ref[...] = image
    drift = drift_ref[...]
    image_two = two(image)
    total = jnp.zeros((1, MANY), f32)
    for at in range(0, HALF * DATA, CHUNK):
        part = pl.ds(at, CHUNK)
        rows = rows_ref[part, :]
        projected = nn(rows, image_two[0]) + nn(rows, image_two[1])
        total += jnp.sum(projected * projected * factor_ref[part, :], axis=0, keepdims=True)
    square = kernel_ref[mine, :] * kernel_ref[mine, :]
    along = stacked(two(x_ref[:, mine].T), image_two)
    gap = jnp.sum(x_ref[...] * image, axis=0, keepdims=True) - along
    total += cross * jnp.sum(square * gap * gap, axis=0, keepdims=True)
    length = jnp.sum(image * image, axis=0, keepdims=True)
    total += prior_precision * jnp.sum(square, axis=0, keepdims=True) * length
    figures = (
        jnp.sum(drift * drift, axis=0, keepdims=True),
        jnp.sum(drift * image, axis=0, keepdims=True),
        length,
        total / MANY,
    )
    for at, value in enumerate(figures):
        sums_ref[at : at + 1, :] = jnp.broadcast_to(
            jnp.sum(value, axis=1, keepdims=True), (1, HALF)
        )
    sums_ref[4:, :] = jnp.zeros((4, HALF), f32)


def call(kernel, outs, *args, scratch=()):
    whole = pl.BlockSpec(memory_space=pltpu.VMEM)
    specs = [pl.BlockSpec(memory_space=pltpu.SMEM) if a.size == 1 else whole for a in args]
    return pl.pallas_call(
        kernel,
        out_shape=[jax.ShapeDtypeStruct(s, t) for s, t in outs],
        in_specs=specs,
        out_specs=[whole] * len(outs),
        scratch_shapes=scratch,
        compiler_params=pltpu.CompilerParams(vmem_limit_bytes=VMEM_LIMIT),
    )(*args)


def per_device(particles, data_rows, labels):
    core = lax.axis_index("c").astype(jnp.int32)[None]
    sign = (2 * labels - 1).astype(bf16)
    rows = (data_rows * sign[:, :, None]).reshape(8 * DATA, SLICE)
    rounded = lax.reduce_precision(particles, 8, 7)
    high, low = rounded.astype(bf16), (particles - rounded).astype(bf16)
    pieces = gathered(jnp.concatenate([rows, high, low], axis=0))
    count = HALF * DATA
    rows, turned, hot, x_own = call(
        assemble_kernel,
        [((count, WIDE), bf16), ((WIDE, count), bf16), ((count, MANY), bf16), ((WIDE, HALF), f32)],
        core, *pieces,
    )
    grad_outs = [((WIDE, HALF), f32), ((count, HALF), f32)]
    square = ((MANY, MANY), f32)
    long = ((WIDE, MANY), f32)
    out = ((8, SLICE), f32)
    outputs = []
    for newton_step in range(NEWTON):
        if newton_step == 0:
            x_other = swap_cores(x_own)
            grad, curve = call(grad_kernel, grad_outs, rows, turned, hot, x_own)
            grad_other = swap_cores(grad)
            kernel, x = call(start_kernel, [square, long], core, x_own, x_other)
        else:
            grad, curve, x, update = call(
                next_kernel, grad_outs + [long, out],
                core, rows, turned, hot, x, drift, image, sums, sums_other,
            )
            outputs.append(update)
            grad_other = swap_cores(grad)
            (kernel,) = call(again_kernel, [square], x)
        drift, image_own, factor = call(
            first_kernel,
            [long, long, ((count, MANY), f32)],
            core, rows, turned, hot, x, kernel, grad, grad_other, curve,
            scratch=[pltpu.VMEM((2, count, MANY), bf16)],
        )
        image, sums = call(
            second_kernel,
            [long, ((8, HALF), f32)],
            core, rows, x, kernel, factor, drift, image_own, swap_cores(image_own),
        )
        sums_other = swap_cores(sums)
    outputs += call(last_kernel, [out], core, drift, image, sums, sums_other)
    return jnp.stack(outputs)


def solution(mesh):
    torus = Mesh(mesh.devices.reshape(4, 4, 2, mesh.shape["dim"]), AXES)
    groups = ("y", "x", "c")
    in_specs = (P(groups, "z"), P(groups, None, "z"), P(groups, None))
    out_specs = P(None, groups, "z")
    return jax.shard_map(
        per_device, mesh=torus, in_specs=in_specs, out_specs=out_specs, check_vma=False
    )
```

```python
from functools import partial

import jax
import jax.numpy as jnp
import numpy as np
from jax import lax
from jax.experimental import pallas as pl
from jax.experimental.pallas import tpu as pltpu
from jax.sharding import Mesh
from jax.sharding import PartitionSpec as P


AXES = ("y", "x", "c", "z")
NEWTON = 2
prior_precision = 0.05
like_weight = 4.0
move_size = 0.5

f32 = jnp.float32
bf16 = jnp.bfloat16
WIDE = 1024
MANY = 256
HALF = 128
DATA = 16
SLICE = 256
scale = 1.0 * WIDE
cross = 4.0 / (scale * scale)

MASKS = (1, 3)
ORDERS = ("xyz", "yzx", "zxy")
SPOT = {"y": 0, "x": 1, "z": 3}
ROWS = (768, 768, 512)
STARTS = (0, 768, 1536)
CHUNK = 512
VMEM_LIMIT = 24 * 1024 * 1024


def places():
    return np.ndindex(4, 4, 2, 4)


def spot(at):
    return int(np.ravel_multi_index(at, (4, 4, 2, 4)))


def pairs(axis):
    out = []
    for at in places():
        to = list(at)
        to[SPOT[axis]] ^= MASKS[1 - at[2]]
        out.append((spot(at), spot(to)))
    return out


def cubes():
    groups = {}
    for at in places():
        mask = MASKS[at[2]]
        key = (at[2],) + tuple(min(at[d], at[d] ^ mask) for d in (0, 1, 3))
        groups.setdefault(key, []).append(spot(at))
    return list(groups.values())


def swap_cores(x):
    return lax.ppermute(x, "c", [(0, 1), (1, 0)])


def gathered(copies):
    cube = lax.all_to_all(copies, AXES, 0, 0, axis_index_groups=cubes(), tiled=True)
    parts = [cube[:, 48 * k : 48 * k + 48] for k in range(3)]
    for step in range(3):
        came = [lax.ppermute(p, AXES, pairs(o[step])) for p, o in zip(parts, ORDERS)]
        if step < 2:
            parts = [jnp.concatenate(both, axis=0) for both in zip(parts, came)]
    return [a for both in zip(parts, came) for a in both]


def two(v):
    high = v.astype(bf16)
    return high, (v - high.astype(f32)).astype(bf16)


def nn(a, b):
    return lax.dot_general(a, b, (((1,), (0,)), ((), ())), preferred_element_type=f32)


def tn(a, b):
    return lax.dot_general(a, b, (((0,), (0,)), ((), ())), preferred_element_type=f32)


def stacked(a, b):
    left = jnp.concatenate([a[0], a[1], a[0]], axis=1)
    right = jnp.concatenate([b[0], b[0], b[1]], axis=0)
    return nn(left, right)


def slice_at(info_ref, k):
    core, z = info_ref[0], info_ref[1]
    seen = (0, 3, 1, 2)
    turned = (z ^ (z >> 1)) & 1
    return jnp.where(core == 0, k ^ (z & 2), jnp.where(turned == 1, seen[k ^ 2], seen[k]))


def cols(k):
    return slice(k * SLICE, (k + 1) * SLICE)


def span(color):
    return slice(STARTS[color], STARTS[color] + ROWS[color])


def half_of(core):
    return pl.ds(pl.multiple_of(core * HALF, HALF), HALF)


def in_order(core, own, other, axis):
    pair = jnp.where(core == 0, own, other), jnp.where(core == 0, other, own)
    return jnp.concatenate(pair, axis=axis)


def prepare_kernel(x_ref, rows_ref, labels_ref, out_ref):
    sign = (2 * labels_ref[...] - 1).astype(f32).T
    pieces = [rows_ref[p].astype(f32) * sign[:, p : p + 1] for p in range(8)]
    whole = jnp.concatenate([p.astype(bf16) for p in pieces] + list(two(x_ref[...])), axis=0)
    for k in range(8):
        out_ref[k] = whole


def assemble_kernel(info_ref, a0, b0, a1, b1, a2, b2, rows_ref, turned_ref, hot_ref, x_ref, tail_ref):
    refs = ((a0, b0), (a1, b1), (a2, b2))
    for k in range(4):
        first = pl.multiple_of(slice_at(info_ref, k) * SLICE, SLICE)
        for color in range(3):
            count = ROWS[color] // 16
            for at in range(16):
                step = {"z": k >> 1, "y": at >> 3, "x": (at >> 1) & 1}
                order = ORDERS[color]
                unit = step[order[1]] * 16 + step[order[0]] * 8
                unit += ((at >> 2) & 1) * 4 + (at & 1) * 2 + (k & 1)
                ref = refs[color][step[order[2]]]
                start = STARTS[color] + at * count
                rows_ref[start : start + count, pl.ds(first, SLICE)] = ref[unit, :count, :]
                if color == 2:
                    high, low = ref[unit, 32:40, :], ref[unit, 40:48, :]
                    tail_ref[at * 8 : at * 8 + 8, pl.ds(first, SLICE)] = high.astype(
                        f32
                    ) + low.astype(f32)
    for k in range(4):
        for color in range(3):
            turned_ref[cols(k), span(color)] = rows_ref[span(color), cols(k)].T
        x_ref[cols(k), :] = tail_ref[:, cols(k)].T
    for color, first in enumerate((0, 3, 6)):
        count = ROWS[color]
        row = lax.broadcasted_iota(jnp.int32, (count, HALF), 0)
        place = (row * 43691) >> 21 if color < 2 else row >> 5
        owner = place * 8 + first + ((row - place * (count // 16)) >> 4)
        hot = owner == lax.broadcasted_iota(jnp.int32, (count, HALF), 1)
        hot = jnp.where(hot, 1.0, 0.0).astype(bf16)
        hot_ref[span(color), :HALF] = hot
        hot_ref[span(color), HALF:] = hot


def gradient(rows_ref, turned_ref, hot_ref, x, grad_ref, curve_ref):
    both = jnp.concatenate(two(x), axis=1)
    weights = []
    for at in range(0, HALF * DATA, CHUNK):
        part = pl.ds(at, CHUNK)
        logit = nn(rows_ref[part, :], both)
        hot = hot_ref[part, :HALF].astype(f32)
        logit = jnp.sum((logit[:, :HALF] + logit[:, HALF:]) * hot, axis=1, keepdims=True)
        prob = 1.0 / (1.0 + jnp.exp(logit))
        curve_ref[part, :] = jnp.broadcast_to(like_weight * prob * (1.0 - prob), (CHUNK, HALF))
        weights.append(jnp.concatenate(two(like_weight * prob * hot), axis=1))
    total = nn(turned_ref[...], jnp.concatenate(weights, axis=0))
    grad_ref[...] = total[:, :HALF] + total[:, HALF:] - (prior_precision + 2.0 / scale) * x


def grad_kernel(rows_ref, turned_ref, hot_ref, x_ref, grad_ref, curve_ref):
    gradient(rows_ref, turned_ref, hot_ref, x_ref[...], grad_ref, curve_ref)


def factors(own_ref, other_ref):
    mu0, mu1, mu2 = (own_ref[k : k + 1, :1] for k in range(3))
    mu3 = own_ref[3:4, :1] + other_ref[3:4, :1]
    alpha = mu0 / mu1
    left = mu0 - 2.0 * alpha * mu1 + alpha * alpha * mu2
    grown = 1.0 + left / mu0
    gamma = left / (grown * grown * mu1 - 2.0 * grown * alpha * mu2 + alpha * alpha * mu3)
    return alpha + gamma * grown, -gamma * alpha


def own_update(info_ref, on_drift, on_image, drift_ref, image_ref, turn_ref):
    mine = half_of(info_ref[0])
    own = pl.ds(pl.multiple_of(info_ref[1] * SLICE, SLICE), SLICE)
    turn_ref[...] = (on_drift * drift_ref[own, mine] + on_image * image_ref[own, mine]).T
    return turn_ref[pl.ds(pl.multiple_of(info_ref[2] * 8, 8), 8), :]


def next_kernel(
    info_ref, rows_ref, turned_ref, hot_ref, x_ref, drift_ref, image_ref, own_ref, other_ref,
    grad_ref, curve_ref, new_ref, out_ref, turn_ref,
):
    on_drift, on_image = factors(own_ref, other_ref)
    out_ref[...] = own_update(info_ref, on_drift, on_image, drift_ref, image_ref, turn_ref)
    update = on_drift * drift_ref[...] + on_image * image_ref[...]
    new_ref[...] = x_ref[...] + move_size * update
    mine = half_of(info_ref[0])
    gradient(rows_ref, turned_ref, hot_ref, new_ref[:, mine], grad_ref, curve_ref)


def last_kernel(
    info_ref, drift_ref, image_ref, own_ref, other_ref, before_ref, out_ref, turn_ref
):
    on_drift, on_image = factors(own_ref, other_ref)
    out_ref[0] = before_ref[...]
    out_ref[1] = own_update(info_ref, on_drift, on_image, drift_ref, image_ref, turn_ref)


def similarity(x, kernel_ref):
    high, low = two(x)
    gram = tn(high, high) + (tn(high, low) + tn(low, high))
    shape = (MANY, MANY)
    same = lax.broadcasted_iota(jnp.int32, shape, 0) == lax.broadcasted_iota(jnp.int32, shape, 1)
    diag = jnp.where(same, gram, 0.0)
    squares = jnp.sum(diag, axis=1, keepdims=True) + jnp.sum(diag, axis=0, keepdims=True)
    kernel_ref[...] = jnp.exp((2.0 * gram - squares) / scale)


def start_kernel(info_ref, own_ref, other_ref, kernel_ref, x_ref):
    x = in_order(info_ref[0], own_ref[...], other_ref[...], 1)
    x_ref[...] = x
    similarity(x, kernel_ref)


def again_kernel(x_ref, kernel_ref):
    similarity(x_ref[...], kernel_ref)


def first_kernel(
    info_ref, rows_ref, turned_ref, hot_ref, x_ref, kernel_ref, own_ref, other_ref, curve_ref,
    drift_ref, image_ref, factor_ref, weighted_ref,
):
    core = info_ref[0]
    mine = half_of(core)
    x = x_ref[...]
    grad = in_order(core, own_ref[...], other_ref[...], 1)
    drift = stacked(two(grad), two(kernel_ref[...]))
    total = jnp.sum(kernel_ref[...], axis=0, keepdims=True)
    drift = (drift + (2.0 / scale) * total * x) / MANY
    drift_ref[...] = drift
    drift_two = two(drift)
    kernel_own = kernel_ref[mine, :]
    square = kernel_own * kernel_own
    square_two = jnp.concatenate(two(square), axis=0)
    for at in range(0, HALF * DATA, CHUNK):
        part = pl.ds(at, CHUNK)
        curve = curve_ref[part, :]
        factor = nn(hot_ref[part, :], square_two) * jnp.concatenate([curve, curve], axis=1)
        factor_ref[part, :] = factor
        rows = rows_ref[part, :]
        high, low = two((nn(rows, drift_two[0]) + nn(rows, drift_two[1])) * factor)
        weighted_ref[0, part, :] = high
        weighted_ref[1, part, :] = low
    x_own = x_ref[:, mine]
    x_two = two(x_own)
    along = stacked(two(x_own.T), drift_two)
    q = square * (jnp.sum(x * drift, axis=0, keepdims=True) - along)
    pull = x * jnp.sum(q, axis=0, keepdims=True) - stacked(x_two, two(q))
    turned = turned_ref[...]
    image_ref[...] = (
        (nn(turned, weighted_ref[0]) + nn(turned, weighted_ref[1]))
        + (prior_precision * jnp.sum(square, axis=0, keepdims=True) * drift + cross * pull)
    ) / MANY


def second_kernel(
    info_ref, rows_ref, x_ref, kernel_ref, factor_ref, drift_ref, own_ref, other_ref,
    image_ref, sums_ref,
):
    mine = half_of(info_ref[0])
    image = own_ref[...] + other_ref[...]
    image_ref[...] = image
    drift = drift_ref[...]
    image_two = two(image)
    total = jnp.zeros((1, MANY), f32)
    for at in range(0, HALF * DATA, CHUNK):
        part = pl.ds(at, CHUNK)
        rows = rows_ref[part, :]
        projected = nn(rows, image_two[0]) + nn(rows, image_two[1])
        total += jnp.sum(projected * projected * factor_ref[part, :], axis=0, keepdims=True)
    square = kernel_ref[mine, :] * kernel_ref[mine, :]
    along = stacked(two(x_ref[:, mine].T), image_two)
    gap = jnp.sum(x_ref[...] * image, axis=0, keepdims=True) - along
    total += cross * jnp.sum(square * gap * gap, axis=0, keepdims=True)
    length = jnp.sum(image * image, axis=0, keepdims=True)
    total += prior_precision * jnp.sum(square, axis=0, keepdims=True) * length
    figures = (
        jnp.sum(drift * drift, axis=0, keepdims=True),
        jnp.sum(drift * image, axis=0, keepdims=True),
        length,
        total / MANY,
    )
    for at, value in enumerate(figures):
        sums_ref[at : at + 1, :] = jnp.broadcast_to(
            jnp.sum(value, axis=1, keepdims=True), (1, HALF)
        )
    sums_ref[4:, :] = jnp.zeros((4, HALF), f32)


def call(kernel, outs, *args, scratch=()):
    whole = pl.BlockSpec(memory_space=pltpu.VMEM)
    specs = [pl.BlockSpec(memory_space=pltpu.SMEM) if a.size == 3 else whole for a in args]
    return pl.pallas_call(
        kernel,
        out_shape=[jax.ShapeDtypeStruct(s, t) for s, t in outs],
        in_specs=specs,
        out_specs=[whole] * len(outs),
        scratch_shapes=scratch,
        compiler_params=pltpu.CompilerParams(vmem_limit_bytes=VMEM_LIMIT),
    )(*args)


def own_place(core, u):
    return jnp.where(core == 0, u & 1, u >> 1)


def per_device(particles, data_rows, labels):
    core, z, y, x = (lax.axis_index(a).astype(jnp.int32) for a in ("c", "z", "y", "x"))
    info = jnp.stack([core, z, own_place(core, y) * 4 + own_place(core, x)])
    (copies,) = call(
        prepare_kernel, [((8, 8 * DATA + 16, SLICE), bf16)], particles, data_rows, labels
    )
    count = HALF * DATA
    rows, turned, hot, x_own = call(
        assemble_kernel,
        [((count, WIDE), bf16), ((WIDE, count), bf16), ((count, MANY), bf16), ((WIDE, HALF), f32)],
        info, *gathered(copies), scratch=[pltpu.VMEM((HALF, WIDE), f32)],
    )
    grad_outs = [((WIDE, HALF), f32), ((count, HALF), f32)]
    square = ((MANY, MANY), f32)
    long = ((WIDE, MANY), f32)
    out = ((8, SLICE), f32)
    turn = [pltpu.VMEM((HALF, SLICE), f32)]
    for newton_step in range(NEWTON):
        if newton_step == 0:
            x_other = swap_cores(x_own)
            grad, curve = call(grad_kernel, grad_outs, rows, turned, hot, x_own)
            grad_other = swap_cores(grad)
            kernel, x = call(start_kernel, [square, long], info, x_own, x_other)
        else:
            grad, curve, x, update = call(
                next_kernel, grad_outs + [long, out],
                info, rows, turned, hot, x, drift, image, sums, sums_other, scratch=turn,
            )
            grad_other = swap_cores(grad)
            (kernel,) = call(again_kernel, [square], x)
        drift, image_own, factor = call(
            first_kernel,
            [long, long, ((count, MANY), f32)],
            info, rows, turned, hot, x, kernel, grad, grad_other, curve,
            scratch=[pltpu.VMEM((2, count, MANY), bf16)],
        )
        image, sums = call(
            second_kernel,
            [long, ((8, HALF), f32)],
            info, rows, x, kernel, factor, drift, image_own, swap_cores(image_own),
        )
        sums_other = swap_cores(sums)
    (updates,) = call(
        last_kernel, [((NEWTON, 8, SLICE), f32)],
        info, drift, image, sums, sums_other, update, scratch=turn,
    )
    return updates


def solution(mesh):
    torus = Mesh(mesh.devices.reshape(4, 4, 2, mesh.shape["dim"]), AXES)
    groups = ("y", "x", "c")
    in_specs = (P(groups, "z"), P(groups, None, "z"), P(groups, None))
    out_specs = P(None, groups, "z")
    return jax.shard_map(
        per_device, mesh=torus, in_specs=in_specs, out_specs=out_specs, check_vma=False
    )
```

```python
from functools import partial

import jax
import jax.numpy as jnp
import numpy as np
from jax import lax
from jax.experimental import pallas as pl
from jax.experimental.pallas import tpu as pltpu
from jax.sharding import Mesh
from jax.sharding import PartitionSpec as P


AXES = ("y", "x", "c", "z")
NEWTON = 2
prior_precision = 0.05
like_weight = 4.0
move_size = 0.5

f32 = jnp.float32
bf16 = jnp.bfloat16
WIDE = 1024
MANY = 256
HALF = 128
DATA = 16
SLICE = 256
scale = 1.0 * WIDE
cross = 4.0 / (scale * scale)

MASKS = (1, 3)
ORDERS = ("xyz", "yzx", "zxy")
SPOT = {"y": 0, "x": 1, "z": 3}
ROWS = (768, 768, 512)
STARTS = (0, 768, 1536)
CHUNK = 512
VMEM_LIMIT = 24 * 1024 * 1024


def places():
    return np.ndindex(4, 4, 2, 4)


def spot(at):
    return int(np.ravel_multi_index(at, (4, 4, 2, 4)))


def pairs(axis):
    out = []
    for at in places():
        to = list(at)
        to[SPOT[axis]] ^= MASKS[1 - at[2]]
        out.append((spot(at), spot(to)))
    return out


def cubes():
    groups = {}
    for at in places():
        mask = MASKS[at[2]]
        key = (at[2],) + tuple(min(at[d], at[d] ^ mask) for d in (0, 1, 3))
        groups.setdefault(key, []).append(spot(at))
    return list(groups.values())


def swap_cores(x):
    return lax.ppermute(x, "c", [(0, 1), (1, 0)])


def gathered(copies):
    cube = lax.all_to_all(copies, AXES, 0, 0, axis_index_groups=cubes(), tiled=True)
    parts = [cube[:, 48 * k : 48 * k + 48] for k in range(3)]
    for step in range(3):
        came = [lax.ppermute(p, AXES, pairs(o[step])) for p, o in zip(parts, ORDERS)]
        if step < 2:
            parts = [jnp.concatenate(both, axis=0) for both in zip(parts, came)]
    return [a for both in zip(parts, came) for a in both]


def two(v):
    high = v.astype(bf16)
    return high, (v - high.astype(f32)).astype(bf16)


def nn(a, b):
    return lax.dot_general(a, b, (((1,), (0,)), ((), ())), preferred_element_type=f32)


def tn(a, b):
    return lax.dot_general(a, b, (((0,), (0,)), ((), ())), preferred_element_type=f32)


def stacked(a, b):
    left = jnp.concatenate([a[0], a[1], a[0]], axis=1)
    right = jnp.concatenate([b[0], b[0], b[1]], axis=0)
    return nn(left, right)


def own_place():
    y, x = lax.axis_index("y"), lax.axis_index("x")
    shift = lax.axis_index("c")
    return ((y >> shift) & 1) * 4 + ((x >> shift) & 1)


def slice_at(k):
    core, z = lax.axis_index("c"), lax.axis_index("z")
    seen = (0, 3, 1, 2)
    turned = (z ^ (z >> 1)) & 1
    return jnp.where(core == 0, k ^ (z & 2), jnp.where(turned == 1, seen[k ^ 2], seen[k]))


def cols(k):
    return slice(k * SLICE, (k + 1) * SLICE)


def span(color):
    return slice(STARTS[color], STARTS[color] + ROWS[color])


def half_of(core):
    return pl.ds(pl.multiple_of(core * HALF, HALF), HALF)


def in_order(core, own, other, axis):
    pair = jnp.where(core == 0, own, other), jnp.where(core == 0, other, own)
    return jnp.concatenate(pair, axis=axis)


def prepare_kernel(x_far, rows_far, labels_far, out_ref, x_ref, rows_ref, labels_ref, done):
    copies = [
        pltpu.make_async_copy(far, near, done.at[k])
        for k, (far, near) in enumerate(
            ((x_far, x_ref), (rows_far, rows_ref), (labels_far, labels_ref))
        )
    ]
    for copy in copies:
        copy.start()
    for copy in copies:
        copy.wait()
    sign = (2 * labels_ref[...] - 1).astype(f32).T
    pieces = [rows_ref[p].astype(f32) * sign[:, p : p + 1] for p in range(8)]
    whole = jnp.concatenate([p.astype(bf16) for p in pieces] + list(two(x_ref[...])), axis=0)
    for k in range(8):
        out_ref[k] = whole


def assemble_kernel(a0, b0, a1, b1, a2, b2, rows_ref, hot_ref, x_ref, tail_ref):
    refs = ((a0, b0), (a1, b1), (a2, b2))
    for k in range(4):
        first = pl.multiple_of(slice_at(k) * SLICE, SLICE)
        for color in range(3):
            count = ROWS[color] // 16
            for at in range(16):
                step = {"z": k >> 1, "y": at >> 3, "x": (at >> 1) & 1}
                order = ORDERS[color]
                unit = step[order[1]] * 16 + step[order[0]] * 8
                unit += ((at >> 2) & 1) * 4 + (at & 1) * 2 + (k & 1)
                ref = refs[color][step[order[2]]]
                start = STARTS[color] + at * count
                rows_ref[start : start + count, pl.ds(first, SLICE)] = ref[unit, :count, :]
                if color == 2:
                    high, low = ref[unit, 32:40, :], ref[unit, 40:48, :]
                    tail_ref[at * 8 : at * 8 + 8, pl.ds(first, SLICE)] = high.astype(
                        f32
                    ) + low.astype(f32)
    for k in range(4):
        x_ref[cols(k), :] = tail_ref[:, cols(k)].T
    for color, first in enumerate((0, 3, 6)):
        count = ROWS[color]
        row = lax.broadcasted_iota(jnp.int32, (count, HALF), 0)
        place = (row * 43691) >> 21 if color < 2 else row >> 5
        owner = place * 8 + first + ((row - place * (count // 16)) >> 4)
        hot = owner == lax.broadcasted_iota(jnp.int32, (count, HALF), 1)
        hot = jnp.where(hot, 1.0, 0.0).astype(bf16)
        hot_ref[span(color), :HALF] = hot
        hot_ref[span(color), HALF:] = hot


def gradient(rows_ref, hot_ref, x, grad_ref, curve_ref):
    both = jnp.concatenate(two(x), axis=1)
    weights = []
    for at in range(0, HALF * DATA, CHUNK):
        part = pl.ds(at, CHUNK)
        logit = nn(rows_ref[part, :], both)
        hot = hot_ref[part, :HALF].astype(f32)
        logit = jnp.sum((logit[:, :HALF] + logit[:, HALF:]) * hot, axis=1, keepdims=True)
        prob = 1.0 / (1.0 + jnp.exp(logit))
        curve_ref[part, :] = jnp.broadcast_to(like_weight * prob * (1.0 - prob), (CHUNK, HALF))
        weights.append(jnp.concatenate(two(like_weight * prob * hot), axis=1))
    total = tn(rows_ref[...], jnp.concatenate(weights, axis=0))
    grad_ref[...] = total[:, :HALF] + total[:, HALF:] - (prior_precision + 2.0 / scale) * x


def grad_kernel(rows_ref, hot_ref, x_ref, grad_ref, curve_ref):
    gradient(rows_ref, hot_ref, x_ref[...], grad_ref, curve_ref)


def factors(own_ref, other_ref):
    mu0, mu1, mu2 = (own_ref[k : k + 1, :1] for k in range(3))
    mu3 = own_ref[3:4, :1] + other_ref[3:4, :1]
    alpha = mu0 / mu1
    left = mu0 - 2.0 * alpha * mu1 + alpha * alpha * mu2
    grown = 1.0 + left / mu0
    gamma = left / (grown * grown * mu1 - 2.0 * grown * alpha * mu2 + alpha * alpha * mu3)
    return alpha + gamma * grown, -gamma * alpha


def own_update(on_drift, on_image, drift_ref, image_ref, turn_ref):
    mine = half_of(lax.axis_index("c"))
    own = pl.ds(pl.multiple_of(lax.axis_index("z") * SLICE, SLICE), SLICE)
    turn_ref[...] = (on_drift * drift_ref[own, mine] + on_image * image_ref[own, mine]).T
    return turn_ref[pl.ds(pl.multiple_of(own_place() * 8, 8), 8), :]


def next_kernel(
    rows_ref, hot_ref, x_ref, drift_ref, image_ref, own_ref, other_ref,
    grad_ref, curve_ref, new_ref, out_ref, turn_ref,
):
    on_drift, on_image = factors(own_ref, other_ref)
    out_ref[...] = own_update(on_drift, on_image, drift_ref, image_ref, turn_ref)
    update = on_drift * drift_ref[...] + on_image * image_ref[...]
    new_ref[...] = x_ref[...] + move_size * update
    mine = half_of(lax.axis_index("c"))
    gradient(rows_ref, hot_ref, new_ref[:, mine], grad_ref, curve_ref)


def last_kernel(
    drift_ref, image_ref, own_ref, other_ref, before_ref, out_ref, turn_ref
):
    on_drift, on_image = factors(own_ref, other_ref)
    out_ref[0] = before_ref[...]
    out_ref[1] = own_update(on_drift, on_image, drift_ref, image_ref, turn_ref)


def similarity(x, kernel_ref):
    high, low = two(x)
    gram = tn(high, high) + (tn(high, low) + tn(low, high))
    shape = (MANY, MANY)
    same = lax.broadcasted_iota(jnp.int32, shape, 0) == lax.broadcasted_iota(jnp.int32, shape, 1)
    diag = jnp.where(same, gram, 0.0)
    squares = jnp.sum(diag, axis=1, keepdims=True) + jnp.sum(diag, axis=0, keepdims=True)
    kernel_ref[...] = jnp.exp((2.0 * gram - squares) / scale)


def start_kernel(own_ref, other_ref, kernel_ref, x_ref):
    x = in_order(lax.axis_index("c"), own_ref[...], other_ref[...], 1)
    x_ref[...] = x
    similarity(x, kernel_ref)


def again_kernel(x_ref, kernel_ref):
    similarity(x_ref[...], kernel_ref)


def first_kernel(
    rows_ref, hot_ref, x_ref, kernel_ref, own_ref, other_ref, curve_ref,
    drift_ref, image_ref, factor_ref, weighted_ref,
):
    core = lax.axis_index("c")
    mine = half_of(core)
    x = x_ref[...]
    grad = in_order(core, own_ref[...], other_ref[...], 1)
    drift = stacked(two(grad), two(kernel_ref[...]))
    total = jnp.sum(kernel_ref[...], axis=0, keepdims=True)
    drift = (drift + (2.0 / scale) * total * x) / MANY
    drift_ref[...] = drift
    drift_two = two(drift)
    kernel_own = kernel_ref[mine, :]
    square = kernel_own * kernel_own
    square_two = jnp.concatenate(two(square), axis=0)
    for at in range(0, HALF * DATA, CHUNK):
        part = pl.ds(at, CHUNK)
        curve = curve_ref[part, :]
        factor = nn(hot_ref[part, :], square_two) * jnp.concatenate([curve, curve], axis=1)
        factor_ref[part, :] = factor
        rows = rows_ref[part, :]
        high, low = two((nn(rows, drift_two[0]) + nn(rows, drift_two[1])) * factor)
        weighted_ref[0, part, :] = high
        weighted_ref[1, part, :] = low
    x_own = x_ref[:, mine]
    x_two = two(x_own)
    along = stacked(two(x_own.T), drift_two)
    q = square * (jnp.sum(x * drift, axis=0, keepdims=True) - along)
    pull = x * jnp.sum(q, axis=0, keepdims=True) - stacked(x_two, two(q))
    image_ref[...] = (
        (tn(rows_ref[...], weighted_ref[0]) + tn(rows_ref[...], weighted_ref[1]))
        + (prior_precision * jnp.sum(square, axis=0, keepdims=True) * drift + cross * pull)
    ) / MANY


def second_kernel(
    rows_ref, x_ref, kernel_ref, factor_ref, drift_ref, own_ref, other_ref,
    image_ref, sums_ref,
):
    mine = half_of(lax.axis_index("c"))
    image = own_ref[...] + other_ref[...]
    image_ref[...] = image
    drift = drift_ref[...]
    image_two = two(image)
    rounded = image_two[0]
    wide = rounded.astype(f32)
    total = jnp.zeros((1, MANY), f32)
    for at in range(0, HALF * DATA, CHUNK):
        part = pl.ds(at, CHUNK)
        rows = rows_ref[part, :]
        projected = nn(rows, rounded)
        total += jnp.sum(projected * projected * factor_ref[part, :], axis=0, keepdims=True)
    fit = jnp.sum(image * wide, axis=0, keepdims=True)
    fit = fit / jnp.maximum(jnp.sum(wide * wide, axis=0, keepdims=True), 1e-30)
    total *= fit * fit
    square = kernel_ref[mine, :] * kernel_ref[mine, :]
    along = stacked(two(x_ref[:, mine].T), image_two)
    gap = jnp.sum(x_ref[...] * image, axis=0, keepdims=True) - along
    total += cross * jnp.sum(square * gap * gap, axis=0, keepdims=True)
    length = jnp.sum(image * image, axis=0, keepdims=True)
    total += prior_precision * jnp.sum(square, axis=0, keepdims=True) * length
    figures = (
        jnp.sum(drift * drift, axis=0, keepdims=True),
        jnp.sum(drift * image, axis=0, keepdims=True),
        length,
        total / MANY,
    )
    for at, value in enumerate(figures):
        sums_ref[at : at + 1, :] = jnp.broadcast_to(
            jnp.sum(value, axis=1, keepdims=True), (1, HALF)
        )
    sums_ref[4:, :] = jnp.zeros((4, HALF), f32)


def call(kernel, outs, *args, scratch=(), far=False):
    whole = pl.BlockSpec(memory_space=pltpu.VMEM)
    return pl.pallas_call(
        kernel,
        out_shape=[jax.ShapeDtypeStruct(s, t) for s, t in outs],
        in_specs=[pl.BlockSpec(memory_space=pltpu.HBM) if far else whole] * len(args),
        out_specs=[whole] * len(outs),
        scratch_shapes=scratch,
        compiler_params=pltpu.CompilerParams(vmem_limit_bytes=VMEM_LIMIT),
    )(*args)


def per_device(particles, data_rows, labels):
    (copies,) = call(
        prepare_kernel,
        [((8, 8 * DATA + 16, SLICE), bf16)],
        particles, data_rows, labels,
        scratch=[
            pltpu.VMEM((8, SLICE), f32),
            pltpu.VMEM((8, DATA, SLICE), bf16),
            pltpu.VMEM((8, DATA), jnp.int32),
            pltpu.SemaphoreType.DMA((3,)),
        ],
        far=True,
    )
    count = HALF * DATA
    rows, hot, x_own = call(
        assemble_kernel,
        [((count, WIDE), bf16), ((count, MANY), bf16), ((WIDE, HALF), f32)],
        *gathered(copies), scratch=[pltpu.VMEM((HALF, WIDE), f32)],
    )
    grad_outs = [((WIDE, HALF), f32), ((count, HALF), f32)]
    square = ((MANY, MANY), f32)
    long = ((WIDE, MANY), f32)
    out = ((8, SLICE), f32)
    turn = [pltpu.VMEM((HALF, SLICE), f32)]
    for newton_step in range(NEWTON):
        if newton_step == 0:
            x_other = swap_cores(x_own)
            grad, curve = call(grad_kernel, grad_outs, rows, hot, x_own)
            grad_other = swap_cores(grad)
            kernel, x = call(start_kernel, [square, long], x_own, x_other)
        else:
            grad, curve, x, update = call(
                next_kernel, grad_outs + [long, out],
                rows, hot, x, drift, image, sums, sums_other, scratch=turn,
            )
            grad_other = swap_cores(grad)
            (kernel,) = call(again_kernel, [square], x)
        drift, image_own, factor = call(
            first_kernel,
            [long, long, ((count, MANY), f32)],
            rows, hot, x, kernel, grad, grad_other, curve,
            scratch=[pltpu.VMEM((2, count, MANY), bf16)],
        )
        image, sums = call(
            second_kernel,
            [long, ((8, HALF), f32)],
            rows, x, kernel, factor, drift, image_own, swap_cores(image_own),
        )
        sums_other = swap_cores(sums)
    (updates,) = call(
        last_kernel, [((NEWTON, 8, SLICE), f32)],
        drift, image, sums, sums_other, update, scratch=turn,
    )
    return updates


def solution(mesh):
    torus = Mesh(mesh.devices.reshape(4, 4, 2, mesh.shape["dim"]), AXES)
    groups = ("y", "x", "c")
    in_specs = (P(groups, "z"), P(groups, None, "z"), P(groups, None))
    out_specs = P(None, groups, "z")
    return jax.shard_map(
        per_device, mesh=torus, in_specs=in_specs, out_specs=out_specs, check_vma=False
    )
```

```python
from functools import partial

import jax
import jax.numpy as jnp
import numpy as np
from jax import lax
from jax.experimental import pallas as pl
from jax.experimental.pallas import tpu as pltpu
from jax.sharding import Mesh
from jax.sharding import PartitionSpec as P


AXES = ("y", "x", "c", "z")
NEWTON = 2
prior_precision = 0.05
like_weight = 4.0
move_size = 0.5

f32 = jnp.float32
bf16 = jnp.bfloat16
WIDE = 1024
MANY = 256
HALF = 128
DATA = 16
SLICE = 256
scale = 1.0 * WIDE
cross = 4.0 / (scale * scale)

MASKS = (1, 3)
ORDERS = ("xyz", "yzx", "zxy")
SPOT = {"y": 0, "x": 1, "z": 3}
ROWS = (768, 768, 512)
STARTS = (0, 768, 1536)
CHUNK = 512
VMEM_LIMIT = 24 * 1024 * 1024


def places():
    return np.ndindex(4, 4, 2, 4)


def spot(at):
    return int(np.ravel_multi_index(at, (4, 4, 2, 4)))


def pairs(axis):
    out = []
    for at in places():
        to = list(at)
        to[SPOT[axis]] ^= MASKS[1 - at[2]]
        out.append((spot(at), spot(to)))
    return out


def cubes():
    groups = {}
    for at in places():
        mask = MASKS[at[2]]
        key = (at[2],) + tuple(min(at[d], at[d] ^ mask) for d in (0, 1, 3))
        groups.setdefault(key, []).append(spot(at))
    return list(groups.values())


def swap_cores(x):
    return lax.ppermute(x, "c", [(0, 1), (1, 0)])


def gathered(copies):
    cube = lax.all_to_all(copies, AXES, 0, 0, axis_index_groups=cubes(), tiled=True)
    parts = [cube[:, 48 * k : 48 * k + 48] for k in range(3)]

    def sent(parts, step):
        return [lax.ppermute(p, AXES, pairs(o[step])) for p, o in zip(parts, ORDERS)]

    near = [jnp.concatenate(both, axis=0) for both in zip(parts, sent(parts, 0))]
    aside = sent(near, 1)
    far = sent(near, 2)
    last = sent(aside, 2)
    return [a for four in zip(near, aside, far, last) for a in four]


def two(v):
    high = v.astype(bf16)
    return high, (v - high.astype(f32)).astype(bf16)


def nn(a, b):
    return lax.dot_general(a, b, (((1,), (0,)), ((), ())), preferred_element_type=f32)


def tn(a, b):
    return lax.dot_general(a, b, (((0,), (0,)), ((), ())), preferred_element_type=f32)


def stacked(a, b):
    left = jnp.concatenate([a[0], a[1], a[0]], axis=1)
    right = jnp.concatenate([b[0], b[0], b[1]], axis=0)
    return nn(left, right)


def own_place():
    y, x = lax.axis_index("y"), lax.axis_index("x")
    shift = lax.axis_index("c")
    return ((y >> shift) & 1) * 4 + ((x >> shift) & 1)


def slice_at(k):
    core, z = lax.axis_index("c"), lax.axis_index("z")
    seen = (0, 3, 1, 2)
    turned = (z ^ (z >> 1)) & 1
    return jnp.where(core == 0, k ^ (z & 2), jnp.where(turned == 1, seen[k ^ 2], seen[k]))


def cols(k):
    return slice(k * SLICE, (k + 1) * SLICE)


def span(color):
    return slice(STARTS[color], STARTS[color] + ROWS[color])


def half_of(core):
    return pl.ds(pl.multiple_of(core * HALF, HALF), HALF)


def in_order(core, own, other, axis):
    pair = jnp.where(core == 0, own, other), jnp.where(core == 0, other, own)
    return jnp.concatenate(pair, axis=axis)


def prepare_kernel(x_far, rows_far, labels_far, out_ref, x_ref, rows_ref, labels_ref, done):
    copies = [
        pltpu.make_async_copy(far, near, done.at[k])
        for k, (far, near) in enumerate(
            ((x_far, x_ref), (rows_far, rows_ref), (labels_far, labels_ref))
        )
    ]
    for copy in copies:
        copy.start()
    for copy in copies:
        copy.wait()
    sign = (2 * labels_ref[...] - 1).astype(f32).T
    pieces = [rows_ref[p].astype(f32) * sign[:, p : p + 1] for p in range(8)]
    whole = jnp.concatenate([p.astype(bf16) for p in pieces] + list(two(x_ref[...])), axis=0)
    for k in range(8):
        out_ref[k] = whole


def assemble_kernel(*refs):
    rows_ref, hot_ref, x_ref, tail_ref = refs[12:]
    for k in range(4):
        first = pl.multiple_of(slice_at(k) * SLICE, SLICE)
        for color in range(3):
            count = ROWS[color] // 16
            for at in range(16):
                step = {"z": k >> 1, "y": at >> 3, "x": (at >> 1) & 1}
                order = ORDERS[color]
                unit = step[order[0]] * 8 + ((at >> 2) & 1) * 4 + (at & 1) * 2 + (k & 1)
                ref = refs[color * 4 + step[order[2]] * 2 + step[order[1]]]
                start = STARTS[color] + at * count
                rows_ref[start : start + count, pl.ds(first, SLICE)] = ref[unit, :count, :]
                if color == 2:
                    high, low = ref[unit, 32:40, :], ref[unit, 40:48, :]
                    tail_ref[at * 8 : at * 8 + 8, pl.ds(first, SLICE)] = high.astype(
                        f32
                    ) + low.astype(f32)
    for k in range(4):
        x_ref[cols(k), :] = tail_ref[:, cols(k)].T
    for color, first in enumerate((0, 3, 6)):
        count = ROWS[color]
        row = lax.broadcasted_iota(jnp.int32, (count, HALF), 0)
        place = (row * 43691) >> 21 if color < 2 else row >> 5
        owner = place * 8 + first + ((row - place * (count // 16)) >> 4)
        hot = owner == lax.broadcasted_iota(jnp.int32, (count, HALF), 1)
        hot = jnp.where(hot, 1.0, 0.0).astype(bf16)
        hot_ref[span(color), :HALF] = hot
        hot_ref[span(color), HALF:] = hot


def gradient(rows_ref, hot_ref, x, grad_ref, curve_ref):
    both = jnp.concatenate(two(x), axis=1)
    weights = []
    for at in range(0, HALF * DATA, CHUNK):
        part = pl.ds(at, CHUNK)
        logit = nn(rows_ref[part, :], both)
        hot = hot_ref[part, :HALF].astype(f32)
        logit = jnp.sum((logit[:, :HALF] + logit[:, HALF:]) * hot, axis=1, keepdims=True)
        prob = 1.0 / (1.0 + jnp.exp(logit))
        curve_ref[part, :] = jnp.broadcast_to(like_weight * prob * (1.0 - prob), (CHUNK, HALF))
        weights.append(jnp.concatenate(two(like_weight * prob * hot), axis=1))
    total = tn(rows_ref[...], jnp.concatenate(weights, axis=0))
    grad_ref[...] = total[:, :HALF] + total[:, HALF:] - (prior_precision + 2.0 / scale) * x


def grad_kernel(rows_ref, hot_ref, x_ref, grad_ref, curve_ref):
    gradient(rows_ref, hot_ref, x_ref[...], grad_ref, curve_ref)


def factors(own_ref, other_ref):
    mu0, mu1, mu2 = (own_ref[k : k + 1, :1] for k in range(3))
    mu3 = own_ref[3:4, :1] + other_ref[3:4, :1]
    alpha = mu0 / mu1
    left = mu0 - 2.0 * alpha * mu1 + alpha * alpha * mu2
    grown = 1.0 + left / mu0
    gamma = left / (grown * grown * mu1 - 2.0 * grown * alpha * mu2 + alpha * alpha * mu3)
    return alpha + gamma * grown, -gamma * alpha


def own_update(on_drift, on_image, drift_ref, image_ref, turn_ref):
    mine = half_of(lax.axis_index("c"))
    own = pl.ds(pl.multiple_of(lax.axis_index("z") * SLICE, SLICE), SLICE)
    turn_ref[...] = (on_drift * drift_ref[own, mine] + on_image * image_ref[own, mine]).T
    return turn_ref[pl.ds(pl.multiple_of(own_place() * 8, 8), 8), :]


def next_kernel(
    rows_ref, hot_ref, x_ref, drift_ref, image_ref, own_ref, other_ref,
    grad_ref, curve_ref, new_ref, out_ref, turn_ref,
):
    on_drift, on_image = factors(own_ref, other_ref)
    out_ref[...] = own_update(on_drift, on_image, drift_ref, image_ref, turn_ref)
    update = on_drift * drift_ref[...] + on_image * image_ref[...]
    new_ref[...] = x_ref[...] + move_size * update
    mine = half_of(lax.axis_index("c"))
    gradient(rows_ref, hot_ref, new_ref[:, mine], grad_ref, curve_ref)


def last_kernel(
    drift_ref, image_ref, own_ref, other_ref, before_ref, out_ref, turn_ref
):
    on_drift, on_image = factors(own_ref, other_ref)
    out_ref[0] = before_ref[...]
    out_ref[1] = own_update(on_drift, on_image, drift_ref, image_ref, turn_ref)


def similarity(x, kernel_ref):
    high, low = two(x)
    gram = tn(high, high) + (tn(high, low) + tn(low, high))
    shape = (MANY, MANY)
    same = lax.broadcasted_iota(jnp.int32, shape, 0) == lax.broadcasted_iota(jnp.int32, shape, 1)
    diag = jnp.where(same, gram, 0.0)
    squares = jnp.sum(diag, axis=1, keepdims=True) + jnp.sum(diag, axis=0, keepdims=True)
    kernel_ref[...] = jnp.exp((2.0 * gram - squares) / scale)


def start_kernel(own_ref, other_ref, kernel_ref, x_ref):
    x = in_order(lax.axis_index("c"), own_ref[...], other_ref[...], 1)
    x_ref[...] = x
    similarity(x, kernel_ref)


def again_kernel(x_ref, kernel_ref):
    similarity(x_ref[...], kernel_ref)


def first_kernel(
    rows_ref, hot_ref, x_ref, kernel_ref, own_ref, other_ref, curve_ref,
    drift_ref, image_ref, factor_ref, weighted_ref,
):
    core = lax.axis_index("c")
    mine = half_of(core)
    x = x_ref[...]
    grad = in_order(core, own_ref[...], other_ref[...], 1)
    drift = stacked(two(grad), two(kernel_ref[...]))
    total = jnp.sum(kernel_ref[...], axis=0, keepdims=True)
    drift = (drift + (2.0 / scale) * total * x) / MANY
    drift_ref[...] = drift
    drift_two = two(drift)
    kernel_own = kernel_ref[mine, :]
    square = kernel_own * kernel_own
    square_two = jnp.concatenate(two(square), axis=0)
    for at in range(0, HALF * DATA, CHUNK):
        part = pl.ds(at, CHUNK)
        curve = curve_ref[part, :]
        factor = nn(hot_ref[part, :], square_two) * jnp.concatenate([curve, curve], axis=1)
        factor_ref[part, :] = factor
        rows = rows_ref[part, :]
        high, low = two((nn(rows, drift_two[0]) + nn(rows, drift_two[1])) * factor)
        weighted_ref[0, part, :] = high
        weighted_ref[1, part, :] = low
    x_own = x_ref[:, mine]
    x_two = two(x_own)
    along = stacked(two(x_own.T), drift_two)
    q = square * (jnp.sum(x * drift, axis=0, keepdims=True) - along)
    pull = x * jnp.sum(q, axis=0, keepdims=True) - stacked(x_two, two(q))
    image_ref[...] = (
        (tn(rows_ref[...], weighted_ref[0]) + tn(rows_ref[...], weighted_ref[1]))
        + (prior_precision * jnp.sum(square, axis=0, keepdims=True) * drift + cross * pull)
    ) / MANY


def second_kernel(
    rows_ref, x_ref, kernel_ref, factor_ref, drift_ref, own_ref, other_ref,
    image_ref, sums_ref,
):
    mine = half_of(lax.axis_index("c"))
    image = own_ref[...] + other_ref[...]
    image_ref[...] = image
    drift = drift_ref[...]
    image_two = two(image)
    rounded = image_two[0]
    wide = rounded.astype(f32)
    total = jnp.zeros((1, MANY), f32)
    for at in range(0, HALF * DATA, CHUNK):
        part = pl.ds(at, CHUNK)
        rows = rows_ref[part, :]
        projected = nn(rows, rounded)
        total += jnp.sum(projected * projected * factor_ref[part, :], axis=0, keepdims=True)
    fit = jnp.sum(image * wide, axis=0, keepdims=True)
    fit = fit / jnp.maximum(jnp.sum(wide * wide, axis=0, keepdims=True), 1e-30)
    total *= fit * fit
    square = kernel_ref[mine, :] * kernel_ref[mine, :]
    along = stacked(two(x_ref[:, mine].T), image_two)
    gap = jnp.sum(x_ref[...] * image, axis=0, keepdims=True) - along
    total += cross * jnp.sum(square * gap * gap, axis=0, keepdims=True)
    length = jnp.sum(image * image, axis=0, keepdims=True)
    total += prior_precision * jnp.sum(square, axis=0, keepdims=True) * length
    figures = (
        jnp.sum(drift * drift, axis=0, keepdims=True),
        jnp.sum(drift * image, axis=0, keepdims=True),
        length,
        total / MANY,
    )
    for at, value in enumerate(figures):
        sums_ref[at : at + 1, :] = jnp.broadcast_to(
            jnp.sum(value, axis=1, keepdims=True), (1, HALF)
        )
    sums_ref[4:, :] = jnp.zeros((4, HALF), f32)


def call(kernel, outs, *args, scratch=(), far=False):
    whole = pl.BlockSpec(memory_space=pltpu.VMEM)
    return pl.pallas_call(
        kernel,
        out_shape=[jax.ShapeDtypeStruct(s, t) for s, t in outs],
        in_specs=[pl.BlockSpec(memory_space=pltpu.HBM) if far else whole] * len(args),
        out_specs=[whole] * len(outs),
        scratch_shapes=scratch,
        compiler_params=pltpu.CompilerParams(vmem_limit_bytes=VMEM_LIMIT),
    )(*args)


def per_device(particles, data_rows, labels):
    (copies,) = call(
        prepare_kernel,
        [((8, 8 * DATA + 16, SLICE), bf16)],
        particles, data_rows, labels,
        scratch=[
            pltpu.VMEM((8, SLICE), f32),
            pltpu.VMEM((8, DATA, SLICE), bf16),
            pltpu.VMEM((8, DATA), jnp.int32),
            pltpu.SemaphoreType.DMA((3,)),
        ],
        far=True,
    )
    count = HALF * DATA
    rows, hot, x_own = call(
        assemble_kernel,
        [((count, WIDE), bf16), ((count, MANY), bf16), ((WIDE, HALF), f32)],
        *gathered(copies), scratch=[pltpu.VMEM((HALF, WIDE), f32)],
    )
    grad_outs = [((WIDE, HALF), f32), ((count, HALF), f32)]
    square = ((MANY, MANY), f32)
    long = ((WIDE, MANY), f32)
    out = ((8, SLICE), f32)
    turn = [pltpu.VMEM((HALF, SLICE), f32)]
    for newton_step in range(NEWTON):
        if newton_step == 0:
            x_other = swap_cores(x_own)
            grad, curve = call(grad_kernel, grad_outs, rows, hot, x_own)
            grad_other = swap_cores(grad)
            kernel, x = call(start_kernel, [square, long], x_own, x_other)
        else:
            grad, curve, x, update = call(
                next_kernel, grad_outs + [long, out],
                rows, hot, x, drift, image, sums, sums_other, scratch=turn,
            )
            grad_other = swap_cores(grad)
            (kernel,) = call(again_kernel, [square], x)
        drift, image_own, factor = call(
            first_kernel,
            [long, long, ((count, MANY), f32)],
            rows, hot, x, kernel, grad, grad_other, curve,
            scratch=[pltpu.VMEM((2, count, MANY), bf16)],
        )
        image, sums = call(
            second_kernel,
            [long, ((8, HALF), f32)],
            rows, x, kernel, factor, drift, image_own, swap_cores(image_own),
        )
        sums_other = swap_cores(sums)
    (updates,) = call(
        last_kernel, [((NEWTON, 8, SLICE), f32)],
        drift, image, sums, sums_other, update, scratch=turn,
    )
    return updates


def solution(mesh):
    torus = Mesh(mesh.devices.reshape(4, 4, 2, mesh.shape["dim"]), AXES)
    groups = ("y", "x", "c")
    in_specs = (P(groups, "z"), P(groups, None, "z"), P(groups, None))
    out_specs = P(None, groups, "z")
    return jax.shard_map(
        per_device, mesh=torus, in_specs=in_specs, out_specs=out_specs, check_vma=False
    )
```

```python
from functools import partial

import jax
import jax.numpy as jnp
import numpy as np
from jax import lax
from jax.experimental import pallas as pl
from jax.experimental.pallas import tpu as pltpu
from jax.sharding import Mesh
from jax.sharding import PartitionSpec as P


AXES = ("y", "x", "c", "z")
NEWTON = 2
prior_precision = 0.05
like_weight = 4.0
move_size = 0.5

f32 = jnp.float32
bf16 = jnp.bfloat16
WIDE = 1024
MANY = 256
HALF = 128
DATA = 16
SLICE = 256
scale = 1.0 * WIDE
cross = 4.0 / (scale * scale)

MASKS = (1, 3)
ORDERS = ("xyz", "yzx", "zxy")
SPOT = {"y": 0, "x": 1, "z": 3}
THIRDS = (96, 0, 48)
FIRSTS = (6, 0, 3)
ROWS = (512, 768, 768)
STARTS = (0, 512, 1280)
CHUNK = 256


def places():
    return np.ndindex(4, 4, 2, 4)


def spot(at):
    return int(np.ravel_multi_index(at, (4, 4, 2, 4)))


def pairs(axis):
    out = []
    for at in places():
        to = list(at)
        to[SPOT[axis]] ^= MASKS[1 - at[2]]
        out.append((spot(at), spot(to)))
    return out


def cubes():
    groups = {}
    for at in places():
        mask = MASKS[at[2]]
        key = (at[2],) + tuple(min(at[d], at[d] ^ mask) for d in (0, 1, 3))
        groups.setdefault(key, []).append(spot(at))
    return list(groups.values())


def swap_cores(x):
    return lax.ppermute(x, "c", [(0, 1), (1, 0)])


def gathered(copies):
    cube = lax.all_to_all(copies, AXES, 0, 0, axis_index_groups=cubes(), tiled=True)
    parts = [cube[:, k : k + 48] for k in THIRDS]

    def sent(parts, step):
        out = []
        for part, order in zip(parts, ORDERS):
            out.append(lax.ppermute(part, AXES, pairs(order[step])))
        return out

    near = [jnp.concatenate(both, axis=0) for both in zip(parts, sent(parts, 0))]
    aside = sent(near, 1)
    far = sent(near, 2)
    last = sent(aside, 2)
    return list(zip(near, aside, far, last))


def two(v):
    high = v.astype(bf16)
    return high, (v - high.astype(f32)).astype(bf16)


def nn(a, b):
    return lax.dot_general(a, b, (((1,), (0,)), ((), ())), preferred_element_type=f32)


def tn(a, b):
    return lax.dot_general(a, b, (((0,), (0,)), ((), ())), preferred_element_type=f32)


def stacked(a, b):
    left = jnp.concatenate([a[0], a[1], a[0]], axis=1)
    right = jnp.concatenate([b[0], b[0], b[1]], axis=0)
    return nn(left, right)


def own_place():
    y, x = lax.axis_index("y"), lax.axis_index("x")
    shift = lax.axis_index("c")
    return ((y >> shift) & 1) * 4 + ((x >> shift) & 1)


def slice_at(k):
    core, z = lax.axis_index("c"), lax.axis_index("z")
    seen = (0, 3, 1, 2)
    turned = (z ^ (z >> 1)) & 1
    return jnp.where(core == 0, k ^ (z & 2), jnp.where(turned == 1, seen[k ^ 2], seen[k]))


def cols(k):
    return slice(k * SLICE, (k + 1) * SLICE)


def span(color):
    return slice(STARTS[color], STARTS[color] + ROWS[color])


def half_of(core):
    return pl.ds(pl.multiple_of(core * HALF, HALF), HALF)


def in_order(core, own, other, axis):
    pair = jnp.where(core == 0, own, other), jnp.where(core == 0, other, own)
    return jnp.concatenate(pair, axis=axis)


def prepare_kernel(x_far, rows_far, labels_far, out_ref, x_ref, rows_ref, labels_ref, done):
    copies = [
        pltpu.make_async_copy(far, near, done.at[k])
        for k, (far, near) in enumerate(
            ((x_far, x_ref), (rows_far, rows_ref), (labels_far, labels_ref))
        )
    ]
    for copy in copies:
        copy.start()
    for copy in copies:
        copy.wait()
    sign = (2 * labels_ref[...] - 1).astype(f32).T
    pieces = [rows_ref[p].astype(f32) * sign[:, p : p + 1] for p in range(8)]
    whole = jnp.concatenate([p.astype(bf16) for p in pieces] + list(two(x_ref[...])), axis=0)
    for k in range(8):
        out_ref[k] = whole


def land(color, refs, rows_ref, hot_ref, tail_ref=None):
    count = ROWS[color] // 16
    order = ORDERS[color]
    for k in range(4):
        slot = pl.ds(pl.multiple_of(slice_at(k) * SLICE, SLICE), SLICE)
        for at in range(16):
            step = {"z": k >> 1, "y": at >> 3, "x": (at >> 1) & 1}
            unit = step[order[0]] * 8 + ((at >> 2) & 1) * 4 + (at & 1) * 2 + (k & 1)
            ref = refs[step[order[2]] * 2 + step[order[1]]]
            rows_ref[at * count : (at + 1) * count, slot] = ref[unit, :count, :]
            if tail_ref is not None:
                high, low = ref[unit, 32:40, :], ref[unit, 40:48, :]
                tail_ref[at * 8 : at * 8 + 8, slot] = high.astype(f32) + low.astype(f32)
    row = lax.broadcasted_iota(jnp.int32, (ROWS[color], HALF), 0)
    place = (row * 43691) >> 21 if count == 48 else row >> 5
    owner = place * 8 + FIRSTS[color] + ((row - place * count) >> 4)
    hot = owner == lax.broadcasted_iota(jnp.int32, (ROWS[color], HALF), 1)
    hot = jnp.where(hot, 1.0, 0.0).astype(bf16)
    hot_ref[:, :HALF] = hot
    hot_ref[:, HALF:] = hot


def gradient(rows_ref, hot_ref, both, curve_ref):
    weights = []
    for at in range(0, rows_ref.shape[0], CHUNK):
        part = pl.ds(at, CHUNK)
        logit = nn(rows_ref[part, :], both)
        hot = hot_ref[part, :HALF].astype(f32)
        logit = jnp.sum((logit[:, :HALF] + logit[:, HALF:]) * hot, axis=1, keepdims=True)
        prob = 1.0 / (1.0 + jnp.exp(logit))
        curve_ref[part, :] = jnp.broadcast_to(like_weight * prob * (1.0 - prob), (CHUNK, HALF))
        weights.append(jnp.concatenate(two(like_weight * prob * hot), axis=1))
    return tn(rows_ref[...], jnp.concatenate(weights, axis=0))


def folded(total):
    return total[:, :HALF] + total[:, HALF:]


def land_kernel(a, b, c, d, rows_ref, hot_ref, x_ref, tail_ref):
    land(0, (a, b, c, d), rows_ref, hot_ref, tail_ref)
    for k in range(4):
        x_ref[cols(k), :] = tail_ref[:, cols(k)].T


def grad_kernel(rows_ref, hot_ref, x_ref, grad_ref, curve_ref):
    x = x_ref[...]
    both = jnp.concatenate(two(x), axis=1)
    grad_ref[...] = folded(gradient(rows_ref, hot_ref, both, curve_ref)) - (
        prior_precision + 2.0 / scale
    ) * x


def land_grad_kernel(color, a, b, c, d, x_ref, before_ref, rows_ref, hot_ref, grad_ref, curve_ref):
    land(color, (a, b, c, d), rows_ref, hot_ref)
    both = jnp.concatenate(two(x_ref[...]), axis=1)
    grad_ref[...] = before_ref[...] + folded(gradient(rows_ref, hot_ref, both, curve_ref))


def factors(own_ref, other_ref):
    mu0, mu1, mu2 = (own_ref[k : k + 1, :1] for k in range(3))
    mu3 = own_ref[3:4, :1] + other_ref[3:4, :1]
    alpha = mu0 / mu1
    left = mu0 - 2.0 * alpha * mu1 + alpha * alpha * mu2
    grown = 1.0 + left / mu0
    gamma = left / (grown * grown * mu1 - 2.0 * grown * alpha * mu2 + alpha * alpha * mu3)
    return alpha + gamma * grown, -gamma * alpha


def own_update(on_drift, on_image, drift_ref, image_ref, turn_ref):
    mine = half_of(lax.axis_index("c"))
    own = pl.ds(pl.multiple_of(lax.axis_index("z") * SLICE, SLICE), SLICE)
    turn_ref[...] = (on_drift * drift_ref[own, mine] + on_image * image_ref[own, mine]).T
    return turn_ref[pl.ds(pl.multiple_of(own_place() * 8, 8), 8), :]


def next_kernel(
    r0, r1, r2, h0, h1, h2, x_ref, drift_ref, image_ref, own_ref, other_ref,
    grad_ref, c0, c1, c2, new_ref, out_ref, turn_ref,
):
    on_drift, on_image = factors(own_ref, other_ref)
    out_ref[...] = own_update(on_drift, on_image, drift_ref, image_ref, turn_ref)
    update = on_drift * drift_ref[...] + on_image * image_ref[...]
    new_ref[...] = x_ref[...] + move_size * update
    x = new_ref[:, half_of(lax.axis_index("c"))]
    both = jnp.concatenate(two(x), axis=1)
    total = gradient(r0, h0, both, c0) + gradient(r1, h1, both, c1) + gradient(r2, h2, both, c2)
    grad_ref[...] = folded(total) - (prior_precision + 2.0 / scale) * x


def last_kernel(
    drift_ref, image_ref, own_ref, other_ref, before_ref, out_ref, turn_ref
):
    on_drift, on_image = factors(own_ref, other_ref)
    out_ref[0] = before_ref[...]
    out_ref[1] = own_update(on_drift, on_image, drift_ref, image_ref, turn_ref)


def similarity(x, kernel_ref):
    high, low = two(x)
    gram = tn(high, high) + (tn(high, low) + tn(low, high))
    shape = (MANY, MANY)
    same = lax.broadcasted_iota(jnp.int32, shape, 0) == lax.broadcasted_iota(jnp.int32, shape, 1)
    diag = jnp.where(same, gram, 0.0)
    squares = jnp.sum(diag, axis=1, keepdims=True) + jnp.sum(diag, axis=0, keepdims=True)
    kernel_ref[...] = jnp.exp((2.0 * gram - squares) / scale)


def start_kernel(own_ref, other_ref, kernel_ref, x_ref):
    x = in_order(lax.axis_index("c"), own_ref[...], other_ref[...], 1)
    x_ref[...] = x
    similarity(x, kernel_ref)


def again_kernel(x_ref, kernel_ref):
    similarity(x_ref[...], kernel_ref)


def first_kernel(
    r0, r1, r2, h0, h1, h2, c0, c1, c2, x_ref, kernel_ref, own_ref, other_ref,
    drift_ref, image_ref, factor_ref, weighted_ref,
):
    core = lax.axis_index("c")
    mine = half_of(core)
    x = x_ref[...]
    grad = in_order(core, own_ref[...], other_ref[...], 1)
    drift = stacked(two(grad), two(kernel_ref[...]))
    total = jnp.sum(kernel_ref[...], axis=0, keepdims=True)
    drift = (drift + (2.0 / scale) * total * x) / MANY
    drift_ref[...] = drift
    drift_two = two(drift)
    kernel_own = kernel_ref[mine, :]
    square = kernel_own * kernel_own
    square_two = jnp.concatenate(two(square), axis=0)
    thirds = (r0, r1, r2)
    for color, (rows_ref, hot_ref, curve_ref) in enumerate(zip(thirds, (h0, h1, h2), (c0, c1, c2))):
        for at in range(0, ROWS[color], CHUNK):
            part, to = pl.ds(at, CHUNK), pl.ds(STARTS[color] + at, CHUNK)
            curve = curve_ref[part, :]
            factor = nn(hot_ref[part, :], square_two) * jnp.concatenate([curve, curve], axis=1)
            factor_ref[to, :] = factor
            rows = rows_ref[part, :]
            high, low = two((nn(rows, drift_two[0]) + nn(rows, drift_two[1])) * factor)
            weighted_ref[0, to, :] = high
            weighted_ref[1, to, :] = low
    x_own = x_ref[:, mine]
    x_two = two(x_own)
    along = stacked(two(x_own.T), drift_two)
    q = square * (jnp.sum(x * drift, axis=0, keepdims=True) - along)
    pull = x * jnp.sum(q, axis=0, keepdims=True) - stacked(x_two, two(q))
    image_ref[...] = (
        sum(
            tn(rows_ref[...], weighted_ref[k, span(color), :])
            for color, rows_ref in enumerate(thirds)
            for k in range(2)
        )
        + (prior_precision * jnp.sum(square, axis=0, keepdims=True) * drift + cross * pull)
    ) / MANY


def second_kernel(
    r0, r1, r2, x_ref, kernel_ref, factor_ref, drift_ref, own_ref, other_ref,
    image_ref, sums_ref,
):
    mine = half_of(lax.axis_index("c"))
    image = own_ref[...] + other_ref[...]
    image_ref[...] = image
    drift = drift_ref[...]
    image_two = two(image)
    rounded = image_two[0]
    wide = rounded.astype(f32)
    total = jnp.zeros((1, MANY), f32)
    for color, rows_ref in enumerate((r0, r1, r2)):
        for at in range(0, ROWS[color], CHUNK):
            projected = nn(rows_ref[pl.ds(at, CHUNK), :], rounded)
            factor = factor_ref[pl.ds(STARTS[color] + at, CHUNK), :]
            total += jnp.sum(projected * projected * factor, axis=0, keepdims=True)
    fit = jnp.sum(image * wide, axis=0, keepdims=True)
    fit = fit / jnp.maximum(jnp.sum(wide * wide, axis=0, keepdims=True), 1e-30)
    total *= fit * fit
    square = kernel_ref[mine, :] * kernel_ref[mine, :]
    along = stacked(two(x_ref[:, mine].T), image_two)
    gap = jnp.sum(x_ref[...] * image, axis=0, keepdims=True) - along
    total += cross * jnp.sum(square * gap * gap, axis=0, keepdims=True)
    length = jnp.sum(image * image, axis=0, keepdims=True)
    total += prior_precision * jnp.sum(square, axis=0, keepdims=True) * length
    figures = (
        jnp.sum(drift * drift, axis=0, keepdims=True),
        jnp.sum(drift * image, axis=0, keepdims=True),
        length,
        total / MANY,
    )
    for at, value in enumerate(figures):
        sums_ref[at : at + 1, :] = jnp.broadcast_to(
            jnp.sum(value, axis=1, keepdims=True), (1, HALF)
        )
    sums_ref[4:, :] = jnp.zeros((4, HALF), f32)


def call(kernel, outs, *args, scratch=(), far=False):
    whole = pl.BlockSpec(memory_space=pltpu.VMEM)
    return pl.pallas_call(
        kernel,
        out_shape=[jax.ShapeDtypeStruct(s, t) for s, t in outs],
        in_specs=[pl.BlockSpec(memory_space=pltpu.HBM) if far else whole] * len(args),
        out_specs=[whole] * len(outs),
        scratch_shapes=scratch,
        compiler_params=pltpu.CompilerParams(vmem_limit_bytes=(60 if far else 24) * 1024 * 1024),
    )(*args)


def per_device(particles, data_rows, labels):
    (copies,) = call(
        prepare_kernel,
        [((8, 8 * DATA + 16, SLICE), bf16)],
        particles, data_rows, labels,
        scratch=[
            pltpu.VMEM((8, SLICE), f32),
            pltpu.VMEM((8, DATA, SLICE), bf16),
            pltpu.VMEM((8, DATA), jnp.int32),
            pltpu.SemaphoreType.DMA((3,)),
        ],
        far=True,
    )
    pieces = gathered(copies)
    count = HALF * DATA
    tall = ((count, MANY), f32)
    square = ((MANY, MANY), f32)
    long = ((WIDE, MANY), f32)
    half = ((WIDE, HALF), f32)
    turn = [pltpu.VMEM((HALF, SLICE), f32)]
    rows_of = [((r, WIDE), bf16) for r in ROWS]
    hot_of = [((r, MANY), bf16) for r in ROWS]
    curve_of = [((r, HALF), f32) for r in ROWS]
    rows, hot, curve = [None] * 3, [None] * 3, [None] * 3
    rows[0], hot[0], x_own = call(
        land_kernel, [rows_of[0], hot_of[0], half], *pieces[0],
        scratch=[pltpu.VMEM((HALF, WIDE), f32)],
    )
    x_other = swap_cores(x_own)
    grad, curve[0] = call(grad_kernel, [half, curve_of[0]], rows[0], hot[0], x_own)
    kernel, x = call(start_kernel, [square, long], x_own, x_other)
    for color in (1, 2):
        rows[color], hot[color], grad, curve[color] = call(
            partial(land_grad_kernel, color),
            [rows_of[color], hot_of[color], half, curve_of[color]],
            *pieces[color], x_own, grad,
        )
    for newton_step in range(NEWTON):
        if newton_step > 0:
            grad, *curve, x, update = call(
                next_kernel, [half, *curve_of, long, ((8, SLICE), f32)],
                *rows, *hot, x, drift, image, sums, sums_other, scratch=turn,
            )
        grad_other = swap_cores(grad)
        if newton_step > 0:
            (kernel,) = call(again_kernel, [square], x)
        drift, image_own, factor = call(
            first_kernel,
            [long, long, tall],
            *rows, *hot, *curve, x, kernel, grad, grad_other,
            scratch=[pltpu.VMEM((2, count, MANY), bf16)],
        )
        image, sums = call(
            second_kernel,
            [long, ((8, HALF), f32)],
            *rows, x, kernel, factor, drift, image_own, swap_cores(image_own),
        )
        sums_other = swap_cores(sums)
    (updates,) = call(
        last_kernel, [((NEWTON, 8, SLICE), f32)],
        drift, image, sums, sums_other, update, scratch=turn,
    )
    return updates


def solution(mesh):
    torus = Mesh(mesh.devices.reshape(4, 4, 2, mesh.shape["dim"]), AXES)
    groups = ("y", "x", "c")
    in_specs = (P(groups, "z"), P(groups, None, "z"), P(groups, None))
    out_specs = P(None, groups, "z")

    return jax.shard_map(
        per_device, mesh=torus, in_specs=in_specs, out_specs=out_specs, check_vma=False
    )
```

```python
from functools import partial

import jax
import jax.numpy as jnp
import numpy as np
from jax import lax
from jax.experimental import pallas as pl
from jax.experimental.pallas import tpu as pltpu
from jax.sharding import Mesh
from jax.sharding import PartitionSpec as P


AXES = ("y", "x", "c", "z")
NEWTON = 2
prior_precision = 0.05
like_weight = 4.0
move_size = 0.5

f32 = jnp.float32
bf16 = jnp.bfloat16
WIDE = 1024
MANY = 256
HALF = 128
DATA = 16
SLICE = 256
scale = 1.0 * WIDE
cross = 4.0 / (scale * scale)

MASKS = (1, 3)
ORDERS = ("xyz", "yzx", "zxy")
SPOT = {"y": 0, "x": 1, "z": 3}
THIRDS = (96, 0, 48)
FIRSTS = (6, 0, 3)
ROWS = (512, 768, 768)
STARTS = (0, 512, 1280)
CHUNK = 256


def places():
    return np.ndindex(4, 4, 2, 4)


def spot(at):
    return int(np.ravel_multi_index(at, (4, 4, 2, 4)))


def pairs(axis):
    out = []
    for at in places():
        to = list(at)
        to[SPOT[axis]] ^= MASKS[1 - at[2]]
        out.append((spot(at), spot(to)))
    return out


def cubes():
    groups = {}
    for at in places():
        mask = MASKS[at[2]]
        key = (at[2],) + tuple(min(at[d], at[d] ^ mask) for d in (0, 1, 3))
        groups.setdefault(key, []).append(spot(at))
    return list(groups.values())


def swap_cores(x):
    return lax.ppermute(x, "c", [(0, 1), (1, 0)])


def gathered(copies):
    cube = lax.all_to_all(copies, AXES, 0, 0, axis_index_groups=cubes(), tiled=True)
    parts = [cube[:, k : k + 48] for k in THIRDS]

    def sent(parts, step):
        out = []
        for part, order in zip(parts, ORDERS):
            out.append(lax.ppermute(part, AXES, pairs(order[step])))
        return out

    near = [jnp.concatenate(both, axis=0) for both in zip(parts, sent(parts, 0))]
    aside = sent(near, 1)
    far = sent(near, 2)
    last = sent(aside, 2)
    return list(zip(near, aside, far, last))


def two(v):
    high = v.astype(bf16)
    return high, (v - high.astype(f32)).astype(bf16)


def nn(a, b):
    return lax.dot_general(a, b, (((1,), (0,)), ((), ())), preferred_element_type=f32)


def tn(a, b):
    return lax.dot_general(a, b, (((0,), (0,)), ((), ())), preferred_element_type=f32)


def stacked(a, b):
    left = jnp.concatenate([a[0], a[1], a[0]], axis=1)
    right = jnp.concatenate([b[0], b[0], b[1]], axis=0)
    return nn(left, right)


def own_place():
    y, x = lax.axis_index("y"), lax.axis_index("x")
    shift = lax.axis_index("c")
    return ((y >> shift) & 1) * 4 + ((x >> shift) & 1)


def slice_at(k):
    core, z = lax.axis_index("c"), lax.axis_index("z")
    seen = (0, 3, 1, 2)
    turned = (z ^ (z >> 1)) & 1
    return jnp.where(core == 0, k ^ (z & 2), jnp.where(turned == 1, seen[k ^ 2], seen[k]))


def cols(k):
    return slice(k * SLICE, (k + 1) * SLICE)


def span(color):
    return slice(STARTS[color], STARTS[color] + ROWS[color])


def half_of(core):
    return pl.ds(pl.multiple_of(core * HALF, HALF), HALF)


def in_order(core, own, other, axis):
    pair = jnp.where(core == 0, own, other), jnp.where(core == 0, other, own)
    return jnp.concatenate(pair, axis=axis)


def prepare_kernel(x_far, rows_far, labels_far, out_ref, x_ref, rows_ref, labels_ref, done):
    copies = [
        pltpu.make_async_copy(far, near, done.at[k])
        for k, (far, near) in enumerate(
            ((x_far, x_ref), (rows_far, rows_ref), (labels_far, labels_ref))
        )
    ]
    for copy in copies:
        copy.start()
    for copy in copies:
        copy.wait()
    sign = (2 * labels_ref[...] - 1).astype(f32).T
    pieces = [rows_ref[p].astype(f32) * sign[:, p : p + 1] for p in range(8)]
    whole = jnp.concatenate([p.astype(bf16) for p in pieces] + list(two(x_ref[...])), axis=0)
    for k in range(8):
        out_ref[k] = whole


def land(color, refs, rows_ref, hot_ref, tail_ref=None):
    count = ROWS[color] // 16
    order = ORDERS[color]
    for k in range(4):
        slot = pl.ds(pl.multiple_of(slice_at(k) * SLICE, SLICE), SLICE)
        for at in range(16):
            step = {"z": k >> 1, "y": at >> 3, "x": (at >> 1) & 1}
            unit = step[order[0]] * 8 + ((at >> 2) & 1) * 4 + (at & 1) * 2 + (k & 1)
            ref = refs[step[order[2]] * 2 + step[order[1]]]
            rows_ref[at * count : (at + 1) * count, slot] = ref[unit, :count, :]
            if tail_ref is not None:
                high, low = ref[unit, 32:40, :], ref[unit, 40:48, :]
                tail_ref[at * 8 : at * 8 + 8, slot] = high.astype(f32) + low.astype(f32)
    row = lax.broadcasted_iota(jnp.int32, (ROWS[color], HALF), 0)
    place = (row * 43691) >> 21 if count == 48 else row >> 5
    owner = place * 8 + FIRSTS[color] + ((row - place * count) >> 4)
    hot = owner == lax.broadcasted_iota(jnp.int32, (ROWS[color], HALF), 1)
    hot = jnp.where(hot, 1.0, 0.0).astype(bf16)
    hot_ref[...] = hot


def gradient(rows_ref, hot_ref, both, curve_ref):
    weights = []
    for at in range(0, rows_ref.shape[0], CHUNK):
        part = pl.ds(at, CHUNK)
        logit = nn(rows_ref[part, :], both)
        hot = hot_ref[part, :].astype(f32)
        logit = jnp.sum((logit[:, :HALF] + logit[:, HALF:]) * hot, axis=1, keepdims=True)
        prob = 1.0 / (1.0 + jnp.exp(logit))
        curve_ref[part, :] = jnp.broadcast_to(like_weight * prob * (1.0 - prob), (CHUNK, HALF))
        weights.append(jnp.concatenate(two(like_weight * prob * hot), axis=1))
    return tn(rows_ref[...], jnp.concatenate(weights, axis=0))


def folded(total):
    return total[:, :HALF] + total[:, HALF:]


def land_kernel(a, b, c, d, rows_ref, hot_ref, x_ref, tail_ref):
    land(0, (a, b, c, d), rows_ref, hot_ref, tail_ref)
    for k in range(4):
        x_ref[cols(k), :] = tail_ref[:, cols(k)].T


def grad_kernel(rows_ref, hot_ref, x_ref, grad_ref, curve_ref):
    x = x_ref[...]
    both = jnp.concatenate(two(x), axis=1)
    grad_ref[...] = folded(gradient(rows_ref, hot_ref, both, curve_ref)) - (
        prior_precision + 2.0 / scale
    ) * x


def land_grad_kernel(color, a, b, c, d, x_ref, before_ref, rows_ref, hot_ref, grad_ref, curve_ref):
    land(color, (a, b, c, d), rows_ref, hot_ref)
    both = jnp.concatenate(two(x_ref[...]), axis=1)
    grad_ref[...] = before_ref[...] + folded(gradient(rows_ref, hot_ref, both, curve_ref))


def factors(own_ref, other_ref):
    mu0, mu1, mu2 = (own_ref[k : k + 1, :1] for k in range(3))
    mu3 = own_ref[3:4, :1] + other_ref[3:4, :1]
    alpha = mu0 / mu1
    left = mu0 - 2.0 * alpha * mu1 + alpha * alpha * mu2
    grown = 1.0 + left / mu0
    gamma = left / (grown * grown * mu1 - 2.0 * grown * alpha * mu2 + alpha * alpha * mu3)
    return alpha + gamma * grown, -gamma * alpha


def own_update(on_drift, on_image, drift_ref, image_refs, turn_ref):
    mine = half_of(lax.axis_index("c"))
    z = lax.axis_index("z")
    own = pl.ds(pl.multiple_of(z * SLICE, SLICE), SLICE)
    near = pl.ds(pl.multiple_of((z & 1) * SLICE, SLICE), SLICE)
    image = jnp.where(z < 2, image_refs[0][near, mine], image_refs[1][near, mine])
    turn_ref[...] = (on_drift * drift_ref[own, mine] + on_image * image).T
    return turn_ref[pl.ds(pl.multiple_of(own_place() * 8, 8), 8), :]


def next_kernel(
    r0, r1, r2, h0, h1, h2, x_ref, drift_ref, image_a, image_b, own_ref, other_ref,
    grad_ref, c0, c1, c2, new_ref, out_ref, turn_ref,
):
    on_drift, on_image = factors(own_ref, other_ref)
    images = (image_a, image_b)
    out_ref[...] = own_update(on_drift, on_image, drift_ref, images, turn_ref)
    for k, image_ref in enumerate(images):
        near = slice(k * WIDE // 2, (k + 1) * WIDE // 2)
        update = on_drift * drift_ref[near, :] + on_image * image_ref[...]
        new_ref[near, :] = x_ref[near, :] + move_size * update
    x = new_ref[:, half_of(lax.axis_index("c"))]
    both = jnp.concatenate(two(x), axis=1)
    total = gradient(r0, h0, both, c0) + gradient(r1, h1, both, c1) + gradient(r2, h2, both, c2)
    grad_ref[...] = folded(total) - (prior_precision + 2.0 / scale) * x


def last_kernel(
    drift_ref, image_a, image_b, own_ref, other_ref, before_ref, out_ref, turn_ref
):
    on_drift, on_image = factors(own_ref, other_ref)
    out_ref[0] = before_ref[...]
    out_ref[1] = own_update(on_drift, on_image, drift_ref, (image_a, image_b), turn_ref)


def similarity(x, kernel_ref):
    high, low = two(x)
    gram = tn(high, high) + (tn(high, low) + tn(low, high))
    shape = (MANY, MANY)
    same = lax.broadcasted_iota(jnp.int32, shape, 0) == lax.broadcasted_iota(jnp.int32, shape, 1)
    diag = jnp.where(same, gram, 0.0)
    squares = jnp.sum(diag, axis=1, keepdims=True) + jnp.sum(diag, axis=0, keepdims=True)
    kernel_ref[...] = jnp.exp((2.0 * gram - squares) / scale)


def start_kernel(own_ref, other_ref, kernel_ref, x_ref):
    x = in_order(lax.axis_index("c"), own_ref[...], other_ref[...], 1)
    x_ref[...] = x
    similarity(x, kernel_ref)


def again_kernel(x_ref, kernel_ref):
    similarity(x_ref[...], kernel_ref)


def spread(thirds, weighted_ref, near):
    return sum(
        tn(rows_ref[:, near], weighted_ref[k, span(color), :])
        for color, rows_ref in enumerate(thirds)
        for k in range(2)
    )


def image_part(thirds, near, x_ref, drift, square, q, weighted_ref):
    mine = half_of(lax.axis_index("c"))
    pull = x_ref[near, :] * jnp.sum(q, axis=0, keepdims=True)
    pull = pull - stacked(two(x_ref[near, mine]), two(q))
    own = prior_precision * jnp.sum(square, axis=0, keepdims=True) * drift
    return (spread(thirds, weighted_ref, near) + (own + cross * pull)) / MANY


def first_kernel(
    r0, r1, r2, c0, c1, c2, x_ref, kernel_ref, own_ref, other_ref,
    drift_ref, image_ref, factor_ref, weighted_ref, q_ref, square_ref,
):
    core = lax.axis_index("c")
    mine = half_of(core)
    x = x_ref[...]
    grad = in_order(core, own_ref[...], other_ref[...], 1)
    drift = stacked(two(grad), two(kernel_ref[...]))
    total = jnp.sum(kernel_ref[...], axis=0, keepdims=True)
    drift = (drift + (2.0 / scale) * total * x) / MANY
    drift_ref[...] = drift
    drift_two = two(drift)
    kernel_own = kernel_ref[mine, :]
    square = kernel_own * kernel_own
    square_ref[...] = square
    thirds = (r0, r1, r2)
    for color, (rows_ref, curve_ref) in enumerate(zip(thirds, (c0, c1, c2))):
        count = ROWS[color] // 256
        for at in range(0, ROWS[color], CHUNK):
            part, to = pl.ds(at, CHUNK), pl.ds(STARTS[color] + at, CHUNK)
            pieces = []
            for group in range(at // DATA, (at + CHUNK) // DATA):
                j = group // count * 8 + FIRSTS[color] + group % count
                curve = curve_ref[pl.ds(group * DATA, DATA), :]
                wide = jnp.concatenate([curve, curve], axis=1)
                pieces.append(jnp.broadcast_to(square_ref[j : j + 1, :], wide.shape) * wide)
            factor = jnp.concatenate(pieces, axis=0)
            factor_ref[to, :] = factor
            rows = rows_ref[part, :]
            high, low = two((nn(rows, drift_two[0]) + nn(rows, drift_two[1])) * factor)
            weighted_ref[0, to, :] = high
            weighted_ref[1, to, :] = low
    along = stacked(two(x_ref[:, mine].T), drift_two)
    q = square * (jnp.sum(x * drift, axis=0, keepdims=True) - along)
    q_ref[...] = q
    near = slice(0, WIDE // 2)
    image_ref[...] = image_part(thirds, near, x_ref, drift[near], square, q, weighted_ref)


def rest_kernel(r0, r1, r2, x_ref, kernel_ref, drift_ref, weighted_ref, q_ref, image_ref):
    kernel_own = kernel_ref[half_of(lax.axis_index("c")), :]
    near = slice(WIDE // 2, WIDE)
    image_ref[...] = image_part(
        (r0, r1, r2), near, x_ref, drift_ref[near, :], kernel_own * kernel_own, q_ref[...],
        weighted_ref,
    )


def read_image(near, x_ref, drift_ref, image):
    rounded = image.astype(bf16)
    wide = rounded.astype(f32)
    pairs_ = (
        (drift_ref[near, :], drift_ref[near, :]),
        (drift_ref[near, :], image),
        (image, image),
        (image, wide),
        (wide, wide),
        (x_ref[near, :], image),
    )
    sums = [jnp.sum(a * b, axis=0, keepdims=True) for a, b in pairs_]
    x_own = x_ref[near, half_of(lax.axis_index("c"))]
    return sums, stacked(two(x_own.T), two(image)), rounded


def second_kernel(
    r0, r1, r2, x_ref, drift_ref, own_ref, other_ref,
    image_ref, projected_ref, along_ref, sums_ref,
):
    near = slice(0, WIDE // 2)
    image = own_ref[...] + other_ref[...]
    image_ref[...] = image
    sums, along, rounded = read_image(near, x_ref, drift_ref, image)
    along_ref[...] = along
    for at, value in enumerate(sums):
        sums_ref[at : at + 1, :] = value
    sums_ref[6:, :] = jnp.zeros((2, MANY), f32)
    for color, rows_ref in enumerate((r0, r1, r2)):
        projected_ref[span(color), :] = nn(rows_ref[:, near], rounded)


def third_kernel(
    r0, r1, r2, x_ref, kernel_ref, factor_ref, drift_ref, projected_ref, along_ref, before_ref,
    own_ref, other_ref,
    image_ref, sums_ref,
):
    near = slice(WIDE // 2, WIDE)
    image = own_ref[...] + other_ref[...]
    image_ref[...] = image
    sums, along, rounded = read_image(near, x_ref, drift_ref, image)
    sums = [value + before_ref[at : at + 1, :] for at, value in enumerate(sums)]
    total = jnp.zeros((1, MANY), f32)
    for color, rows_ref in enumerate((r0, r1, r2)):
        for at in range(0, ROWS[color], CHUNK):
            to = pl.ds(STARTS[color] + at, CHUNK)
            projected = projected_ref[to, :] + nn(rows_ref[pl.ds(at, CHUNK), near], rounded)
            total += jnp.sum(projected * projected * factor_ref[to, :], axis=0, keepdims=True)
    fit = sums[3] / jnp.maximum(sums[4], 1e-30)
    total *= fit * fit
    mine = half_of(lax.axis_index("c"))
    square = kernel_ref[mine, :] * kernel_ref[mine, :]
    gap = sums[5] - (along + along_ref[...])
    total += cross * jnp.sum(square * gap * gap, axis=0, keepdims=True)
    total += prior_precision * jnp.sum(square, axis=0, keepdims=True) * sums[2]
    for at, value in enumerate((*sums[:3], total / MANY)):
        sums_ref[at : at + 1, :] = jnp.broadcast_to(
            jnp.sum(value, axis=1, keepdims=True), (1, HALF)
        )
    sums_ref[4:, :] = jnp.zeros((4, HALF), f32)


def call(kernel, outs, *args, scratch=(), far=False):
    whole = pl.BlockSpec(memory_space=pltpu.VMEM)
    return pl.pallas_call(
        kernel,
        out_shape=[jax.ShapeDtypeStruct(s, t) for s, t in outs],
        in_specs=[pl.BlockSpec(memory_space=pltpu.HBM) if far else whole] * len(args),
        out_specs=[whole] * len(outs),
        scratch_shapes=scratch,
        compiler_params=pltpu.CompilerParams(vmem_limit_bytes=(60 if far else 24) * 1024 * 1024),
    )(*args)


def per_device(particles, data_rows, labels):
    (copies,) = call(
        prepare_kernel,
        [((8, 8 * DATA + 16, SLICE), bf16)],
        particles, data_rows, labels,
        scratch=[
            pltpu.VMEM((8, SLICE), f32),
            pltpu.VMEM((8, DATA, SLICE), bf16),
            pltpu.VMEM((8, DATA), jnp.int32),
            pltpu.SemaphoreType.DMA((3,)),
        ],
        far=True,
    )
    pieces = gathered(copies)
    count = HALF * DATA
    tall = ((count, MANY), f32)
    square = ((MANY, MANY), f32)
    long = ((WIDE, MANY), f32)
    wing = ((WIDE // 2, MANY), f32)
    low = ((HALF, MANY), f32)
    half = ((WIDE, HALF), f32)
    turn = [pltpu.VMEM((HALF, SLICE), f32)]
    rows_of = [((r, WIDE), bf16) for r in ROWS]
    hot_of = [((r, HALF), bf16) for r in ROWS]
    curve_of = [((r, HALF), f32) for r in ROWS]
    rows, hot, curve = [None] * 3, [None] * 3, [None] * 3
    rows[0], hot[0], x_own = call(
        land_kernel, [rows_of[0], hot_of[0], half], *pieces[0],
        scratch=[pltpu.VMEM((HALF, WIDE), f32)],
    )
    x_other = swap_cores(x_own)
    grad, curve[0] = call(grad_kernel, [half, curve_of[0]], rows[0], hot[0], x_own)
    kernel, x = call(start_kernel, [square, long], x_own, x_other)
    for color in (1, 2):
        rows[color], hot[color], grad, curve[color] = call(
            partial(land_grad_kernel, color),
            [rows_of[color], hot_of[color], half, curve_of[color]],
            *pieces[color], x_own, grad,
        )
    for newton_step in range(NEWTON):
        if newton_step > 0:
            grad, *curve, x, update = call(
                next_kernel, [half, *curve_of, long, ((8, SLICE), f32)],
                *rows, *hot, x, drift, *image, sums, sums_other, scratch=turn,
            )
        grad_other = swap_cores(grad)
        if newton_step > 0:
            (kernel,) = call(again_kernel, [square], x)
        drift, own_a, factor, weighted, q = call(
            first_kernel,
            [long, wing, tall, ((2, count, MANY), bf16), low],
            *rows, *curve, x, kernel, grad, grad_other,
            scratch=[pltpu.VMEM((HALF, MANY), f32)],
        )
        other_a = swap_cores(own_a)
        (own_b,) = call(rest_kernel, [wing], *rows, x, kernel, drift, weighted, q)
        other_b = swap_cores(own_b)
        image_a, projected, along, partial_sums = call(
            second_kernel, [wing, tall, low, ((8, MANY), f32)],
            *rows, x, drift, own_a, other_a,
        )
        image_b, sums = call(
            third_kernel, [wing, ((8, HALF), f32)],
            *rows, x, kernel, factor, drift, projected, along, partial_sums, own_b, other_b,
        )
        image = (image_a, image_b)
        sums_other = swap_cores(sums)
    (updates,) = call(
        last_kernel, [((NEWTON, 8, SLICE), f32)],
        drift, *image, sums, sums_other, update, scratch=turn,
    )
    return updates


def solution(mesh):
    torus = Mesh(mesh.devices.reshape(4, 4, 2, mesh.shape["dim"]), AXES)
    groups = ("y", "x", "c")
    in_specs = (P(groups, "z"), P(groups, None, "z"), P(groups, None))
    out_specs = P(None, groups, "z")

    return jax.shard_map(
        per_device, mesh=torus, in_specs=in_specs, out_specs=out_specs, check_vma=False
    )
```

```python
from functools import partial

import jax
import jax.numpy as jnp
import numpy as np
from jax import lax
from jax.experimental import pallas as pl
from jax.experimental.pallas import tpu as pltpu
from jax.sharding import Mesh
from jax.sharding import PartitionSpec as P


AXES = ("y", "x", "c", "z")
NEWTON = 2
prior_precision = 0.05
like_weight = 4.0
move_size = 0.5

f32 = jnp.float32
bf16 = jnp.bfloat16
WIDE = 1024
MANY = 256
HALF = 128
DATA = 16
SLICE = 256
scale = 1.0 * WIDE
cross = 4.0 / (scale * scale)

MASKS = (1, 3)
ORDERS = ("xyz", "yzx", "zxy")
SPOT = {"y": 0, "x": 1, "z": 3}
THIRDS = (96, 0, 48)
FIRSTS = (6, 0, 3)
ROWS = (512, 768, 768)
STARTS = (0, 512, 1280)
CHUNK = 256


def places():
    return np.ndindex(4, 4, 2, 4)


def spot(at):
    return int(np.ravel_multi_index(at, (4, 4, 2, 4)))


def pairs(axis):
    out = []
    for at in places():
        to = list(at)
        to[SPOT[axis]] ^= MASKS[1 - at[2]]
        out.append((spot(at), spot(to)))
    return out


def cubes():
    groups = {}
    for at in places():
        mask = MASKS[at[2]]
        key = (at[2],) + tuple(min(at[d], at[d] ^ mask) for d in (0, 1, 3))
        groups.setdefault(key, []).append(spot(at))
    return list(groups.values())


def swap_cores(x):
    return lax.ppermute(x, "c", [(0, 1), (1, 0)])


def gathered(copies):
    cube = lax.all_to_all(copies, AXES, 0, 0, axis_index_groups=cubes(), tiled=True)
    parts = [cube[:, k : k + 48] for k in THIRDS]

    def sent(parts, step):
        out = []
        for part, order in zip(parts, ORDERS):
            out.append(lax.ppermute(part, AXES, pairs(order[step])))
        return out

    near = [jnp.concatenate(both, axis=0) for both in zip(parts, sent(parts, 0))]
    aside = sent(near, 1)
    far = sent(near, 2)
    last = sent(aside, 2)
    return list(zip(near, aside, far, last))


def two(v):
    high = v.astype(bf16)
    return high, (v - high.astype(f32)).astype(bf16)


def nn(a, b):
    return lax.dot_general(a, b, (((1,), (0,)), ((), ())), preferred_element_type=f32)


def tn(a, b):
    return lax.dot_general(a, b, (((0,), (0,)), ((), ())), preferred_element_type=f32)


def stacked(a, b):
    left = jnp.concatenate([a[0], a[1], a[0]], axis=1)
    right = jnp.concatenate([b[0], b[0], b[1]], axis=0)
    return nn(left, right)


def own_place():
    y, x = lax.axis_index("y"), lax.axis_index("x")
    shift = lax.axis_index("c")
    return ((y >> shift) & 1) * 4 + ((x >> shift) & 1)


def slice_at(k):
    core, z = lax.axis_index("c"), lax.axis_index("z")
    seen = (0, 3, 1, 2)
    turned = (z ^ (z >> 1)) & 1
    return jnp.where(core == 0, k ^ (z & 2), jnp.where(turned == 1, seen[k ^ 2], seen[k]))


def cols(k):
    return slice(k * SLICE, (k + 1) * SLICE)


def span(color):
    return slice(STARTS[color], STARTS[color] + ROWS[color])


def half_of(core):
    return pl.ds(pl.multiple_of(core * HALF, HALF), HALF)


def in_order(core, own, other, axis):
    pair = jnp.where(core == 0, own, other), jnp.where(core == 0, other, own)
    return jnp.concatenate(pair, axis=axis)


def prepare_kernel(x_far, rows_far, labels_far, out_ref, x_ref, rows_ref, labels_ref, done):
    copies = [
        pltpu.make_async_copy(far, near, done.at[k])
        for k, (far, near) in enumerate(
            ((x_far, x_ref), (rows_far, rows_ref), (labels_far, labels_ref))
        )
    ]
    for copy in copies:
        copy.start()
    for copy in copies:
        copy.wait()
    sign = (2 * labels_ref[...] - 1).astype(f32).T
    pieces = [rows_ref[p].astype(f32) * sign[:, p : p + 1] for p in range(8)]
    whole = jnp.concatenate([p.astype(bf16) for p in pieces] + list(two(x_ref[...])), axis=0)
    for k in range(8):
        out_ref[k] = whole


def land(color, refs, arrived, rows_ref, tail_ref):
    count = ROWS[color] // 16
    order = ORDERS[color]
    for k in range(4):
        slot = pl.ds(pl.multiple_of(slice_at(k) * SLICE, SLICE), SLICE)
        for at in range(16):
            step = {"z": k >> 1, "y": at >> 3, "x": (at >> 1) & 1}
            which = step[order[2]] * 2 + step[order[1]]
            if which not in arrived:
                continue
            unit = step[order[0]] * 8 + ((at >> 2) & 1) * 4 + (at & 1) * 2 + (k & 1)
            ref = refs[which]
            start = STARTS[color] + at * count
            rows_ref[start : start + count, slot] = ref[unit, :count, :]
            if color == 0:
                high, low = ref[unit, 32:40, :], ref[unit, 40:48, :]
                tail_ref[at * 8 : at * 8 + 8, slot] = high.astype(f32) + low.astype(f32)


def early_kernel(*refs):
    rows_ref, tail_ref, hot_ref = refs[9:]
    for color in range(3):
        land(color, refs[3 * color : 3 * color + 3], (0, 1, 2), rows_ref, tail_ref)
        count = ROWS[color] // 16
        row = lax.broadcasted_iota(jnp.int32, (ROWS[color], HALF), 0)
        place = (row * 43691) >> 21 if count == 48 else row >> 5
        owner = place * 8 + FIRSTS[color] + ((row - place * count) >> 4)
        hot = owner == lax.broadcasted_iota(jnp.int32, (ROWS[color], HALF), 1)
        hot_ref[span(color), :] = jnp.where(hot, 1.0, 0.0).astype(bf16)


def gradient(rows_ref, hot_ref, x, curve_ref, start, stop):
    both = jnp.concatenate(two(x), axis=1)
    weights = []
    for at in range(start, stop, CHUNK):
        part = pl.ds(at, CHUNK)
        logit = nn(rows_ref[part, :], both)
        hot = hot_ref[part, :].astype(f32)
        logit = jnp.sum((logit[:, :HALF] + logit[:, HALF:]) * hot, axis=1, keepdims=True)
        prob = 1.0 / (1.0 + jnp.exp(logit))
        curve_ref[part, :] = jnp.broadcast_to(like_weight * prob * (1.0 - prob), (CHUNK, HALF))
        weights.append(jnp.concatenate(two(like_weight * prob * hot), axis=1))
    total = tn(rows_ref[start:stop, :], jnp.concatenate(weights, axis=0))
    return total[:, :HALF] + total[:, HALF:]


def position_kernel(_, __, hot_ref, d, rows_ref, tail_ref, x_ref, grad_ref, curve_ref):
    land(0, (None, None, None, d), (3,), rows_ref, tail_ref)
    for k in range(4):
        x_ref[cols(k), :] = tail_ref[:, cols(k)].T
    x = x_ref[...]
    part = gradient(rows_ref, hot_ref, x, curve_ref, 0, ROWS[0])
    grad_ref[...] = part - (prior_precision + 2.0 / scale) * x


def grad_kernel(color, _, before_ref, __, hot_ref, x_ref, d, rows_ref, grad_ref, curve_ref):
    land(color, (None, None, None, d), (3,), rows_ref, None)
    start = STARTS[color]
    part = gradient(rows_ref, hot_ref, x_ref[...], curve_ref, start, start + ROWS[color])
    grad_ref[...] = before_ref[...] + part


def factors(own_ref, other_ref):
    mu0, mu1, mu2 = (own_ref[k : k + 1, :1] for k in range(3))
    mu3 = own_ref[3:4, :1] + other_ref[3:4, :1]
    alpha = mu0 / mu1
    left = mu0 - 2.0 * alpha * mu1 + alpha * alpha * mu2
    grown = 1.0 + left / mu0
    gamma = left / (grown * grown * mu1 - 2.0 * grown * alpha * mu2 + alpha * alpha * mu3)
    return alpha + gamma * grown, -gamma * alpha


def own_update(on_drift, on_image, drift_ref, image_refs, turn_ref):
    mine = half_of(lax.axis_index("c"))
    z = lax.axis_index("z")
    own = pl.ds(pl.multiple_of(z * SLICE, SLICE), SLICE)
    near = pl.ds(pl.multiple_of((z & 1) * SLICE, SLICE), SLICE)
    image = jnp.where(z < 2, image_refs[0][near, mine], image_refs[1][near, mine])
    turn_ref[...] = (on_drift * drift_ref[own, mine] + on_image * image).T
    return turn_ref[pl.ds(pl.multiple_of(own_place() * 8, 8), 8), :]


def next_kernel(
    rows_ref, hot_ref, x_ref, drift_ref, image_a, image_b, own_ref, other_ref,
    grad_ref, curve_ref, new_ref, out_ref, turn_ref,
):
    on_drift, on_image = factors(own_ref, other_ref)
    images = (image_a, image_b)
    out_ref[...] = own_update(on_drift, on_image, drift_ref, images, turn_ref)
    for k, image_ref in enumerate(images):
        near = slice(k * WIDE // 2, (k + 1) * WIDE // 2)
        update = on_drift * drift_ref[near, :] + on_image * image_ref[...]
        new_ref[near, :] = x_ref[near, :] + move_size * update
    x = new_ref[:, half_of(lax.axis_index("c"))]
    part = gradient(rows_ref, hot_ref, x, curve_ref, 0, HALF * DATA)
    grad_ref[...] = part - (prior_precision + 2.0 / scale) * x


def last_kernel(
    drift_ref, image_a, image_b, own_ref, other_ref, before_ref, out_ref, turn_ref
):
    on_drift, on_image = factors(own_ref, other_ref)
    out_ref[0] = before_ref[...]
    out_ref[1] = own_update(on_drift, on_image, drift_ref, (image_a, image_b), turn_ref)


def similarity(x, kernel_ref):
    high, low = two(x)
    gram = tn(high, high) + (tn(high, low) + tn(low, high))
    shape = (MANY, MANY)
    same = lax.broadcasted_iota(jnp.int32, shape, 0) == lax.broadcasted_iota(jnp.int32, shape, 1)
    diag = jnp.where(same, gram, 0.0)
    squares = jnp.sum(diag, axis=1, keepdims=True) + jnp.sum(diag, axis=0, keepdims=True)
    kernel_ref[...] = jnp.exp((2.0 * gram - squares) / scale)


def start_kernel(own_ref, other_ref, kernel_ref, x_ref):
    x = in_order(lax.axis_index("c"), own_ref[...], other_ref[...], 1)
    x_ref[...] = x
    similarity(x, kernel_ref)


def again_kernel(x_ref, kernel_ref):
    similarity(x_ref[...], kernel_ref)


def spread(rows_ref, weighted_ref, near):
    rows = rows_ref[:, near]
    return tn(rows, weighted_ref[0]) + tn(rows, weighted_ref[1])


def image_part(rows_ref, near, x_ref, drift, square, q, weighted_ref):
    mine = half_of(lax.axis_index("c"))
    pull = x_ref[near, :] * jnp.sum(q, axis=0, keepdims=True)
    pull = pull - stacked(two(x_ref[near, mine]), two(q))
    own = prior_precision * jnp.sum(square, axis=0, keepdims=True) * drift
    return (spread(rows_ref, weighted_ref, near) + (own + cross * pull)) / MANY


def first_kernel(
    rows_ref, curve_ref, x_ref, kernel_ref, own_ref, other_ref,
    drift_ref, image_ref, factor_ref, weighted_ref, q_ref, square_ref,
):
    core = lax.axis_index("c")
    mine = half_of(core)
    x = x_ref[...]
    grad = in_order(core, own_ref[...], other_ref[...], 1)
    drift = stacked(two(grad), two(kernel_ref[...]))
    total = jnp.sum(kernel_ref[...], axis=0, keepdims=True)
    drift = (drift + (2.0 / scale) * total * x) / MANY
    drift_ref[...] = drift
    drift_two = two(drift)
    kernel_own = kernel_ref[mine, :]
    square = kernel_own * kernel_own
    square_ref[...] = square
    for color in range(3):
        count = ROWS[color] // 256
        for at in range(0, ROWS[color], CHUNK):
            to = pl.ds(STARTS[color] + at, CHUNK)
            pieces = []
            for group in range(at // DATA, (at + CHUNK) // DATA):
                j = group // count * 8 + FIRSTS[color] + group % count
                curve = curve_ref[pl.ds(STARTS[color] + group * DATA, DATA), :]
                wide = jnp.concatenate([curve, curve], axis=1)
                pieces.append(jnp.broadcast_to(square_ref[j : j + 1, :], wide.shape) * wide)
            factor = jnp.concatenate(pieces, axis=0)
            factor_ref[to, :] = factor
            rows = rows_ref[to, :]
            high, low = two((nn(rows, drift_two[0]) + nn(rows, drift_two[1])) * factor)
            weighted_ref[0, to, :] = high
            weighted_ref[1, to, :] = low
    along = stacked(two(x_ref[:, mine].T), drift_two)
    q = square * (jnp.sum(x * drift, axis=0, keepdims=True) - along)
    q_ref[...] = q
    near = slice(0, WIDE // 2)
    image_ref[...] = image_part(rows_ref, near, x_ref, drift[near], square, q, weighted_ref)


def rest_kernel(rows_ref, x_ref, kernel_ref, drift_ref, weighted_ref, q_ref, image_ref):
    kernel_own = kernel_ref[half_of(lax.axis_index("c")), :]
    near = slice(WIDE // 2, WIDE)
    image_ref[...] = image_part(
        rows_ref, near, x_ref, drift_ref[near, :], kernel_own * kernel_own, q_ref[...],
        weighted_ref,
    )


def read_image(near, x_ref, drift_ref, image):
    rounded = image.astype(bf16)
    wide = rounded.astype(f32)
    pairs_ = (
        (drift_ref[near, :], drift_ref[near, :]),
        (drift_ref[near, :], image),
        (image, image),
        (image, wide),
        (wide, wide),
        (x_ref[near, :], image),
    )
    sums = [jnp.sum(a * b, axis=0, keepdims=True) for a, b in pairs_]
    x_own = x_ref[near, half_of(lax.axis_index("c"))]
    return sums, stacked(two(x_own.T), two(image)), rounded


def second_kernel(
    rows_ref, x_ref, drift_ref, own_ref, other_ref,
    image_ref, projected_ref, along_ref, sums_ref,
):
    near = slice(0, WIDE // 2)
    image = own_ref[...] + other_ref[...]
    image_ref[...] = image
    sums, along, rounded = read_image(near, x_ref, drift_ref, image)
    along_ref[...] = along
    for at, value in enumerate(sums):
        sums_ref[at : at + 1, :] = value
    sums_ref[6:, :] = jnp.zeros((2, MANY), f32)
    projected_ref[...] = nn(rows_ref[:, near], rounded)


def third_kernel(
    rows_ref, x_ref, kernel_ref, factor_ref, drift_ref, projected_ref, along_ref, before_ref,
    own_ref, other_ref,
    image_ref, sums_ref,
):
    near = slice(WIDE // 2, WIDE)
    image = own_ref[...] + other_ref[...]
    image_ref[...] = image
    sums, along, rounded = read_image(near, x_ref, drift_ref, image)
    sums = [value + before_ref[at : at + 1, :] for at, value in enumerate(sums)]
    total = jnp.zeros((1, MANY), f32)
    for at in range(0, HALF * DATA, CHUNK):
        to = pl.ds(at, CHUNK)
        projected = projected_ref[to, :] + nn(rows_ref[to, near], rounded)
        total += jnp.sum(projected * projected * factor_ref[to, :], axis=0, keepdims=True)
    fit = sums[3] / jnp.maximum(sums[4], 1e-30)
    total *= fit * fit
    mine = half_of(lax.axis_index("c"))
    square = kernel_ref[mine, :] * kernel_ref[mine, :]
    gap = sums[5] - (along + along_ref[...])
    total += cross * jnp.sum(square * gap * gap, axis=0, keepdims=True)
    total += prior_precision * jnp.sum(square, axis=0, keepdims=True) * sums[2]
    for at, value in enumerate((*sums[:3], total / MANY)):
        sums_ref[at : at + 1, :] = jnp.broadcast_to(
            jnp.sum(value, axis=1, keepdims=True), (1, HALF)
        )
    sums_ref[4:, :] = jnp.zeros((4, HALF), f32)


def call(kernel, outs, *args, scratch=(), far=False, aliases=None):
    whole = pl.BlockSpec(memory_space=pltpu.VMEM)
    return pl.pallas_call(
        kernel,
        out_shape=[jax.ShapeDtypeStruct(s, t) for s, t in outs],
        in_specs=[pl.BlockSpec(memory_space=pltpu.HBM) if far else whole] * len(args),
        out_specs=[whole] * len(outs),
        scratch_shapes=scratch,
        input_output_aliases=aliases or {},
        compiler_params=pltpu.CompilerParams(vmem_limit_bytes=(60 if far else 24) * 1024 * 1024),
    )(*args)


def per_device(particles, data_rows, labels):
    (copies,) = call(
        prepare_kernel,
        [((8, 8 * DATA + 16, SLICE), bf16)],
        particles, data_rows, labels,
        scratch=[
            pltpu.VMEM((8, SLICE), f32),
            pltpu.VMEM((8, DATA, SLICE), bf16),
            pltpu.VMEM((8, DATA), jnp.int32),
            pltpu.SemaphoreType.DMA((3,)),
        ],
        far=True,
    )
    pieces = gathered(copies)
    count = HALF * DATA
    tall = ((count, MANY), f32)
    square = ((MANY, MANY), f32)
    long = ((WIDE, MANY), f32)
    wing = ((WIDE // 2, MANY), f32)
    low = ((HALF, MANY), f32)
    half = ((WIDE, HALF), f32)
    turn = [pltpu.VMEM((HALF, SLICE), f32)]
    rows_of = ((count, WIDE), bf16)
    tail_of = ((HALF, WIDE), f32)
    curve_of = ((count, HALF), f32)
    rows, tail, hot = call(
        early_kernel,
        [rows_of, tail_of, ((count, HALF), bf16)],
        *(a for four in pieces for a in four[:3]),
    )
    rows, tail, x_own, grad, curve = call(
        position_kernel,
        [rows_of, tail_of, half, half, curve_of],
        rows, tail, hot, pieces[0][3],
        aliases={0: 0, 1: 1},
    )
    x_other = swap_cores(x_own)
    for color in (1, 2):
        rows, grad, curve = call(
            partial(grad_kernel, color),
            [rows_of, half, curve_of],
            rows, grad, curve, hot, x_own, pieces[color][3],
            aliases={0: 0, 1: 1, 2: 2},
        )
    kernel, x = call(start_kernel, [square, long], x_own, x_other)
    for newton_step in range(NEWTON):
        if newton_step > 0:
            grad, curve, x, update = call(
                next_kernel, [half, curve_of, long, ((8, SLICE), f32)],
                rows, hot, x, drift, *image, sums, sums_other, scratch=turn,
            )
        grad_other = swap_cores(grad)
        if newton_step > 0:
            (kernel,) = call(again_kernel, [square], x)
        drift, own_a, factor, weighted, q = call(
            first_kernel,
            [long, wing, tall, ((2, count, MANY), bf16), low],
            rows, curve, x, kernel, grad, grad_other,
            scratch=[pltpu.VMEM((HALF, MANY), f32)],
        )
        other_a = swap_cores(own_a)
        (own_b,) = call(rest_kernel, [wing], rows, x, kernel, drift, weighted, q)
        other_b = swap_cores(own_b)
        image_a, projected, along, partial_sums = call(
            second_kernel, [wing, tall, low, ((8, MANY), f32)],
            rows, x, drift, own_a, other_a,
        )
        image_b, sums = call(
            third_kernel, [wing, ((8, HALF), f32)],
            rows, x, kernel, factor, drift, projected, along, partial_sums, own_b, other_b,
        )
        image = (image_a, image_b)
        sums_other = swap_cores(sums)
    (updates,) = call(
        last_kernel, [((NEWTON, 8, SLICE), f32)],
        drift, *image, sums, sums_other, update, scratch=turn,
    )
    return updates


def solution(mesh):
    torus = Mesh(mesh.devices.reshape(4, 4, 2, mesh.shape["dim"]), AXES)
    groups = ("y", "x", "c")
    in_specs = (P(groups, "z"), P(groups, None, "z"), P(groups, None))
    out_specs = P(None, groups, "z")

    return jax.shard_map(
        per_device, mesh=torus, in_specs=in_specs, out_specs=out_specs, check_vma=False
    )
```

```python
from functools import partial

import jax
import jax.numpy as jnp
import numpy as np
from jax import lax
from jax.experimental import pallas as pl
from jax.experimental.pallas import tpu as pltpu
from jax.sharding import Mesh
from jax.sharding import PartitionSpec as P


AXES = ("y", "x", "c", "z")
NEWTON = 2
prior_precision = 0.05
like_weight = 4.0
move_size = 0.5

f32 = jnp.float32
bf16 = jnp.bfloat16
WIDE = 1024
MANY = 256
HALF = 128
DATA = 16
SLICE = 256
scale = 1.0 * WIDE
cross = 4.0 / (scale * scale)

MASKS = (1, 3)
ORDERS = ("xyz", "yzx", "zxy")
SPOT = {"y": 0, "x": 1, "z": 3}
THIRDS = (96, 0, 48)
FIRSTS = (6, 0, 3)
ROWS = (512, 768, 768)
STARTS = (0, 512, 1280)
CHUNK = 256
LONG_CHUNK = 256


def places():
    return np.ndindex(4, 4, 2, 4)


def spot(at):
    return int(np.ravel_multi_index(at, (4, 4, 2, 4)))


def pairs(axis):
    out = []
    for at in places():
        to = list(at)
        to[SPOT[axis]] ^= MASKS[1 - at[2]]
        out.append((spot(at), spot(to)))
    return out


def cubes():
    groups = {}
    for at in places():
        mask = MASKS[at[2]]
        key = (at[2],) + tuple(min(at[d], at[d] ^ mask) for d in (0, 1, 3))
        groups.setdefault(key, []).append(spot(at))
    return list(groups.values())


def swap_cores(x):
    return lax.ppermute(x, "c", [(0, 1), (1, 0)])


def gathered(copies):
    cube = lax.all_to_all(copies, AXES, 0, 0, axis_index_groups=cubes(), tiled=True)
    parts = [cube[:, k : k + 48] for k in THIRDS]

    def sent(parts, step):
        out = []
        for part, order in zip(parts, ORDERS):
            out.append(lax.ppermute(part, AXES, pairs(order[step])))
        return out

    near = [jnp.concatenate(both, axis=0) for both in zip(parts, sent(parts, 0))]
    aside = sent(near, 1)
    far = sent(near, 2)
    last = sent(aside, 2)
    return list(zip(near, aside, far, last))


def two(v):
    high = v.astype(bf16)
    return high, (v - high.astype(f32)).astype(bf16)


def nn(a, b):
    return lax.dot_general(a, b, (((1,), (0,)), ((), ())), preferred_element_type=f32)


def tn(a, b):
    return lax.dot_general(a, b, (((0,), (0,)), ((), ())), preferred_element_type=f32)


def stacked(a, b):
    left = jnp.concatenate([a[0], a[1], a[0]], axis=1)
    right = jnp.concatenate([b[0], b[0], b[1]], axis=0)
    return nn(left, right)


def own_place():
    y, x = lax.axis_index("y"), lax.axis_index("x")
    shift = lax.axis_index("c")
    return ((y >> shift) & 1) * 4 + ((x >> shift) & 1)


def slice_at(k):
    core, z = lax.axis_index("c"), lax.axis_index("z")
    seen = (0, 3, 1, 2)
    turned = (z ^ (z >> 1)) & 1
    return jnp.where(core == 0, k ^ (z & 2), jnp.where(turned == 1, seen[k ^ 2], seen[k]))


def cols(k):
    return slice(k * SLICE, (k + 1) * SLICE)


def span(color):
    return slice(STARTS[color], STARTS[color] + ROWS[color])


def owner_of(row):
    color = sum(row >= s for s in STARTS[1:])
    count = ROWS[color] // 256
    group = (row - STARTS[color]) // DATA
    return group // count * 8 + FIRSTS[color] + group % count


def half_of(core):
    return pl.ds(pl.multiple_of(core * HALF, HALF), HALF)


def in_order(core, own, other, axis):
    pair = jnp.where(core == 0, own, other), jnp.where(core == 0, other, own)
    return jnp.concatenate(pair, axis=axis)


def prepare_kernel(x_far, rows_far, labels_far, out_ref, x_ref, rows_ref, labels_ref, done):
    copies = [
        pltpu.make_async_copy(far, near, done.at[k])
        for k, (far, near) in enumerate(
            ((x_far, x_ref), (rows_far, rows_ref), (labels_far, labels_ref))
        )
    ]
    for copy in copies:
        copy.start()
    for copy in copies:
        copy.wait()
    sign = (2 * labels_ref[...] - 1).astype(f32).T
    pieces = [rows_ref[p].astype(f32) * sign[:, p : p + 1] for p in range(8)]
    whole = jnp.concatenate([p.astype(bf16) for p in pieces] + list(two(x_ref[...])), axis=0)
    for k in range(8):
        out_ref[k] = whole


def land(color, refs, arrived, rows_ref, tail_ref):
    count = ROWS[color] // 16
    order = ORDERS[color]
    for k in range(4):
        slot = pl.ds(pl.multiple_of(slice_at(k) * SLICE, SLICE), SLICE)
        for at in range(16):
            step = {"z": k >> 1, "y": at >> 3, "x": (at >> 1) & 1}
            which = step[order[2]] * 2 + step[order[1]]
            if which not in arrived:
                continue
            unit = step[order[0]] * 8 + ((at >> 2) & 1) * 4 + (at & 1) * 2 + (k & 1)
            ref = refs[which]
            start = STARTS[color] + at * count
            rows_ref[start : start + count, slot] = ref[unit, :count, :]
            if color == 0:
                high, low = ref[unit, 32:40, :], ref[unit, 40:48, :]
                tail_ref[at * 8 : at * 8 + 8, slot] = high.astype(f32) + low.astype(f32)


def early_kernel(*refs):
    rows_ref, tail_ref, hot_ref = refs[9:]
    for color in range(3):
        land(color, refs[3 * color : 3 * color + 3], (0, 1, 2), rows_ref, tail_ref)
        count = ROWS[color] // 16
        row = lax.broadcasted_iota(jnp.int32, (ROWS[color], HALF), 0)
        place = (row * 43691) >> 21 if count == 48 else row >> 5
        owner = place * 8 + FIRSTS[color] + ((row - place * count) >> 4)
        hot = owner == lax.broadcasted_iota(jnp.int32, (ROWS[color], HALF), 1)
        hot_ref[span(color), :] = jnp.where(hot, 1.0, 0.0).astype(bf16)


def gradient(rows_ref, hot_ref, x, curve_ref, start, stop):
    both = jnp.concatenate(two(x), axis=1)
    weights = []
    for at in range(start, stop, CHUNK):
        part = pl.ds(at, CHUNK)
        logit = nn(rows_ref[part, :], both)
        hot = hot_ref[part, :].astype(f32)
        logit = jnp.sum((logit[:, :HALF] + logit[:, HALF:]) * hot, axis=1, keepdims=True)
        prob = 1.0 / (1.0 + jnp.exp(logit))
        curve_ref[part, :] = jnp.broadcast_to(like_weight * prob * (1.0 - prob), (CHUNK, HALF))
        weights.append(jnp.concatenate(two(like_weight * prob * hot), axis=1))
    total = tn(rows_ref[start:stop, :], jnp.concatenate(weights, axis=0))
    return total[:, :HALF] + total[:, HALF:]


def position_kernel(_, __, hot_ref, d, rows_ref, tail_ref, x_ref, grad_ref, curve_ref):
    land(0, (None, None, None, d), (3,), rows_ref, tail_ref)
    for k in range(4):
        x_ref[cols(k), :] = tail_ref[:, cols(k)].T
    x = x_ref[...]
    part = gradient(rows_ref, hot_ref, x, curve_ref, 0, ROWS[0])
    grad_ref[...] = part - (prior_precision + 2.0 / scale) * x


def grad_kernel(color, _, before_ref, __, hot_ref, x_ref, d, rows_ref, grad_ref, curve_ref):
    land(color, (None, None, None, d), (3,), rows_ref, None)
    start = STARTS[color]
    part = gradient(rows_ref, hot_ref, x_ref[...], curve_ref, start, start + ROWS[color])
    grad_ref[...] = before_ref[...] + part


def factors(own_ref, other_ref):
    mu0, mu1, mu2 = (own_ref[k : k + 1, :1] for k in range(3))
    mu3 = own_ref[3:4, :1] + other_ref[3:4, :1]
    alpha = mu0 / mu1
    left = mu0 - 2.0 * alpha * mu1 + alpha * alpha * mu2
    grown = 1.0 + left / mu0
    gamma = left / (grown * grown * mu1 - 2.0 * grown * alpha * mu2 + alpha * alpha * mu3)
    return alpha + gamma * grown, -gamma * alpha


def own_kernel(drift_ref, image_a, image_b, out_ref, turn_ref):
    mine = half_of(lax.axis_index("c"))
    z = lax.axis_index("z")
    own = pl.ds(pl.multiple_of(z * SLICE, SLICE), SLICE)
    near = pl.ds(pl.multiple_of((z & 1) * SLICE, SLICE), SLICE)
    image = jnp.where(z < 2, image_a[near, mine], image_b[near, mine])
    for k, value in enumerate((drift_ref[own, mine], image)):
        turn_ref[...] = value.T
        out_ref[k] = turn_ref[pl.ds(pl.multiple_of(own_place() * 8, 8), 8), :]


def next_kernel(
    rows_ref, hot_ref, x_ref, drift_ref, image_a, image_b, own_ref, other_ref,
    grad_ref, curve_ref, new_ref, factors_ref,
):
    on_drift, on_image = factors(own_ref, other_ref)
    factors_ref[0:1, :] = jnp.broadcast_to(on_drift, (1, HALF))
    factors_ref[1:2, :] = jnp.broadcast_to(on_image, (1, HALF))
    factors_ref[2:, :] = jnp.zeros((6, HALF), f32)
    for k, image_ref in enumerate((image_a, image_b)):
        near = slice(k * WIDE // 2, (k + 1) * WIDE // 2)
        update = on_drift * drift_ref[near, :] + on_image * image_ref[...]
        new_ref[near, :] = x_ref[near, :] + move_size * update
    x = new_ref[:, half_of(lax.axis_index("c"))]
    part = gradient(rows_ref, hot_ref, x, curve_ref, 0, HALF * DATA)
    grad_ref[...] = part - (prior_precision + 2.0 / scale) * x


def last_kernel(before_ref, factors_ref, own_ref, sums_ref, other_ref, out_ref):
    out_ref[0] = factors_ref[:1, :1] * before_ref[0] + factors_ref[1:2, :1] * before_ref[1]
    on_drift, on_image = factors(sums_ref, other_ref)
    out_ref[1] = on_drift * own_ref[0] + on_image * own_ref[1]


def similarity(x, grad_ref, kernel_ref, drift_ref):
    high, low = two(x)
    gram = tn(high, high) + (tn(high, low) + tn(low, high))
    shape = (MANY, MANY)
    same = lax.broadcasted_iota(jnp.int32, shape, 0) == lax.broadcasted_iota(jnp.int32, shape, 1)
    diag = jnp.where(same, gram, 0.0)
    squares = jnp.sum(diag, axis=1, keepdims=True) + jnp.sum(diag, axis=0, keepdims=True)
    kernel = jnp.exp((2.0 * gram - squares) / scale)
    kernel_ref[...] = kernel
    total = jnp.sum(kernel, axis=0, keepdims=True)
    own = two(kernel_ref[half_of(lax.axis_index("c")), :])
    drift_ref[...] = (2.0 / scale) * total * x + stacked(two(grad_ref[...]), own)


def start_kernel(grad_ref, own_ref, other_ref, kernel_ref, drift_ref, x_ref):
    x = in_order(lax.axis_index("c"), own_ref[...], other_ref[...], 1)
    x_ref[...] = x
    similarity(x, grad_ref, kernel_ref, drift_ref)


def again_kernel(grad_ref, x_ref, kernel_ref, drift_ref):
    similarity(x_ref[...], grad_ref, kernel_ref, drift_ref)


def spread(rows_ref, weighted_ref, near):
    return sum(
        tn(rows_ref[span(color), near], weighted_ref[k, span(color), :])
        for color in range(3)
        for k in range(2)
    )


def image_part(rows_ref, near, x_ref, drift, square, q, weighted_ref):
    mine = half_of(lax.axis_index("c"))
    pull = x_ref[near, :] * jnp.sum(q, axis=0, keepdims=True)
    pull = pull - stacked(two(x_ref[near, mine]), two(q))
    own = prior_precision * jnp.sum(square, axis=0, keepdims=True) * drift
    return (spread(rows_ref, weighted_ref, near) + (own + cross * pull)) / MANY


def first_kernel(
    rows_ref, curve_ref, x_ref, kernel_ref, own_ref, other_ref,
    drift_ref, image_ref, factor_ref, weighted_ref, q_ref, square_ref,
):
    core = lax.axis_index("c")
    mine = half_of(core)
    x = x_ref[...]
    drift = (own_ref[...] + stacked(two(other_ref[...]), two(kernel_ref[half_of(1 - core), :]))) / MANY
    drift_ref[...] = drift
    drift_two = two(drift)
    kernel_own = kernel_ref[mine, :]
    square = kernel_own * kernel_own
    square_ref[...] = square
    for at in range(0, HALF * DATA, LONG_CHUNK):
        to = pl.ds(at, LONG_CHUNK)
        pieces = []
        for start in range(at, at + LONG_CHUNK, DATA):
            j = owner_of(start)
            curve = curve_ref[pl.ds(start, DATA), :]
            wide = jnp.concatenate([curve, curve], axis=1)
            pieces.append(jnp.broadcast_to(square_ref[j : j + 1, :], wide.shape) * wide)
        factor = jnp.concatenate(pieces, axis=0)
        factor_ref[to, :] = factor
        rows = rows_ref[to, :]
        high, low = two((nn(rows, drift_two[0]) + nn(rows, drift_two[1])) * factor)
        weighted_ref[0, to, :] = high
        weighted_ref[1, to, :] = low
    along = stacked(two(x_ref[:, mine].T), drift_two)
    q = square * (jnp.sum(x * drift, axis=0, keepdims=True) - along)
    q_ref[...] = q
    near = slice(0, WIDE // 2)
    image_ref[...] = image_part(rows_ref, near, x_ref, drift[near], square, q, weighted_ref)


def rest_kernel(rows_ref, x_ref, kernel_ref, drift_ref, weighted_ref, q_ref, image_ref):
    kernel_own = kernel_ref[half_of(lax.axis_index("c")), :]
    near = slice(WIDE // 2, WIDE)
    image_ref[...] = image_part(
        rows_ref, near, x_ref, drift_ref[near, :], kernel_own * kernel_own, q_ref[...],
        weighted_ref,
    )


def read_image(near, x_ref, drift_ref, image):
    rounded = image.astype(bf16)
    wide = rounded.astype(f32)
    pairs_ = (
        (drift_ref[near, :], drift_ref[near, :]),
        (drift_ref[near, :], image),
        (image, image),
        (image, wide),
        (wide, wide),
        (x_ref[near, :], image),
    )
    sums = [jnp.sum(a * b, axis=0, keepdims=True) for a, b in pairs_]
    x_own = x_ref[near, half_of(lax.axis_index("c"))]
    return sums, stacked(two(x_own.T), two(image)), rounded


def second_kernel(
    rows_ref, x_ref, drift_ref, own_ref, other_ref,
    image_ref, projected_ref, along_ref, sums_ref,
):
    near = slice(0, WIDE // 2)
    image = own_ref[...] + other_ref[...]
    image_ref[...] = image
    sums, along, rounded = read_image(near, x_ref, drift_ref, image)
    along_ref[...] = along
    for at, value in enumerate(sums):
        sums_ref[at : at + 1, :] = value
    sums_ref[6:, :] = jnp.zeros((2, MANY), f32)
    projected_ref[...] = nn(rows_ref[:, near], rounded)


def third_kernel(
    rows_ref, x_ref, kernel_ref, factor_ref, drift_ref, projected_ref, along_ref, before_ref,
    own_ref, other_ref,
    image_ref, sums_ref,
):
    near = slice(WIDE // 2, WIDE)
    image = own_ref[...] + other_ref[...]
    image_ref[...] = image
    sums, along, rounded = read_image(near, x_ref, drift_ref, image)
    sums = [value + before_ref[at : at + 1, :] for at, value in enumerate(sums)]
    total = jnp.zeros((1, MANY), f32)
    for at in range(0, HALF * DATA, CHUNK):
        to = pl.ds(at, CHUNK)
        projected = projected_ref[to, :] + nn(rows_ref[to, near], rounded)
        total += jnp.sum(projected * projected * factor_ref[to, :], axis=0, keepdims=True)
    fit = sums[3] / jnp.maximum(sums[4], 1e-30)
    total *= fit * fit
    mine = half_of(lax.axis_index("c"))
    square = kernel_ref[mine, :] * kernel_ref[mine, :]
    gap = sums[5] - (along + along_ref[...])
    total += cross * jnp.sum(square * gap * gap, axis=0, keepdims=True)
    total += prior_precision * jnp.sum(square, axis=0, keepdims=True) * sums[2]
    for at, value in enumerate((*sums[:3], total / MANY)):
        sums_ref[at : at + 1, :] = jnp.broadcast_to(
            jnp.sum(value, axis=1, keepdims=True), (1, HALF)
        )
    sums_ref[4:, :] = jnp.zeros((4, HALF), f32)


def call(kernel, outs, *args, scratch=(), far=False, aliases=None):
    whole = pl.BlockSpec(memory_space=pltpu.VMEM)
    return pl.pallas_call(
        kernel,
        out_shape=[pltpu.VMEM(s, t) if far else jax.ShapeDtypeStruct(s, t) for s, t in outs],
        in_specs=[pl.BlockSpec(memory_space=pltpu.HBM) if far else whole] * len(args),
        out_specs=[whole] * len(outs),
        scratch_shapes=scratch,
        input_output_aliases=aliases or {},
        compiler_params=pltpu.CompilerParams(vmem_limit_bytes=(60 if far else 24) * 1024 * 1024),
    )(*args)


def per_device(particles, data_rows, labels):
    (copies,) = call(
        prepare_kernel,
        [((8, 8 * DATA + 16, SLICE), bf16)],
        particles, data_rows, labels,
        scratch=[
            pltpu.VMEM((8, SLICE), f32),
            pltpu.VMEM((8, DATA, SLICE), bf16),
            pltpu.VMEM((8, DATA), jnp.int32),
            pltpu.SemaphoreType.DMA((3,)),
        ],
        far=True,
    )
    pieces = gathered(copies)
    count = HALF * DATA
    tall = ((count, MANY), f32)
    square = ((MANY, MANY), f32)
    long = ((WIDE, MANY), f32)
    wing = ((WIDE // 2, MANY), f32)
    low = ((HALF, MANY), f32)
    half = ((WIDE, HALF), f32)
    turn = [pltpu.VMEM((HALF, SLICE), f32)]
    rows_of = ((count, WIDE), bf16)
    tail_of = ((HALF, WIDE), f32)
    curve_of = ((count, HALF), f32)
    rows, tail, hot = call(
        early_kernel,
        [rows_of, tail_of, ((count, HALF), bf16)],
        *(a for four in pieces for a in four[:3]),
    )
    rows, tail, x_own, grad, curve = call(
        position_kernel,
        [rows_of, tail_of, half, half, curve_of],
        rows, tail, hot, pieces[0][3],
        aliases={0: 0, 1: 1},
    )
    x_other = swap_cores(x_own)
    for color in (1, 2):
        rows, grad, curve = call(
            partial(grad_kernel, color),
            [rows_of, half, curve_of],
            rows, grad, curve, hot, x_own, pieces[color][3],
            aliases={0: 0, 1: 1, 2: 2},
        )
    kernel, partial_drift, x = call(
        start_kernel, [square, long, long], grad, x_own, x_other
    )
    own = []
    for newton_step in range(NEWTON):
        if newton_step > 0:
            grad, curve, x, weights = call(
                next_kernel, [half, curve_of, long, ((8, HALF), f32)],
                rows, hot, x, drift, *image, sums, sums_other,
            )
        grad_other = swap_cores(grad)
        if newton_step > 0:
            kernel, partial_drift = call(again_kernel, [square, long], grad, x)
        drift, own_a, factor, weighted, q = call(
            first_kernel,
            [long, wing, tall, ((2, count, MANY), bf16), low],
            rows, curve, x, kernel, partial_drift, grad_other,
            scratch=[pltpu.VMEM((HALF, MANY), f32)],
        )
        other_a = swap_cores(own_a)
        (own_b,) = call(rest_kernel, [wing], rows, x, kernel, drift, weighted, q)
        other_b = swap_cores(own_b)
        image_a, projected, along, partial_sums = call(
            second_kernel, [wing, tall, low, ((8, MANY), f32)],
            rows, x, drift, own_a, other_a,
        )
        image_b, sums = call(
            third_kernel, [wing, ((8, HALF), f32)],
            rows, x, kernel, factor, drift, projected, along, partial_sums, own_b, other_b,
        )
        image = (image_a, image_b)
        sums_other = swap_cores(sums)
        own += call(own_kernel, [((2, 8, SLICE), f32)], drift, *image, scratch=turn)
    (updates,) = call(
        last_kernel, [((NEWTON, 8, SLICE), f32)], own[0], weights, own[1], sums, sums_other
    )
    return updates


def solution(mesh):
    torus = Mesh(mesh.devices.reshape(4, 4, 2, mesh.shape["dim"]), AXES)
    groups = ("y", "x", "c")
    in_specs = (P(groups, "z"), P(groups, None, "z"), P(groups, None))
    out_specs = P(None, groups, "z")

    return jax.shard_map(
        per_device, mesh=torus, in_specs=in_specs, out_specs=out_specs, check_vma=False
    )
```

```python
from functools import partial

import jax
import jax.numpy as jnp
import numpy as np
from jax import lax
from jax.experimental import pallas as pl
from jax.experimental.pallas import tpu as pltpu
from jax.sharding import Mesh
from jax.sharding import PartitionSpec as P


AXES = ("y", "x", "c", "z")
NEWTON = 2
prior_precision = 0.05
like_weight = 4.0
move_size = 0.5

f32 = jnp.float32
bf16 = jnp.bfloat16
WIDE = 1024
MANY = 256
HALF = 128
DATA = 16
SLICE = 256
scale = 1.0 * WIDE
cross = 4.0 / (scale * scale)

MASKS = (1, 3)
ORDERS = ("xyz", "yzx", "zxy")
SPOT = {"y": 0, "x": 1, "z": 3}
THIRDS = (96, 0, 48)
FIRSTS = (6, 0, 3)
ROWS = (512, 768, 768)
STARTS = (0, 512, 1280)
CHUNK = 256
LONG_CHUNK = 512


def places():
    return np.ndindex(4, 4, 2, 4)


def spot(at):
    return int(np.ravel_multi_index(at, (4, 4, 2, 4)))


def pairs(axis):
    out = []
    for at in places():
        to = list(at)
        to[SPOT[axis]] ^= MASKS[1 - at[2]]
        out.append((spot(at), spot(to)))
    return out


def cubes():
    groups = {}
    for at in places():
        mask = MASKS[at[2]]
        key = (at[2],) + tuple(min(at[d], at[d] ^ mask) for d in (0, 1, 3))
        groups.setdefault(key, []).append(spot(at))
    return list(groups.values())


def swap_cores(x):
    return lax.ppermute(x, "c", [(0, 1), (1, 0)])


def gathered(copies):
    cube = lax.all_to_all(copies, AXES, 0, 0, axis_index_groups=cubes(), tiled=True)
    parts = [cube[:, k : k + 48] for k in THIRDS]

    def sent(parts, step):
        out = []
        for part, order in zip(parts, ORDERS):
            out.append(lax.ppermute(part, AXES, pairs(order[step])))
        return out

    near = [jnp.concatenate(both, axis=0) for both in zip(parts, sent(parts, 0))]
    aside = sent(near, 1)
    far = sent(near, 2)
    last = sent(aside, 2)
    return list(zip(near, aside, far, last))


def two(v):
    high = v.astype(bf16)
    return high, (v - high.astype(f32)).astype(bf16)


def nn(a, b):
    return lax.dot_general(a, b, (((1,), (0,)), ((), ())), preferred_element_type=f32)


def tn(a, b):
    return lax.dot_general(a, b, (((0,), (0,)), ((), ())), preferred_element_type=f32)


def stacked(a, b):
    left = jnp.concatenate([a[0], a[1], a[0]], axis=1)
    right = jnp.concatenate([b[0], b[0], b[1]], axis=0)
    return nn(left, right)


def own_place():
    y, x = lax.axis_index("y"), lax.axis_index("x")
    shift = lax.axis_index("c")
    return ((y >> shift) & 1) * 4 + ((x >> shift) & 1)


def slice_at(k):
    core, z = lax.axis_index("c"), lax.axis_index("z")
    seen = (0, 3, 1, 2)
    turned = (z ^ (z >> 1)) & 1
    return jnp.where(core == 0, k ^ (z & 2), jnp.where(turned == 1, seen[k ^ 2], seen[k]))


def cols(k):
    return slice(k * SLICE, (k + 1) * SLICE)


def span(color):
    return slice(STARTS[color], STARTS[color] + ROWS[color])


def owner_of(row):
    color = sum(row >= s for s in STARTS[1:])
    count = ROWS[color] // 256
    group = (row - STARTS[color]) // DATA
    return group // count * 8 + FIRSTS[color] + group % count


def half_of(core):
    return pl.ds(pl.multiple_of(core * HALF, HALF), HALF)


def in_order(core, own, other, axis):
    pair = jnp.where(core == 0, own, other), jnp.where(core == 0, other, own)
    return jnp.concatenate(pair, axis=axis)


def prepare_kernel(x_far, rows_far, labels_far, out_ref, x_ref, rows_ref, labels_ref, done):
    copies = [
        pltpu.make_async_copy(far, near, done.at[k])
        for k, (far, near) in enumerate(
            ((x_far, x_ref), (rows_far, rows_ref), (labels_far, labels_ref))
        )
    ]
    for copy in copies:
        copy.start()
    for copy in copies:
        copy.wait()
    sign = (2 * labels_ref[...] - 1).astype(f32).T
    pieces = [rows_ref[p].astype(f32) * sign[:, p : p + 1] for p in range(8)]
    whole = jnp.concatenate([p.astype(bf16) for p in pieces] + list(two(x_ref[...])), axis=0)
    for k in range(8):
        out_ref[k] = whole


def land(color, refs, arrived, rows_ref, tail_ref):
    count = ROWS[color] // 16
    order = ORDERS[color]
    for k in range(4):
        slot = pl.ds(pl.multiple_of(slice_at(k) * SLICE, SLICE), SLICE)
        for at in range(16):
            step = {"z": k >> 1, "y": at >> 3, "x": (at >> 1) & 1}
            which = step[order[2]] * 2 + step[order[1]]
            if which not in arrived:
                continue
            unit = step[order[0]] * 8 + ((at >> 2) & 1) * 4 + (at & 1) * 2 + (k & 1)
            ref = refs[which]
            start = STARTS[color] + at * count
            rows_ref[start : start + count, slot] = ref[unit, :count, :]
            if color == 0:
                high, low = ref[unit, 32:40, :], ref[unit, 40:48, :]
                tail_ref[at * 8 : at * 8 + 8, slot] = high.astype(f32) + low.astype(f32)


def early_kernel(*refs):
    rows_ref, tail_ref, hot_ref = refs[9:]
    for color in range(3):
        land(color, refs[3 * color : 3 * color + 3], (0, 1, 2), rows_ref, tail_ref)
        count = ROWS[color] // 16
        row = lax.broadcasted_iota(jnp.int32, (ROWS[color], HALF), 0)
        place = (row * 43691) >> 21 if count == 48 else row >> 5
        owner = place * 8 + FIRSTS[color] + ((row - place * count) >> 4)
        hot = owner == lax.broadcasted_iota(jnp.int32, (ROWS[color], HALF), 1)
        hot_ref[span(color), :] = jnp.where(hot, 1.0, 0.0).astype(bf16)


def gradient(rows_ref, hot_ref, x, curve_ref, start, stop):
    both = jnp.concatenate(two(x), axis=1)
    weights = []
    for at in range(start, stop, CHUNK):
        part = pl.ds(at, CHUNK)
        logit = nn(rows_ref[part, :], both)
        hot = hot_ref[part, :].astype(f32)
        logit = jnp.sum((logit[:, :HALF] + logit[:, HALF:]) * hot, axis=1, keepdims=True)
        prob = 1.0 / (1.0 + jnp.exp(logit))
        curve_ref[part, :] = jnp.broadcast_to(like_weight * prob * (1.0 - prob), (CHUNK, HALF))
        weights.append(jnp.concatenate(two(like_weight * prob * hot), axis=1))
    weights = jnp.concatenate(weights, axis=0)
    halves = (slice(0, WIDE // 2), slice(WIDE // 2, WIDE))
    total = [tn(rows_ref[start:stop, near], weights) for near in halves]
    return jnp.concatenate([t[:, :HALF] + t[:, HALF:] for t in total], axis=0)


def position_kernel(_, __, hot_ref, d, rows_ref, tail_ref, x_ref, grad_ref, curve_ref):
    land(0, (None, None, None, d), (3,), rows_ref, tail_ref)
    for k in range(4):
        x_ref[cols(k), :] = tail_ref[:, cols(k)].T
    x = x_ref[...]
    part = gradient(rows_ref, hot_ref, x, curve_ref, 0, ROWS[0])
    grad_ref[...] = part - (prior_precision + 2.0 / scale) * x


def grad_kernel(color, _, before_ref, __, hot_ref, x_ref, d, rows_ref, grad_ref, curve_ref):
    land(color, (None, None, None, d), (3,), rows_ref, None)
    start = STARTS[color]
    part = gradient(rows_ref, hot_ref, x_ref[...], curve_ref, start, start + ROWS[color])
    grad_ref[...] = before_ref[...] + part


def factors(own_ref, other_ref):
    mu0, mu1, mu2 = (own_ref[k : k + 1, :1] for k in range(3))
    mu3 = own_ref[3:4, :1] + other_ref[3:4, :1]
    alpha = mu0 / mu1
    left = mu0 - 2.0 * alpha * mu1 + alpha * alpha * mu2
    grown = 1.0 + left / mu0
    gamma = left / (grown * grown * mu1 - 2.0 * grown * alpha * mu2 + alpha * alpha * mu3)
    return alpha + gamma * grown, -gamma * alpha


def own_kernel(drift_ref, image_a, image_b, out_ref, turn_ref):
    mine = half_of(lax.axis_index("c"))
    z = lax.axis_index("z")
    own = pl.ds(pl.multiple_of(z * SLICE, SLICE), SLICE)
    near = pl.ds(pl.multiple_of((z & 1) * SLICE, SLICE), SLICE)
    image = jnp.where(z < 2, image_a[near, mine], image_b[near, mine])
    for k, value in enumerate((drift_ref[own, mine], image)):
        turn_ref[...] = value.T
        out_ref[k] = turn_ref[pl.ds(pl.multiple_of(own_place() * 8, 8), 8), :]


def next_kernel(
    rows_ref, hot_ref, x_ref, drift_ref, image_a, image_b, own_ref, other_ref,
    grad_ref, curve_ref, new_ref, factors_ref,
):
    on_drift, on_image = factors(own_ref, other_ref)
    factors_ref[0:1, :] = jnp.broadcast_to(on_drift, (1, HALF))
    factors_ref[1:2, :] = jnp.broadcast_to(on_image, (1, HALF))
    factors_ref[2:, :] = jnp.zeros((6, HALF), f32)
    for k, image_ref in enumerate((image_a, image_b)):
        near = slice(k * WIDE // 2, (k + 1) * WIDE // 2)
        update = on_drift * drift_ref[near, :] + on_image * image_ref[...]
        new_ref[near, :] = x_ref[near, :] + move_size * update
    x = new_ref[:, half_of(lax.axis_index("c"))]
    part = gradient(rows_ref, hot_ref, x, curve_ref, 0, HALF * DATA)
    grad_ref[...] = part - (prior_precision + 2.0 / scale) * x


def last_kernel(before_ref, factors_ref, own_ref, sums_ref, other_ref, out_ref):
    out_ref[0] = factors_ref[:1, :1] * before_ref[0] + factors_ref[1:2, :1] * before_ref[1]
    on_drift, on_image = factors(sums_ref, other_ref)
    out_ref[1] = on_drift * own_ref[0] + on_image * own_ref[1]


def similarity(x, grad_ref, kernel_ref, drift_ref):
    high, low = two(x)
    gram = tn(high, high) + (tn(high, low) + tn(low, high))
    shape = (MANY, MANY)
    same = lax.broadcasted_iota(jnp.int32, shape, 0) == lax.broadcasted_iota(jnp.int32, shape, 1)
    diag = jnp.where(same, gram, 0.0)
    squares = jnp.sum(diag, axis=1, keepdims=True) + jnp.sum(diag, axis=0, keepdims=True)
    kernel = jnp.exp((2.0 * gram - squares) / scale)
    kernel_ref[...] = kernel
    total = jnp.sum(kernel, axis=0, keepdims=True)
    own = two(kernel_ref[half_of(lax.axis_index("c")), :])
    drift_ref[...] = (2.0 / scale) * total * x + stacked(two(grad_ref[...]), own)


def start_kernel(grad_ref, own_ref, other_ref, kernel_ref, drift_ref, x_ref):
    x = in_order(lax.axis_index("c"), own_ref[...], other_ref[...], 1)
    x_ref[...] = x
    similarity(x, grad_ref, kernel_ref, drift_ref)


def again_kernel(grad_ref, x_ref, kernel_ref, drift_ref):
    similarity(x_ref[...], grad_ref, kernel_ref, drift_ref)


def spread(rows_ref, weighted_ref, near):
    return sum(
        tn(rows_ref[span(color), near], weighted_ref[k, span(color), :])
        for color in range(3)
        for k in range(2)
    )


def image_part(rows_ref, near, x_ref, drift, square, q, weighted_ref):
    mine = half_of(lax.axis_index("c"))
    pull = x_ref[near, :] * jnp.sum(q, axis=0, keepdims=True)
    pull = pull - stacked(two(x_ref[near, mine]), two(q))
    own = prior_precision * jnp.sum(square, axis=0, keepdims=True) * drift
    return (spread(rows_ref, weighted_ref, near) + (own + cross * pull)) / MANY


def first_kernel(
    rows_ref, curve_ref, x_ref, kernel_ref, own_ref, other_ref,
    drift_ref, image_ref, factor_ref, weighted_ref, q_ref, square_ref,
):
    core = lax.axis_index("c")
    mine = half_of(core)
    x = x_ref[...]
    drift = (own_ref[...] + stacked(two(other_ref[...]), two(kernel_ref[half_of(1 - core), :]))) / MANY
    drift_ref[...] = drift
    drift_two = two(drift)
    kernel_own = kernel_ref[mine, :]
    square = kernel_own * kernel_own
    square_ref[...] = square
    for at in range(0, HALF * DATA, CHUNK):
        to = pl.ds(at, CHUNK)
        pieces = []
        for start in range(at, at + CHUNK, DATA):
            j = owner_of(start)
            curve = curve_ref[pl.ds(start, DATA), :]
            wide = jnp.concatenate([curve, curve], axis=1)
            pieces.append(jnp.broadcast_to(square_ref[j : j + 1, :], wide.shape) * wide)
        factor = jnp.concatenate(pieces, axis=0)
        factor_ref[to, :] = factor
        rows = rows_ref[to, :]
        high, low = two((nn(rows, drift_two[0]) + nn(rows, drift_two[1])) * factor)
        weighted_ref[0, to, :] = high
        weighted_ref[1, to, :] = low
    along = stacked(two(x_ref[:, mine].T), drift_two)
    q = square * (jnp.sum(x * drift, axis=0, keepdims=True) - along)
    q_ref[...] = q
    near = slice(0, WIDE // 2)
    image_ref[...] = image_part(rows_ref, near, x_ref, drift[near], square, q, weighted_ref)


def rest_kernel(rows_ref, x_ref, kernel_ref, drift_ref, weighted_ref, q_ref, image_ref):
    kernel_own = kernel_ref[half_of(lax.axis_index("c")), :]
    near = slice(WIDE // 2, WIDE)
    image_ref[...] = image_part(
        rows_ref, near, x_ref, drift_ref[near, :], kernel_own * kernel_own, q_ref[...],
        weighted_ref,
    )


def read_image(near, x_ref, drift_ref, image):
    rounded = image.astype(bf16)
    wide = rounded.astype(f32)
    pairs_ = (
        (drift_ref[near, :], drift_ref[near, :]),
        (drift_ref[near, :], image),
        (image, image),
        (image, wide),
        (wide, wide),
        (x_ref[near, :], image),
    )
    sums = [jnp.sum(a * b, axis=0, keepdims=True) for a, b in pairs_]
    x_own = x_ref[near, half_of(lax.axis_index("c"))]
    return sums, stacked(two(x_own.T), two(image)), rounded


def second_kernel(
    rows_ref, x_ref, drift_ref, own_ref, other_ref,
    image_ref, projected_ref, along_ref, sums_ref,
):
    near = slice(0, WIDE // 2)
    image = own_ref[...] + other_ref[...]
    image_ref[...] = image
    sums, along, rounded = read_image(near, x_ref, drift_ref, image)
    along_ref[...] = along
    for at, value in enumerate(sums):
        sums_ref[at : at + 1, :] = value
    sums_ref[6:, :] = jnp.zeros((2, MANY), f32)
    projected_ref[...] = nn(rows_ref[:, near], rounded)


def third_kernel(
    rows_ref, x_ref, kernel_ref, factor_ref, drift_ref, projected_ref, along_ref, before_ref,
    own_ref, other_ref,
    image_ref, sums_ref,
):
    near = slice(WIDE // 2, WIDE)
    image = own_ref[...] + other_ref[...]
    image_ref[...] = image
    sums, along, rounded = read_image(near, x_ref, drift_ref, image)
    sums = [value + before_ref[at : at + 1, :] for at, value in enumerate(sums)]
    total = jnp.zeros((1, MANY), f32)
    for at in range(0, HALF * DATA, LONG_CHUNK):
        to = pl.ds(at, LONG_CHUNK)
        projected = projected_ref[to, :] + nn(rows_ref[to, near], rounded)
        total += jnp.sum(projected * projected * factor_ref[to, :], axis=0, keepdims=True)
    fit = sums[3] / jnp.maximum(sums[4], 1e-30)
    total *= fit * fit
    mine = half_of(lax.axis_index("c"))
    square = kernel_ref[mine, :] * kernel_ref[mine, :]
    gap = sums[5] - (along + along_ref[...])
    total += cross * jnp.sum(square * gap * gap, axis=0, keepdims=True)
    total += prior_precision * jnp.sum(square, axis=0, keepdims=True) * sums[2]
    for at, value in enumerate((*sums[:3], total / MANY)):
        sums_ref[at : at + 1, :] = jnp.broadcast_to(
            jnp.sum(value, axis=1, keepdims=True), (1, HALF)
        )
    sums_ref[4:, :] = jnp.zeros((4, HALF), f32)


def call(kernel, outs, *args, scratch=(), far=False, aliases=None):
    whole = pl.BlockSpec(memory_space=pltpu.VMEM)
    return pl.pallas_call(
        kernel,
        out_shape=[pltpu.VMEM(s, t) if far else jax.ShapeDtypeStruct(s, t) for s, t in outs],
        in_specs=[pl.BlockSpec(memory_space=pltpu.HBM) if far else whole] * len(args),
        out_specs=[whole] * len(outs),
        scratch_shapes=scratch,
        input_output_aliases=aliases or {},
        compiler_params=pltpu.CompilerParams(vmem_limit_bytes=(60 if far else 24) * 1024 * 1024),
    )(*args)


def per_device(particles, data_rows, labels):
    (copies,) = call(
        prepare_kernel,
        [((8, 8 * DATA + 16, SLICE), bf16)],
        particles, data_rows, labels,
        scratch=[
            pltpu.VMEM((8, SLICE), f32),
            pltpu.VMEM((8, DATA, SLICE), bf16),
            pltpu.VMEM((8, DATA), jnp.int32),
            pltpu.SemaphoreType.DMA((3,)),
        ],
        far=True,
    )
    pieces = gathered(copies)
    count = HALF * DATA
    tall = ((count, MANY), f32)
    square = ((MANY, MANY), f32)
    long = ((WIDE, MANY), f32)
    wing = ((WIDE // 2, MANY), f32)
    low = ((HALF, MANY), f32)
    half = ((WIDE, HALF), f32)
    turn = [pltpu.VMEM((HALF, SLICE), f32)]
    rows_of = ((count, WIDE), bf16)
    tail_of = ((HALF, WIDE), f32)
    curve_of = ((count, HALF), f32)
    rows, tail, hot = call(
        early_kernel,
        [rows_of, tail_of, ((count, HALF), bf16)],
        *(a for four in pieces for a in four[:3]),
    )
    rows, tail, x_own, grad, curve = call(
        position_kernel,
        [rows_of, tail_of, half, half, curve_of],
        rows, tail, hot, pieces[0][3],
        aliases={0: 0, 1: 1},
    )
    x_other = swap_cores(x_own)
    for color in (1, 2):
        rows, grad, curve = call(
            partial(grad_kernel, color),
            [rows_of, half, curve_of],
            rows, grad, curve, hot, x_own, pieces[color][3],
            aliases={0: 0, 1: 1, 2: 2},
        )
    kernel, partial_drift, x = call(
        start_kernel, [square, long, long], grad, x_own, x_other
    )
    own = []
    for newton_step in range(NEWTON):
        if newton_step > 0:
            grad, curve, x, weights = call(
                next_kernel, [half, curve_of, long, ((8, HALF), f32)],
                rows, hot, x, drift, *image, sums, sums_other,
            )
        grad_other = swap_cores(grad)
        if newton_step > 0:
            kernel, partial_drift = call(again_kernel, [square, long], grad, x)
        drift, own_a, factor, weighted, q = call(
            first_kernel,
            [long, wing, tall, ((2, count, MANY), bf16), low],
            rows, curve, x, kernel, partial_drift, grad_other,
            scratch=[pltpu.VMEM((HALF, MANY), f32)],
        )
        other_a = swap_cores(own_a)
        (own_b,) = call(rest_kernel, [wing], rows, x, kernel, drift, weighted, q)
        other_b = swap_cores(own_b)
        image_a, projected, along, partial_sums = call(
            second_kernel, [wing, tall, low, ((8, MANY), f32)],
            rows, x, drift, own_a, other_a,
        )
        image_b, sums = call(
            third_kernel, [wing, ((8, HALF), f32)],
            rows, x, kernel, factor, drift, projected, along, partial_sums, own_b, other_b,
        )
        image = (image_a, image_b)
        sums_other = swap_cores(sums)
        own += call(own_kernel, [((2, 8, SLICE), f32)], drift, *image, scratch=turn)
    (updates,) = call(
        last_kernel, [((NEWTON, 8, SLICE), f32)], own[0], weights, own[1], sums, sums_other
    )
    return updates


def solution(mesh):
    torus = Mesh(mesh.devices.reshape(4, 4, 2, mesh.shape["dim"]), AXES)
    groups = ("y", "x", "c")
    in_specs = (P(groups, "z"), P(groups, None, "z"), P(groups, None))
    out_specs = P(None, groups, "z")

    return jax.shard_map(
        per_device, mesh=torus, in_specs=in_specs, out_specs=out_specs, check_vma=False
    )
```

```python
from functools import partial

import jax
import jax.numpy as jnp
import numpy as np
from jax import lax
from jax.experimental import pallas as pl
from jax.experimental.pallas import tpu as pltpu
from jax.sharding import Mesh
from jax.sharding import PartitionSpec as P


AXES = ("y", "x", "c", "z")
NEWTON = 2
prior_precision = 0.05
like_weight = 4.0
move_size = 0.5

f32 = jnp.float32
bf16 = jnp.bfloat16
WIDE = 1024
MANY = 256
HALF = 128
DATA = 16
SLICE = 256
scale = 1.0 * WIDE
cross = 4.0 / (scale * scale)

MASKS = (1, 3)
ORDERS = ("xyz", "yzx", "zxy")
SPOT = {"y": 0, "x": 1, "z": 3}
THIRDS = (96, 0, 48)
FIRSTS = (6, 0, 3)
ROWS = (512, 768, 768)
STARTS = (0, 512, 1280)
CHUNK = 256
LONG_CHUNK = 2048


def places():
    return np.ndindex(4, 4, 2, 4)


def spot(at):
    return int(np.ravel_multi_index(at, (4, 4, 2, 4)))


def pairs(axis):
    out = []
    for at in places():
        to = list(at)
        to[SPOT[axis]] ^= MASKS[1 - at[2]]
        out.append((spot(at), spot(to)))
    return out


def cubes():
    groups = {}
    for at in places():
        mask = MASKS[at[2]]
        key = (at[2],) + tuple(min(at[d], at[d] ^ mask) for d in (0, 1, 3))
        groups.setdefault(key, []).append(spot(at))
    return list(groups.values())


def swap_cores(x):
    return lax.ppermute(x, "c", [(0, 1), (1, 0)])


def gathered(copies):
    cube = lax.all_to_all(copies, AXES, 0, 0, axis_index_groups=cubes(), tiled=True)
    parts = [cube[:, k : k + 48] for k in THIRDS]

    def sent(parts, step):
        out = []
        for part, order in zip(parts, ORDERS):
            out.append(lax.ppermute(part, AXES, pairs(order[step])))
        return out

    near = [jnp.concatenate(both, axis=0) for both in zip(parts, sent(parts, 0))]
    aside = sent(near, 1)
    far = sent(near, 2)
    last = sent(aside, 2)
    return list(zip(near, aside, far, last))


def two(v):
    high = v.astype(bf16)
    return high, (v - high.astype(f32)).astype(bf16)


def nn(a, b):
    return lax.dot_general(a, b, (((1,), (0,)), ((), ())), preferred_element_type=f32)


def tn(a, b):
    return lax.dot_general(a, b, (((0,), (0,)), ((), ())), preferred_element_type=f32)


def stacked(a, b):
    left = jnp.concatenate([a[0], a[1], a[0]], axis=1)
    right = jnp.concatenate([b[0], b[0], b[1]], axis=0)
    return nn(left, right)


def own_place():
    y, x = lax.axis_index("y"), lax.axis_index("x")
    shift = lax.axis_index("c")
    return ((y >> shift) & 1) * 4 + ((x >> shift) & 1)


def slice_at(k):
    core, z = lax.axis_index("c"), lax.axis_index("z")
    seen = (0, 3, 1, 2)
    turned = (z ^ (z >> 1)) & 1
    return jnp.where(core == 0, k ^ (z & 2), jnp.where(turned == 1, seen[k ^ 2], seen[k]))


def cols(k):
    return slice(k * SLICE, (k + 1) * SLICE)


def span(color):
    return slice(STARTS[color], STARTS[color] + ROWS[color])


def owner_of(row):
    color = sum(row >= s for s in STARTS[1:])
    count = ROWS[color] // 256
    group = (row - STARTS[color]) // DATA
    return group // count * 8 + FIRSTS[color] + group % count


def half_of(core):
    return pl.ds(pl.multiple_of(core * HALF, HALF), HALF)


def in_order(core, own, other, axis):
    pair = jnp.where(core == 0, own, other), jnp.where(core == 0, other, own)
    return jnp.concatenate(pair, axis=axis)


def prepare_kernel(x_far, rows_far, labels_far, out_ref, x_ref, rows_ref, labels_ref, done):
    copies = [
        pltpu.make_async_copy(far, near, done.at[k])
        for k, (far, near) in enumerate(
            ((x_far, x_ref), (rows_far, rows_ref), (labels_far, labels_ref))
        )
    ]
    for copy in copies:
        copy.start()
    for copy in copies:
        copy.wait()
    sign = (2 * labels_ref[...] - 1).astype(f32).T
    pieces = [rows_ref[p].astype(f32) * sign[:, p : p + 1] for p in range(8)]
    whole = jnp.concatenate([p.astype(bf16) for p in pieces] + list(two(x_ref[...])), axis=0)
    for k in range(8):
        out_ref[k] = whole


def land(color, refs, arrived, rows_ref, tail_ref):
    count = ROWS[color] // 16
    order = ORDERS[color]
    for k in range(4):
        slot = pl.ds(pl.multiple_of(slice_at(k) * SLICE, SLICE), SLICE)
        for at in range(16):
            step = {"z": k >> 1, "y": at >> 3, "x": (at >> 1) & 1}
            which = step[order[2]] * 2 + step[order[1]]
            if which not in arrived:
                continue
            unit = step[order[0]] * 8 + ((at >> 2) & 1) * 4 + (at & 1) * 2 + (k & 1)
            ref = refs[which]
            start = STARTS[color] + at * count
            rows_ref[start : start + count, slot] = ref[unit, :count, :]
            if color == 0:
                high, low = ref[unit, 32:40, :], ref[unit, 40:48, :]
                tail_ref[at * 8 : at * 8 + 8, slot] = high.astype(f32) + low.astype(f32)


def early_kernel(*refs):
    rows_ref, tail_ref, hot_ref = refs[9:]
    for color in range(3):
        land(color, refs[3 * color : 3 * color + 3], (0, 1, 2), rows_ref, tail_ref)
        count = ROWS[color] // 16
        row = lax.broadcasted_iota(jnp.int32, (ROWS[color], HALF), 0)
        place = (row * 43691) >> 21 if count == 48 else row >> 5
        owner = place * 8 + FIRSTS[color] + ((row - place * count) >> 4)
        hot = owner == lax.broadcasted_iota(jnp.int32, (ROWS[color], HALF), 1)
        hot_ref[span(color), :] = jnp.where(hot, 1.0, 0.0).astype(bf16)


def gradient(rows_ref, hot_ref, x, curve_ref, start, stop):
    both = jnp.concatenate(two(x), axis=1)
    weights = []
    for at in range(start, stop, CHUNK):
        part = pl.ds(at, CHUNK)
        logit = nn(rows_ref[part, :], both)
        hot = hot_ref[part, :].astype(f32)
        logit = jnp.sum((logit[:, :HALF] + logit[:, HALF:]) * hot, axis=1, keepdims=True)
        prob = 1.0 / (1.0 + jnp.exp(logit))
        curve_ref[part, :] = jnp.broadcast_to(like_weight * prob * (1.0 - prob), (CHUNK, HALF))
        weights.append(jnp.concatenate(two(like_weight * prob * hot), axis=1))
    weights = jnp.concatenate(weights, axis=0)
    halves = (slice(0, WIDE // 2), slice(WIDE // 2, WIDE))
    total = [tn(rows_ref[start:stop, near], weights) for near in halves]
    return jnp.concatenate([t[:, :HALF] + t[:, HALF:] for t in total], axis=0)


def position_kernel(_, __, hot_ref, d, rows_ref, tail_ref, x_ref, grad_ref, curve_ref):
    land(0, (None, None, None, d), (3,), rows_ref, tail_ref)
    for k in range(4):
        x_ref[cols(k), :] = tail_ref[:, cols(k)].T
    x = x_ref[...]
    part = gradient(rows_ref, hot_ref, x, curve_ref, 0, ROWS[0])
    grad_ref[...] = part - (prior_precision + 2.0 / scale) * x


def grad_kernel(color, _, before_ref, __, hot_ref, x_ref, d, rows_ref, grad_ref, curve_ref):
    land(color, (None, None, None, d), (3,), rows_ref, None)
    start = STARTS[color]
    part = gradient(rows_ref, hot_ref, x_ref[...], curve_ref, start, start + ROWS[color])
    grad_ref[...] = before_ref[...] + part


def factors(own_ref, other_ref):
    mu0, mu1, mu2 = (own_ref[k : k + 1, :1] for k in range(3))
    mu3 = own_ref[3:4, :1] + other_ref[3:4, :1]
    alpha = mu0 / mu1
    left = mu0 - 2.0 * alpha * mu1 + alpha * alpha * mu2
    grown = 1.0 + left / mu0
    gamma = left / (grown * grown * mu1 - 2.0 * grown * alpha * mu2 + alpha * alpha * mu3)
    return alpha + gamma * grown, -gamma * alpha


def own_kernel(drift_ref, image_a, image_b, out_ref, turn_ref):
    mine = half_of(lax.axis_index("c"))
    z = lax.axis_index("z")
    own = pl.ds(pl.multiple_of(z * SLICE, SLICE), SLICE)
    near = pl.ds(pl.multiple_of((z & 1) * SLICE, SLICE), SLICE)
    image = jnp.where(z < 2, image_a[near, mine], image_b[near, mine])
    for k, value in enumerate((drift_ref[own, mine], image)):
        turn_ref[...] = value.T
        out_ref[k] = turn_ref[pl.ds(pl.multiple_of(own_place() * 8, 8), 8), :]


def next_kernel(
    rows_ref, hot_ref, x_ref, drift_ref, image_a, image_b, own_ref, other_ref,
    grad_ref, curve_ref, new_ref, factors_ref,
):
    on_drift, on_image = factors(own_ref, other_ref)
    factors_ref[0:1, :] = jnp.broadcast_to(on_drift, (1, HALF))
    factors_ref[1:2, :] = jnp.broadcast_to(on_image, (1, HALF))
    factors_ref[2:, :] = jnp.zeros((6, HALF), f32)
    for k, image_ref in enumerate((image_a, image_b)):
        near = slice(k * WIDE // 2, (k + 1) * WIDE // 2)
        update = on_drift * drift_ref[near, :] + on_image * image_ref[...]
        new_ref[near, :] = x_ref[near, :] + move_size * update
    x = new_ref[:, half_of(lax.axis_index("c"))]
    part = gradient(rows_ref, hot_ref, x, curve_ref, 0, HALF * DATA)
    grad_ref[...] = part - (prior_precision + 2.0 / scale) * x


def last_kernel(before_ref, factors_ref, own_ref, sums_ref, other_ref, out_ref):
    out_ref[0] = factors_ref[:1, :1] * before_ref[0] + factors_ref[1:2, :1] * before_ref[1]
    on_drift, on_image = factors(sums_ref, other_ref)
    out_ref[1] = on_drift * own_ref[0] + on_image * own_ref[1]


def similarity(x_ref, grad_ref, kernel_ref, drift_ref, turned_ref):
    x = x_ref[...]
    for k, value in enumerate(two(x_ref[:, half_of(lax.axis_index("c"))].T)):
        turned_ref[k] = value
    high, low = two(x)
    mixed = tn(high, low)
    gram = tn(high, high) + (mixed + mixed.T)
    shape = (MANY, MANY)
    same = lax.broadcasted_iota(jnp.int32, shape, 0) == lax.broadcasted_iota(jnp.int32, shape, 1)
    diag = jnp.where(same, gram, 0.0)
    squares = jnp.sum(diag, axis=1, keepdims=True) + jnp.sum(diag, axis=0, keepdims=True)
    kernel = jnp.exp((2.0 * gram - squares) / scale)
    kernel_ref[...] = kernel
    total = jnp.sum(kernel, axis=0, keepdims=True)
    own = two(kernel_ref[half_of(lax.axis_index("c")), :])
    drift_ref[...] = (2.0 / scale) * total * x + stacked(two(grad_ref[...]), own)


def start_kernel(grad_ref, own_ref, other_ref, kernel_ref, drift_ref, turned_ref, x_ref):
    x = in_order(lax.axis_index("c"), own_ref[...], other_ref[...], 1)
    x_ref[...] = x
    similarity(x_ref, grad_ref, kernel_ref, drift_ref, turned_ref)


def again_kernel(grad_ref, x_ref, kernel_ref, drift_ref, turned_ref):
    similarity(x_ref, grad_ref, kernel_ref, drift_ref, turned_ref)


def spread(rows_ref, weighted_ref, near):
    return sum(
        tn(rows_ref[span(color), near], weighted_ref[k, span(color), :])
        for color in range(3)
        for k in range(2)
    )


def image_part(rows_ref, near, x_ref, drift, square, q, weighted_ref):
    mine = half_of(lax.axis_index("c"))
    pull = x_ref[near, :] * jnp.sum(q, axis=0, keepdims=True)
    pull = pull - stacked(two(x_ref[near, mine]), two(q))
    own = prior_precision * jnp.sum(square, axis=0, keepdims=True) * drift
    return (spread(rows_ref, weighted_ref, near) + (own + cross * pull)) / MANY


def first_kernel(
    rows_ref, curve_ref, x_ref, turned_ref, kernel_ref, own_ref, other_ref,
    drift_ref, image_ref, factor_ref, weighted_ref, q_ref, square_ref,
):
    core = lax.axis_index("c")
    mine = half_of(core)
    x = x_ref[...]
    drift = (own_ref[...] + stacked(two(other_ref[...]), two(kernel_ref[half_of(1 - core), :]))) / MANY
    drift_ref[...] = drift
    drift_two = two(drift)
    kernel_own = kernel_ref[mine, :]
    square = kernel_own * kernel_own
    square_ref[...] = square
    for at in range(0, HALF * DATA, CHUNK):
        to = pl.ds(at, CHUNK)
        pieces = []
        for start in range(at, at + CHUNK, DATA):
            j = owner_of(start)
            curve = curve_ref[pl.ds(start, DATA), :]
            wide = jnp.concatenate([curve, curve], axis=1)
            pieces.append(jnp.broadcast_to(square_ref[j : j + 1, :], wide.shape) * wide)
        factor = jnp.concatenate(pieces, axis=0)
        factor_ref[to, :] = factor
        rows = rows_ref[to, :]
        high, low = two((nn(rows, drift_two[0]) + nn(rows, drift_two[1])) * factor)
        weighted_ref[0, to, :] = high
        weighted_ref[1, to, :] = low
    along = stacked((turned_ref[0], turned_ref[1]), drift_two)
    q = square * (jnp.sum(x * drift, axis=0, keepdims=True) - along)
    q_ref[...] = q
    near = slice(0, WIDE // 2)
    image_ref[...] = image_part(rows_ref, near, x_ref, drift[near], square, q, weighted_ref)


def rest_kernel(rows_ref, x_ref, kernel_ref, drift_ref, weighted_ref, q_ref, image_ref):
    kernel_own = kernel_ref[half_of(lax.axis_index("c")), :]
    near = slice(WIDE // 2, WIDE)
    image_ref[...] = image_part(
        rows_ref, near, x_ref, drift_ref[near, :], kernel_own * kernel_own, q_ref[...],
        weighted_ref,
    )


def read_image(near, x_ref, turned_ref, drift_ref, image):
    rounded = image.astype(bf16)
    wide = rounded.astype(f32)
    pairs_ = (
        (drift_ref[near, :], drift_ref[near, :]),
        (drift_ref[near, :], image),
        (image, image),
        (image, wide),
        (wide, wide),
        (x_ref[near, :], image),
    )
    sums = [jnp.sum(a * b, axis=0, keepdims=True) for a, b in pairs_]
    x_own = (turned_ref[0, :, near], turned_ref[1, :, near])
    return sums, stacked(x_own, two(image)), rounded


def second_kernel(
    rows_ref, x_ref, turned_ref, drift_ref, own_ref, other_ref,
    image_ref, projected_ref, along_ref, sums_ref,
):
    near = slice(0, WIDE // 2)
    image = own_ref[...] + other_ref[...]
    image_ref[...] = image
    sums, along, rounded = read_image(near, x_ref, turned_ref, drift_ref, image)
    along_ref[...] = along
    for at, value in enumerate(sums):
        sums_ref[at : at + 1, :] = value
    sums_ref[6:, :] = jnp.zeros((2, MANY), f32)
    projected_ref[...] = nn(rows_ref[:, near], rounded)


def third_kernel(
    rows_ref, x_ref, turned_ref, kernel_ref, factor_ref, drift_ref, projected_ref, along_ref, before_ref,
    own_ref, other_ref,
    image_ref, sums_ref,
):
    near = slice(WIDE // 2, WIDE)
    image = own_ref[...] + other_ref[...]
    image_ref[...] = image
    sums, along, rounded = read_image(near, x_ref, turned_ref, drift_ref, image)
    sums = [value + before_ref[at : at + 1, :] for at, value in enumerate(sums)]
    total = jnp.zeros((1, MANY), f32)
    for at in range(0, HALF * DATA, LONG_CHUNK):
        to = pl.ds(at, LONG_CHUNK)
        projected = projected_ref[to, :] + nn(rows_ref[to, near], rounded)
        total += jnp.sum(projected * projected * factor_ref[to, :], axis=0, keepdims=True)
    fit = sums[3] / jnp.maximum(sums[4], 1e-30)
    total *= fit * fit
    mine = half_of(lax.axis_index("c"))
    square = kernel_ref[mine, :] * kernel_ref[mine, :]
    gap = sums[5] - (along + along_ref[...])
    total += cross * jnp.sum(square * gap * gap, axis=0, keepdims=True)
    total += prior_precision * jnp.sum(square, axis=0, keepdims=True) * sums[2]
    for at, value in enumerate((*sums[:3], total / MANY)):
        sums_ref[at : at + 1, :] = jnp.broadcast_to(
            jnp.sum(value, axis=1, keepdims=True), (1, HALF)
        )
    sums_ref[4:, :] = jnp.zeros((4, HALF), f32)


def call(kernel, outs, *args, scratch=(), far=False, aliases=None):
    whole = pl.BlockSpec(memory_space=pltpu.VMEM)
    return pl.pallas_call(
        kernel,
        out_shape=[pltpu.VMEM(s, t) if far else jax.ShapeDtypeStruct(s, t) for s, t in outs],
        in_specs=[pl.BlockSpec(memory_space=pltpu.HBM) if far else whole] * len(args),
        out_specs=[whole] * len(outs),
        scratch_shapes=scratch,
        input_output_aliases=aliases or {},
        compiler_params=pltpu.CompilerParams(vmem_limit_bytes=(60 if far else 24) * 1024 * 1024),
    )(*args)


def per_device(particles, data_rows, labels):
    (copies,) = call(
        prepare_kernel,
        [((8, 8 * DATA + 16, SLICE), bf16)],
        particles, data_rows, labels,
        scratch=[
            pltpu.VMEM((8, SLICE), f32),
            pltpu.VMEM((8, DATA, SLICE), bf16),
            pltpu.VMEM((8, DATA), jnp.int32),
            pltpu.SemaphoreType.DMA((3,)),
        ],
        far=True,
    )
    pieces = gathered(copies)
    count = HALF * DATA
    tall = ((count, MANY), f32)
    square = ((MANY, MANY), f32)
    long = ((WIDE, MANY), f32)
    wing = ((WIDE // 2, MANY), f32)
    low = ((HALF, MANY), f32)
    half = ((WIDE, HALF), f32)
    turn = [pltpu.VMEM((HALF, SLICE), f32)]
    rows_of = ((count, WIDE), bf16)
    tail_of = ((HALF, WIDE), f32)
    turned_of = ((2, HALF, WIDE), bf16)
    curve_of = ((count, HALF), f32)
    rows, tail, hot = call(
        early_kernel,
        [rows_of, tail_of, ((count, HALF), bf16)],
        *(a for four in pieces for a in four[:3]),
    )
    rows, tail, x_own, grad, curve = call(
        position_kernel,
        [rows_of, tail_of, half, half, curve_of],
        rows, tail, hot, pieces[0][3],
        aliases={0: 0, 1: 1},
    )
    x_other = swap_cores(x_own)
    for color in (1, 2):
        rows, grad, curve = call(
            partial(grad_kernel, color),
            [rows_of, half, curve_of],
            rows, grad, curve, hot, x_own, pieces[color][3],
            aliases={0: 0, 1: 1, 2: 2},
        )
    kernel, partial_drift, turned, x = call(
        start_kernel, [square, long, turned_of, long], grad, x_own, x_other
    )
    own = []
    for newton_step in range(NEWTON):
        if newton_step > 0:
            grad, curve, x, weights = call(
                next_kernel, [half, curve_of, long, ((8, HALF), f32)],
                rows, hot, x, drift, *image, sums, sums_other,
            )
        grad_other = swap_cores(grad)
        if newton_step > 0:
            kernel, partial_drift, turned = call(
                again_kernel, [square, long, turned_of], grad, x
            )
        drift, own_a, factor, weighted, q = call(
            first_kernel,
            [long, wing, tall, ((2, count, MANY), bf16), low],
            rows, curve, x, turned, kernel, partial_drift, grad_other,
            scratch=[pltpu.VMEM((HALF, MANY), f32)],
        )
        other_a = swap_cores(own_a)
        (own_b,) = call(rest_kernel, [wing], rows, x, kernel, drift, weighted, q)
        other_b = swap_cores(own_b)
        image_a, projected, along, partial_sums = call(
            second_kernel, [wing, tall, low, ((8, MANY), f32)],
            rows, x, turned, drift, own_a, other_a,
        )
        image_b, sums = call(
            third_kernel, [wing, ((8, HALF), f32)],
            rows, x, turned, kernel, factor, drift, projected, along, partial_sums, own_b, other_b,
        )
        image = (image_a, image_b)
        sums_other = swap_cores(sums)
        own += call(own_kernel, [((2, 8, SLICE), f32)], drift, *image, scratch=turn)
    (updates,) = call(
        last_kernel, [((NEWTON, 8, SLICE), f32)], own[0], weights, own[1], sums, sums_other
    )
    return updates


def solution(mesh):
    torus = Mesh(mesh.devices.reshape(4, 4, 2, mesh.shape["dim"]), AXES)
    groups = ("y", "x", "c")
    in_specs = (P(groups, "z"), P(groups, None, "z"), P(groups, None))
    out_specs = P(None, groups, "z")

    return jax.shard_map(
        per_device, mesh=torus, in_specs=in_specs, out_specs=out_specs, check_vma=False
    )
```
